32 devices in a mesh: ia: 4 (over y, x), ja: 4 (over z), col: 2 (over core).
Axes of the slice: x: 2, y: 2, z: 4, core: 2. Of those that a mesh axis runs over, the one named last changes fastest.
Arguments:
- pair_rep: bfloat16 [512, 512, 128], P('ia', 'ja'), may hold values from -6 to 6
- norm_gain: float32 [128], replicated, may hold values from 0.1 to 1.9
- weights: bfloat16 [4, 128, 128], P(None, None, 'col'), may hold values from -0.5 to 0.5
- residue_mask: int32 [512], replicated, may hold values 0 or 1
- product_grad: bfloat16 [512, 128, 512], P('ia', 'col', 'ja'), may hold values from -1 to 1
Outputs:
- pair_grad: bfloat16 [512, 512, 128], P('ia', 'ja')
- weight_grads: float32 [4, 128, 128], P(None, None, 'col')
The draws below stay inside these ranges and needn't reach their ends.
All inputs are finite; a program needn't handle non-finite values.
Results may differ from the reference program's by a relative error of at most 0.0067.
Values may be sent and summed in bfloat16 or wider, within the bound.
A program may use at most 128 MiB of HBM per device.

```python
import jax
import jax.numpy as jnp
from jax import lax

C = 128
HID = 128
N = 512


def draw_product_grad(key, part):
    gaussian = jax.random.normal(jax.random.fold_in(key, 11), (N, HID, N), jnp.float32)
    drawn = 0.0625 * gaussian
    return jnp.clip(drawn, -1.0, 1.0).astype(jnp.bfloat16)


def set_ends(result, own_key, least, largest):
    longest = result.shape.index(max(result.shape))
    spots = []
    for shift in (0, 1):
        where = [jax.random.randint(jax.random.fold_in(own_key, axis), (), 0, length) for axis, length in enumerate(result.shape)]
        where[longest] = (where[longest] + shift) % result.shape[longest]
        spots.append(tuple(where))
    return result.at[spots[0]].set(least).at[spots[1]].set(largest)


def levels(rng, extent, shards, least, largest):
    level, own = 1.0, jax.random.fold_in(rng, 6)
    for dim, blocks in shards:
        steps = jnp.exp(jax.random.uniform(jax.random.fold_in(own, dim), (blocks,), jnp.float32, least / len(shards), largest / len(shards)))
        level = level * jnp.repeat(steps, extent[dim] // blocks).reshape([-1 if axis == dim else 1 for axis in range(len(extent))])
    return level


def noise(stream_key, dims, width, reach, shards=(), held_as=jnp.bfloat16):
    level = levels(stream_key, dims, shards, -0.22, 0.18) if shards else 1.0
    entries = jax.random.normal(stream_key, dims, jnp.float32) * width * level
    return jnp.minimum(jnp.maximum(entries, -reach), reach).astype(held_as)


def setup_inputs(seed: int = 0) -> dict:
    seeds = jax.random.split(jax.random.key(seed), 6)
    pair_rep = noise(seeds[0], (N, N, C), 1.0, 6.0, ((0, 4), (1, 4)))
    norm_gain = jnp.clip(1.0 + 0.18 * jax.random.normal(seeds[1], (C,), jnp.float32), 0.1, 1.9)
    weights = noise(seeds[2], (4, C, HID), C ** -0.5, 0.5, ((2, 2),))
    residue_mask = set_ends((jax.random.randint(seeds[3], (N,), 0, 8) < 7).astype(jnp.int32), jax.random.fold_in(seeds[3], 1), 0, 1)
    product_grad = draw_product_grad(jax.random.fold_in(seeds[5], 71), 0)
    return {"pair_rep": pair_rep, "norm_gain": norm_gain, "weights": weights, "residue_mask": residue_mask, "product_grad": product_grad}


CLIP_LIMIT = 64.0

def gate_terms(incoming, linear, gate_pre, pair_valid):
    sigmoid_gate = jax.nn.sigmoid(gate_pre)
    through = incoming * pair_valid
    return (through * sigmoid_gate, through * linear * sigmoid_gate * (1.0 - sigmoid_gate))

def reference(pair_rep, norm_gain, weights, residue_mask, product_grad):
    floats = pair_rep.astype(jnp.float32)
    centred = floats - lax.optimization_barrier(jnp.mean(floats, axis=-1, keepdims=True))
    inv_std = lax.rsqrt(lax.optimization_barrier(jnp.mean(centred * centred, axis=-1, keepdims=True)) + 1e-05)
    unit_rows = centred * inv_std
    normed = (unit_rows * norm_gain).astype(jnp.bfloat16)
    validity = residue_mask.astype(jnp.float32)
    pair_valid = validity[:, None, None] * validity[None, None, :]
    normed_wide = normed.astype(jnp.float32)
    weights_wide = weights.astype(jnp.float32)
    projected = [jnp.einsum('ikd,dc->ick', normed_wide, weights_wide[which]) for which in range(4)]
    left_side = (pair_valid * jax.nn.sigmoid(projected[1]) * projected[0]).astype(jnp.bfloat16)
    right_side = (pair_valid * jax.nn.sigmoid(projected[3]) * projected[2]).astype(jnp.bfloat16)
    grad_wide = product_grad.astype(jnp.float32)
    grad_left = jnp.einsum('icj,jck->ick', grad_wide, right_side.astype(jnp.float32))
    grad_right = jnp.einsum('icj,ick->jck', grad_wide, left_side.astype(jnp.float32))
    lin_a, gate_a = gate_terms(grad_left, projected[0], projected[1], pair_valid)
    lin_b, gate_b = gate_terms(grad_right, projected[2], projected[3], pair_valid)
    raw_list = []
    normed_grad = jnp.zeros(floats.shape, jnp.float32)
    for which, term in enumerate((lin_a, gate_a, lin_b, gate_b)):
        rounded = lax.optimization_barrier(term.astype(jnp.bfloat16)).astype(jnp.float32)
        raw_list.append(jnp.einsum('ikd,ick->dc', normed_wide, rounded))
        normed_grad = normed_grad + jnp.einsum('ick,dc->ikd', rounded, weights_wide[which])
    scaled = normed_grad * norm_gain
    pair_grad = inv_std * (scaled - lax.optimization_barrier(jnp.mean(scaled, axis=-1, keepdims=True)) - unit_rows * lax.optimization_barrier(jnp.mean(scaled * unit_rows, axis=-1, keepdims=True)))
    raw = jnp.stack(raw_list)
    squares = jnp.sum(raw * raw)
    factor = jnp.minimum(1.0, CLIP_LIMIT * lax.rsqrt(squares + 1e-06))
    return (pair_grad.astype(jnp.bfloat16), raw * factor)
```

```python
import functools
import math

import jax
import jax.numpy as jnp
from jax import lax
from jax.experimental import pallas as pl
from jax.experimental.pallas import tpu as pltpu
from jax.sharding import PartitionSpec as P

CLIP_LIMIT = 64.0
MAX_CHUNKS = 4
MESH = pl.DeviceIdType.MESH
NT = (((1,), (1,)), ((), ()))
NN = (((1,), (0,)), ((), ()))
F32 = jnp.float32
BF16 = jnp.bfloat16


def partner(index, step, count):
    if count & (count - 1) == 0:
        return index ^ step
    return (step - index + count) % count


def exchange(value, axis, step, count):
    return lax.ppermute(value, axis, [(a, partner(a, step, count)) for a in range(count)])


def dot(a, b, dims):
    return lax.dot_general(a, b, dims, preferred_element_type=F32)


def eye(n):
    rows = lax.broadcasted_iota(jnp.int32, (n, n), 0)
    cols = lax.broadcasted_iota(jnp.int32, (n, n), 1)
    return jnp.where(rows == cols, 1.0, 0.0).astype(BF16)


class Sizes:
    def __init__(self, na, nz, nh, rows, cols, depth, ch):
        self.na, self.nz, self.nh = na, nz, nh
        self.rb, self.k, self.d, self.ch = rows, cols, depth, ch
        self.g = na * nh
        self.rh = rows // nh
        self.hid = ch * nh
        self.cp = ch // na
        self.nq = math.gcd(self.cp, MAX_CHUNKS)
        self.cq = self.cp // self.nq
        self.nc = self.g * self.cq
        self.i = na * rows
        self.br = math.gcd(self.rh, 16)
        self.nb = self.rh // self.br
        self.sp = self.hid + 8
        self.tp = self.br + 8


def kernel(z_, p_ref, x_hbm, wall_ref, wt_ref, gain_ref, pv_ref, out_ref, raw_ref,
           xv, pg, unit_s, inv_s, nt_s, pr, fac, relay, lrs, lrb, gs, gr, turn, ng,
           xsem, psend, precv, zsend, zrecv, lsend, lrecv, gsend, grecv, osend, orecv):
    s = z_
    na, nz, nh, g_n, nq, cq, cp, nc = s.na, s.nz, s.nh, s.g, s.nq, s.cq, s.cp, s.nc
    rb, rh, k, d, hid, br, nb = s.rb, s.rh, s.k, s.d, s.hid, s.br, s.nb
    a, z, h = lax.axis_index("ia"), lax.axis_index("ja"), lax.axis_index("col")
    me_g = h * na + a
    row0 = a * rb + h * rh

    def plane(g):
        return (lax.rem(g, na), z, lax.div(g, na))

    def peer_g(step):
        return lax.rem(me_g + step, g_n)

    def from_g(step):
        return lax.rem(me_g + g_n - step, g_n)

    barrier = pltpu.get_barrier_semaphore()
    for step in range(1, g_n):
        pl.semaphore_signal(barrier, inc=1, device_id=plane(peer_g(step)), device_id_type=MESH)

    @pl.when(z > 0)
    def _():
        pl.semaphore_signal(barrier, inc=1, device_id=(a, z - 1, h), device_id_type=MESH)

    @pl.when(z < nz - 1)
    def _():
        pl.semaphore_signal(barrier, inc=1, device_id=(a, z + 1, h), device_id_type=MESH)

    xcopy = pltpu.make_async_copy(x_hbm.at[pl.ds(h * rh, rh)], xv, xsem)
    xcopy.start()
    ends = jnp.where(z > 0, 1, 0) + jnp.where(z < nz - 1, 1, 0)
    pl.semaphore_wait(barrier, g_n - 1 + ends)

    def p_copy(q, step):
        return pltpu.make_async_remote_copy(
            src_ref=p_ref.at[lax.rem(a + step, na), q],
            dst_ref=pg.at[z, pl.ds(q * cq, cq), pl.ds(a * rb, rb)],
            send_sem=psend.at[q, step], recv_sem=precv.at[q, step],
            device_id=(lax.rem(a + step, na), z, h), device_id_type=MESH)

    for q in range(nq):
        for step in range(1, na):
            p_copy(q, step).start()
    for q in range(nq):
        for r in range(cq):
            pg[z, q * cq + r, pl.ds(a * rb, rb), :] = p_ref[a, q, r]

    def z_copy(q, block, up):
        ref = pg.at[block, pl.ds(q * cq, cq)]
        return pltpu.make_async_remote_copy(
            src_ref=ref, dst_ref=ref,
            send_sem=zsend.at[q, block, 0 if up else 1], recv_sem=zrecv.at[q, block],
            device_id=(a, z + 1 if up else z - 1, h), device_id_type=MESH)

    def z_own(q):
        for step in range(1, na):
            p_copy(q, step).wait_recv()

        @pl.when(z < nz - 1)
        def _():
            z_copy(q, z, True).start()

        @pl.when(z > 0)
        def _():
            z_copy(q, z, False).start()

    def z_hop(q, hop):
        @pl.when(z >= hop)
        def _():
            z_copy(q, z - hop, True).wait_recv()

            @pl.when(z < nz - 1)
            def _():
                z_copy(q, z - hop, True).start()

        @pl.when(z + hop < nz)
        def _():
            z_copy(q, z + hop, False).wait_recv()

            @pl.when(z > 0)
            def _():
                z_copy(q, z + hop, False).start()

    eye_d = eye(d)
    xcopy.wait()

    def rows_step(t, sub):
        x2 = xv[pl.ds(2 * t, 2)].reshape(2 * k, d)
        xt = dot(eye_d, x2, NT)
        centred = xt - jnp.mean(xt, axis=0, keepdims=True)
        inv = lax.rsqrt(jnp.mean(centred * centred, axis=0, keepdims=True) + 1e-05)
        unit = centred * inv
        normed = (unit * gain_ref[...]).astype(BF16)
        unit_s[t] = unit
        inv_s[t] = inv
        nt_s[t] = normed
        pr[...] = dot(wall_ref[...], normed, NN)
        valid = pv_ref[pl.ds(h * (rh // 2) + t, 1), :]
        for q in range(nq):
            for side in range(2):
                lin = pr[pl.ds((2 * side) * hid + q * nc, nc), :]
                gate = jax.nn.sigmoid(pr[pl.ds((2 * side + 1) * hid + q * nc, nc), :])
                first = valid * gate
                value = first * lin
                fac[t, q, 2 * side] = first.astype(BF16)
                fac[t, q, 2 * side + 1] = (value * (1.0 - gate)).astype(BF16)
                for e in range(2):
                    at = pl.multiple_of((2 * sub + e) * s.sp, 8) + q * nc
                    relay[side, pl.ds(at, nc), :] = value[:, e * k:(e + 1) * k]

    for b in range(nb):
        def one(sub, carry, b=b):
            rows_step(b * (br // 2) + sub, sub)
            return carry
        lax.fori_loop(0, br // 2, one, 0)

        def flush(c, carry, b=b):
            for side in range(2):
                tile = relay[side, pl.ds(c, br, stride=s.sp), :]
                lrs[side, c, pl.ds(b * br, br), :] = tile.astype(BF16)
            return carry
        lax.fori_loop(0, hid, flush, 0, unroll=4)
        if b < nq:
            z_own(b)
    for q in range(nb, nq):
        z_own(q)

    def lr_copy(q, step):
        return pltpu.make_async_remote_copy(
            src_ref=lrs.at[:, pl.ds(q * nc + peer_g(step) * cq, cq)],
            dst_ref=lrb.at[:, pl.ds(q * cq, cq), pl.ds(row0, rh)],
            send_sem=lsend.at[q, step], recv_sem=lrecv.at[q, step],
            device_id=plane(peer_g(step)), device_id_type=MESH)

    for q in range(nq):
        for step in range(1, g_n):
            lr_copy(q, step).start()
    for q in range(nq):
        for side in range(2):
            for r in range(cq):
                lrb[side, q * cq + r, pl.ds(row0, rh), :] = lrs[side, q * nc + me_g * cq + r]

    eye_k = eye(k)

    def triangle(c):
        panel = jnp.concatenate([pg[b, c] for b in range(nz)], axis=1)
        left, right = lrb[0, c], lrb[1, c]
        gs[0, c] = dot(panel, right, NN).astype(BF16)
        left_t = dot(eye_k, left, NT).astype(BF16)
        back_t = dot(left_t, panel, NN).astype(BF16)
        for b in range(nz):
            gs[1, c, b * k:(b + 1) * k, :] = dot(eye_k, back_t[:, b * k:(b + 1) * k], NT).astype(BF16)

    def g_copy(q, step):
        g = peer_g(step)
        return pltpu.make_async_remote_copy(
            src_ref=gs.at[:, pl.ds(q * cq, cq), pl.ds(lax.rem(g, na) * rb + lax.div(g, na) * rh, rh)],
            dst_ref=gr.at[:, pl.ds(q * nc + me_g * cq, cq)],
            send_sem=gsend.at[q, step], recv_sem=grecv.at[q, step],
            device_id=plane(g), device_id_type=MESH)

    def out_copy(b, step):
        ref = out_ref.at[pl.ds(h * rh + b * br, br)]
        return pltpu.make_async_remote_copy(
            src_ref=ref, dst_ref=ref, send_sem=osend.at[b, step], recv_sem=orecv.at[b, step],
            device_id=(a, z, lax.rem(h + step, nh)), device_id_type=MESH)

    def collect(q):
        for step in range(1, g_n):
            g_copy(q, step).wait_recv()
        raw_ref[q] = jnp.zeros((4 * nc, d), F32)
        for b in range(nb):
            def spread(n, carry, b=b):
                for side in range(2):
                    tile = gr[side, q * nc + n, pl.ds(b * br, br), :].astype(F32)
                    turn[side, pl.ds(pl.multiple_of(n * s.tp, 8), br), :] = tile
                return carry
            lax.fori_loop(0, nc, spread, 0, unroll=4)

            def one(sub, carry, b=b):
                t = b * (br // 2) + sub
                parts = []
                for side in range(2):
                    both = jnp.concatenate(
                        [turn[side, pl.ds(2 * sub + e, nc, stride=s.tp), :] for e in range(2)], axis=1)
                    for w in range(2):
                        parts.append((both * fac[t, q, 2 * side + w].astype(F32)).astype(BF16))
                grads = jnp.concatenate(parts, axis=0)
                raw_ref[q] += dot(grads, nt_s[t], NT)
                part = dot(wt_ref[q], grads, NN)
                if q:
                    part = part + ng[t]
                if q < nq - 1:
                    ng[t] = part
                else:
                    unit = unit_s[t]
                    scaled = part * gain_ref[...]
                    first = jnp.mean(scaled, axis=0, keepdims=True)
                    second = jnp.mean(scaled * unit, axis=0, keepdims=True)
                    res = (inv_s[t] * (scaled - first - unit * second)).astype(BF16)
                    for e in range(2):
                        out_ref[h * rh + 2 * t + e] = dot(
                            eye_k, res[:, e * k:(e + 1) * k], NT).astype(BF16)
                return carry
            lax.fori_loop(0, br // 2, one, 0)
            if q == nq - 1:
                for step in range(1, nh):
                    out_copy(b, step).start()

    for hop in range(1, nz - 1):
        for q in range(nq):
            z_hop(q, hop)
    for q in range(nq):
        z_hop(q, nz - 1)
        for step in range(1, g_n):
            lr_copy(q, step).wait_recv()

        def tri(r, carry, q=q):
            triangle(q * cq + r)
            return carry
        lax.fori_loop(0, cq, tri, 0)
        for step in range(1, g_n):
            g_copy(q, step).start()
        for side in range(2):
            for r in range(cq):
                gr[side, q * nc + me_g * cq + r] = gs[side, q * cq + r, pl.ds(row0, rh), :]
        if q:
            collect(q - 1)
    collect(nq - 1)

    for b in range(nb):
        for step in range(1, nh):
            out_copy(b, step).wait()
    for q in range(nq):
        for step in range(1, na):
            p_copy(q, step).wait_send()
        for step in range(1, g_n):
            lr_copy(q, step).wait_send()
            g_copy(q, step).wait_send()
        for hop in range(nz):
            @pl.when((z >= hop) & (z < nz - 1))
            def _(q=q, hop=hop):
                z_copy(q, z - hop, True).wait_send()

            @pl.when((z + hop < nz) & (z > 0))
            def _(q=q, hop=hop):
                z_copy(q, z + hop, False).wait_send()


def on_device(na, nz, nh, pair_rep, norm_gain, weights, residue_mask, product_grad):
    rows, cols, depth = pair_rep.shape
    ch = product_grad.shape[1]
    s = Sizes(na, nz, nh, rows, cols, depth, ch)
    panels = product_grad.transpose(1, 0, 2).reshape(na, s.nq, s.cq, rows, cols)
    every = lax.all_gather(weights, "col", axis=0)
    every = every.reshape(nh, 4, depth, na, s.nq, s.cq)
    wall = every.transpose(1, 4, 0, 3, 5, 2).reshape(4 * s.hid, depth)
    wt = every.transpose(4, 2, 1, 0, 3, 5).reshape(s.nq, depth, 4 * s.nc)
    gain = jnp.broadcast_to(norm_gain[:, None], (depth, 2 * cols))
    validity = residue_mask.astype(F32)
    row_valid = lax.dynamic_slice_in_dim(validity, lax.axis_index("ia") * rows, rows)
    col_valid = lax.dynamic_slice_in_dim(validity, lax.axis_index("ja") * cols, cols)
    valid = (row_valid[:, None] * col_valid[None, :]).reshape(rows // 2, 2 * cols)

    vm = pl.BlockSpec(memory_space=pltpu.VMEM)
    dma = pltpu.SemaphoreType.DMA
    half = s.rh // 2
    scratch = [
        pltpu.VMEM((s.rh, cols, depth), BF16),
        pltpu.VMEM((nz, s.cp, s.i, cols), BF16),
        pltpu.VMEM((half, depth, 2 * cols), F32),
        pltpu.VMEM((half, 1, 2 * cols), F32),
        pltpu.VMEM((half, depth, 2 * cols), BF16),
        pltpu.VMEM((4 * s.hid, 2 * cols), F32),
        pltpu.VMEM((half, s.nq, 4, s.nc, 2 * cols), BF16),
        pltpu.VMEM((2, s.br * s.sp, cols), F32),
        pltpu.VMEM((2, s.hid, s.rh, cols), BF16),
        pltpu.VMEM((2, s.cp, s.i, cols), BF16),
        pltpu.VMEM((2, s.cp, s.i, cols), BF16),
        pltpu.VMEM((2, s.hid, s.rh, cols), BF16),
        pltpu.VMEM((2, s.nc * s.tp, cols), F32),
        pltpu.VMEM((half, depth, 2 * cols), F32),
        dma(()), dma((s.nq, na)), dma((s.nq, na)), dma((s.nq, nz, 2)), dma((s.nq, nz)),
        dma((s.nq, s.g)), dma((s.nq, s.g)), dma((s.nq, s.g)), dma((s.nq, s.g)),
        dma((s.nb, nh)), dma((s.nb, nh)),
    ]
    pair_grad, raw = pl.pallas_call(
        functools.partial(kernel, s),
        out_shape=(
            jax.ShapeDtypeStruct((rows, cols, depth), BF16),
            jax.ShapeDtypeStruct((s.nq, 4 * s.nc, depth), F32),
        ),
        in_specs=[vm, pl.BlockSpec(memory_space=pl.ANY), vm, vm, vm, vm],
        out_specs=(vm, vm),
        scratch_shapes=scratch,
        compiler_params=pltpu.CompilerParams(
            collective_id=0, has_side_effects=True, vmem_limit_bytes=66 * 1000 * 1000),
    )(panels, pair_rep, wall, wt, gain, valid)

    raw = raw.reshape(s.nq, 4, nh, na, s.cq, depth)
    parts = raw.transpose(2, 1, 5, 3, 0, 4).reshape(nh, 4, depth, ch)
    if nh == 2:
        mine = lax.axis_index("col")
        other = lax.dynamic_index_in_dim(parts, 1 - mine, 0, keepdims=False)
        summed = lax.dynamic_index_in_dim(parts, mine, 0, keepdims=False) + exchange(other, "col", 1, 2)
    else:
        summed = lax.dynamic_index_in_dim(lax.psum(parts, "col"), lax.axis_index("col"), 0, keepdims=False)
    for axis, count in (("ia", na), ("ja", nz)):
        if count & (count - 1):
            summed = lax.psum(summed, axis)
            continue
        step = 1
        while step < count:
            summed = summed + exchange(summed, axis, step, count)
            step *= 2
    squares = lax.psum(jnp.sum(summed * summed), "col")
    factor = jnp.minimum(1.0, CLIP_LIMIT * lax.rsqrt(squares + 1e-06))
    return (pair_grad, summed * factor)


def solution(mesh):
    sizes = mesh.shape["ia"], mesh.shape["ja"], mesh.shape["col"]
    placed = (P("ia", "ja", None), P(), P(None, None, "col"), P(), P("ia", "col", "ja"))

    def step(*args):
        return on_device(*sizes, *args)

    return jax.shard_map(
        step,
        mesh=mesh,
        in_specs=placed,
        out_specs=(P("ia", "ja", None), P(None, None, "col")),
        check_vma=False,
    )
```

```python
import functools
import math

import jax
import jax.numpy as jnp
from jax import lax
from jax.experimental import pallas as pl
from jax.experimental.pallas import tpu as pltpu
from jax.sharding import PartitionSpec as P

CLIP_LIMIT = 64.0
MAX_CHUNKS = 4
ROWS_AT_ONCE = 2
VMEM_LIMIT = 66 * 1000 * 1000
MESH = pl.DeviceIdType.MESH
NT = (((1,), (1,)), ((), ()))
NN = (((1,), (0,)), ((), ()))
F32 = jnp.float32
BF16 = jnp.bfloat16


def dot(a, b, dims):
    return lax.dot_general(a, b, dims, preferred_element_type=F32)


def eye(n):
    rows = lax.broadcasted_iota(jnp.int32, (n, n), 0)
    cols = lax.broadcasted_iota(jnp.int32, (n, n), 1)
    return jnp.where(rows == cols, 1.0, 0.0).astype(BF16)


class Sizes:
    def __init__(self, na, nz, nh, rows, cols, depth, ch):
        self.na, self.nz, self.nh = na, nz, nh
        self.rb, self.k, self.d, self.ch = rows, cols, depth, ch
        self.g = na * nh
        self.naz = na * nz
        self.rh = rows // nh
        self.hid = ch * nh
        self.cp = ch // na
        self.nq = math.gcd(self.cp, MAX_CHUNKS)
        self.cq = self.cp // self.nq
        self.m = na * self.cq
        self.nc = self.g * self.cq
        self.i = na * rows
        self.br = math.gcd(self.rh, 16)
        self.nb = self.rh // self.br
        self.bi = math.gcd(self.rb, 16)
        self.sp = self.hid + 8
        self.pp = self.m + 8
        self.tp = self.br + 8
        self.tb = math.gcd(self.br // 2, ROWS_AT_ONCE)
        self.rs = 4 * self.m // self.naz


def kernel(s, p_ref, x_hbm, w_ref, gain_ref, mask_ref, mask_s, out_ref, wg_ref,
           xv, pt, pg, wall, wt, gain, unit_s, inv_s, nt_s, pr, fac, relay, lrs, lrb, gs, gr, turn, ng,
           raw, rx1, mine_s, rx2, rx3, sq,
           xsem, wsend, wrecv, psend, precv, zsend, zrecv, lsend, lrecv, gsend, grecv, osend, orecv,
           r1s, r1r, r2s, r2r, r3s, r3r, qs, qr):
    na, nz, nh, g_n, nq, cq, nc = s.na, s.nz, s.nh, s.g, s.nq, s.cq, s.nc
    rb, rh, k, d, ch, hid, br, nb, m = s.rb, s.rh, s.k, s.d, s.ch, s.hid, s.br, s.nb, s.m
    a, z, h = lax.axis_index("ia"), lax.axis_index("ja"), lax.axis_index("col")
    me_g = h * na + a
    me_n = a * nz + z
    row0 = a * rb + h * rh

    def plane(g):
        return (lax.rem(g, na), z, lax.div(g, na))

    def peer_g(step):
        return lax.rem(me_g + step, g_n)

    def send(src, dst, send_sem, recv_sem, device):
        return pltpu.make_async_remote_copy(
            src_ref=src, dst_ref=dst, send_sem=send_sem, recv_sem=recv_sem,
            device_id=device, device_id_type=MESH)

    barrier = pltpu.get_barrier_semaphore()
    total = s.naz * nh
    for step in range(1, total):
        to = lax.rem(me_n * nh + h + step, total)
        device = (lax.div(to, nz * nh), lax.rem(lax.div(to, nh), nz), lax.rem(to, nh))
        pl.semaphore_signal(barrier, inc=1, device_id=device, device_id_type=MESH)
    xcopy = pltpu.make_async_copy(x_hbm.at[pl.ds(h * rh, rh)], xv, xsem)
    xcopy.start()

    def p_turn(q):
        def block(ib, carry):
            slot = lax.rem(ib, 2)
            for ii in range(s.bi):
                relay[slot, ii * s.pp:ii * s.pp + m, :] = p_ref[ib * s.bi + ii, q * m:(q + 1) * m, :].astype(F32)
            for c in range(m):
                tile = relay[slot, pl.ds(c, s.bi, stride=s.pp), :]
                pt[q * m + c, pl.ds(pl.multiple_of(ib * s.bi, s.bi), s.bi), :] = tile.astype(BF16)
            return carry
        lax.fori_loop(0, rb // s.bi, block, 0)

    def p_copy(q, step):
        to = lax.rem(a + step, na)
        return send(pt.at[pl.ds(q * m + to * cq, cq)], pg.at[z, pl.ds(q * cq, cq), pl.ds(a * rb, rb)],
                    psend.at[q, step], precv.at[q, step], (to, z, h))

    def w_copy(step):
        return send(w_ref, wall.at[h], wsend.at[step], wrecv.at[step], (a, z, lax.rem(h + step, nh)))

    p_turn(0)
    pl.semaphore_wait(barrier, total - 1)
    for step in range(1, nh):
        w_copy(step).start()
    for q in range(nq):
        if q:
            p_turn(q)
        for step in range(1, na):
            p_copy(q, step).start()
    for q in range(nq):
        for r in range(cq):
            pg[z, q * cq + r, pl.ds(a * rb, rb), :] = pt[q * m + a * cq + r]

    def z_copy(q, block, up):
        ref = pg.at[block, pl.ds(q * cq, cq)]
        return send(ref, ref, zsend.at[q, block, 0 if up else 1], zrecv.at[q, block],
                    (a, z + 1 if up else z - 1, h))

    def z_own(q):
        for step in range(1, na):
            p_copy(q, step).wait_recv()

        @pl.when(z < nz - 1)
        def _():
            z_copy(q, z, True).start()

        @pl.when(z > 0)
        def _():
            z_copy(q, z, False).start()

    def z_hop(q, hop):
        @pl.when(z >= hop)
        def _():
            z_copy(q, z - hop, True).wait_recv()

            @pl.when(z < nz - 1)
            def _():
                z_copy(q, z - hop, True).start()

        @pl.when(z + hop < nz)
        def _():
            z_copy(q, z + hop, False).wait_recv()

            @pl.when(z > 0)
            def _():
                z_copy(q, z + hop, False).start()

    eye_d = eye(d)
    column = jnp.transpose(jnp.broadcast_to(gain_ref[...], (k, d)))
    gain[...] = jnp.concatenate([column, column], axis=1)
    wall[h] = w_ref[...]
    for step in range(1, nh):
        w_copy(step).wait_recv()
    for q in range(nq):
        rows = [wall[half, w, q * m:(q + 1) * m, :] for half in range(nh) for w in range(4)]
        wt[q] = dot(eye_d, jnp.concatenate(rows, axis=0), NT).astype(BF16)

    xcopy.wait()
    col_valid = mask_ref[pl.ds(z, 1), :].astype(F32)

    def rows_step(t, sub):
        x2 = xv[pl.ds(2 * t, 2)].reshape(2 * k, d)
        xt = dot(eye_d, x2, NT)
        centred = xt - jnp.mean(xt, axis=0, keepdims=True)
        inv = lax.rsqrt(jnp.mean(centred * centred, axis=0, keepdims=True) + 1e-05)
        unit = centred * inv
        normed = (unit * gain[...]).astype(BF16)
        unit_s[t] = unit
        inv_s[t] = inv
        nt_s[t] = normed
        for half in range(nh):
            pr[half * 4 * ch:(half + 1) * 4 * ch, :] = dot(wall[half].reshape(4 * ch, d), normed, NN)
        valid = jnp.concatenate(
            [col_valid * mask_s[row0 + 2 * t + e].astype(F32) for e in range(2)], axis=1)
        for q in range(nq):
            for side in range(2):
                def part(w):
                    at = [half * 4 * ch + w * ch + q * m for half in range(nh)]
                    return jnp.concatenate([pr[x:x + m, :] for x in at], axis=0)
                lin = part(2 * side)
                gate = jax.nn.sigmoid(part(2 * side + 1))
                first = valid * gate
                value = first * lin
                fac[t, q, 2 * side] = first.astype(BF16)
                fac[t, q, 2 * side + 1] = (value * (1.0 - gate)).astype(BF16)
                for e in range(2):
                    at = pl.multiple_of((2 * sub + e) * s.sp, 8) + q * nc
                    relay[side, pl.ds(at, nc), :] = value[:, e * k:(e + 1) * k]

    for b in range(nb):
        def one(sub, carry, b=b):
            rows_step(b * (br // 2) + sub, sub)
            return carry
        lax.fori_loop(0, br // 2, one, 0)

        def flush(c, carry, b=b):
            for side in range(2):
                tile = relay[side, pl.ds(c, br, stride=s.sp), :]
                lrs[side, c, b * br:(b + 1) * br, :] = tile.astype(BF16)
            return carry
        lax.fori_loop(0, hid, flush, 0, unroll=4)
        if b < nq:
            z_own(b)
    for q in range(nb, nq):
        z_own(q)

    def lr_copy(q, step):
        return send(lrs.at[:, pl.ds(q * nc + peer_g(step) * cq, cq)],
                    lrb.at[:, pl.ds(q * cq, cq), pl.ds(row0, rh)],
                    lsend.at[q, step], lrecv.at[q, step], plane(peer_g(step)))

    for q in range(nq):
        for step in range(1, g_n):
            lr_copy(q, step).start()
    for q in range(nq):
        for side in range(2):
            for r in range(cq):
                lrb[side, q * cq + r, pl.ds(row0, rh), :] = lrs[side, q * nc + me_g * cq + r]

    eye_k = eye(k)

    def triangle(c):
        panel = jnp.concatenate([pg[b, c] for b in range(nz)], axis=1)
        left, right = lrb[0, c], lrb[1, c]
        gs[0, c] = dot(panel, right, NN).astype(BF16)
        left_t = dot(eye_k, left, NT).astype(BF16)
        back_t = dot(left_t, panel, NN).astype(BF16)
        for b in range(nz):
            gs[1, c, b * k:(b + 1) * k, :] = dot(eye_k, back_t[:, b * k:(b + 1) * k], NT).astype(BF16)

    def g_copy(q, b, step):
        g = peer_g(step)
        row = lax.rem(g, na) * rb + lax.div(g, na) * rh + b * br
        return send(gs.at[:, pl.ds(q * cq, cq), pl.ds(row, br)],
                    gr.at[:, pl.ds(q * nc + me_g * cq, cq), pl.ds(b * br, br)],
                    gsend.at[q, b, step], grecv.at[q, b, step], plane(g))

    def out_copy(b, step):
        ref = out_ref.at[pl.ds(h * rh + b * br, br)]
        return send(ref, ref, osend.at[b, step], orecv.at[b, step], (a, z, lax.rem(h + step, nh)))

    def r1_copy(q, step):
        to = lax.rem(h + step, nh)
        return send(raw.at[q, to], rx1.at[q, step], r1s.at[q, step], r1r.at[q, step], (a, z, to))

    def r1_sum(q):
        mine = raw[q, h]
        for step in range(1, nh):
            r1_copy(q, step).wait_recv()
            mine = mine + rx1[q, step]
        for n in range(s.naz):
            mine_s[n, q] = mine[n * s.rs:(n + 1) * s.rs]

    def peer_n(step):
        return lax.rem(me_n + step, s.naz)

    def at_n(n):
        return (lax.div(n, nz), lax.rem(n, nz), h)

    batches = [(0, nq - 1), (nq - 1, nq)] if nq > 1 else [(0, nq)]

    def r2_copy(batch, step):
        lo, hi = batches[batch]
        n = peer_n(step)
        return send(mine_s.at[n, lo:hi], rx2.at[step, lo:hi], r2s.at[batch, step], r2r.at[batch, step], at_n(n))

    def r2_sum(batch):
        lo, hi = batches[batch]
        mine = mine_s[me_n, lo:hi]
        for step in range(1, s.naz):
            r2_copy(batch, step).wait_recv()
            mine = mine + rx2[step, lo:hi]
        rx3[me_n, lo:hi] = mine

    def r3_copy(batch, step):
        lo, hi = batches[batch]
        ref = rx3.at[me_n, lo:hi]
        return send(ref, ref, r3s.at[batch, step], r3r.at[batch, step], at_n(peer_n(step)))

    def sq_copy(step):
        return send(sq.at[0], sq.at[step], qs.at[step], qr.at[step], (a, z, lax.rem(h + step, nh)))

    def gather(q, b):
        for step in range(1, g_n):
            g_copy(q, b, step).wait_recv()

        def spread(n, carry):
            for side in range(2):
                tile = gr[side, q * nc + n, b * br:(b + 1) * br, :].astype(F32)
                turn[side, pl.ds(pl.multiple_of(n * s.tp, 8), br), :] = tile
            return carry
        lax.fori_loop(0, nc, spread, 0, unroll=4)
        if b == 0:
            raw[q] = jnp.zeros((nh, 4 * m, d), F32)

        def one(sub, carry):
            t0 = b * (br // 2) + sub * s.tb
            terms = []
            for side in range(2):
                both = jnp.concatenate(
                    [turn[side, pl.ds(2 * s.tb * sub + e, nc, stride=s.tp), :] for e in range(2 * s.tb)], axis=1)
                for w in range(2):
                    factor = jnp.concatenate([fac[t0 + u, q, 2 * side + w] for u in range(s.tb)], axis=1)
                    terms.append((both * factor.astype(F32)).astype(BF16))
            grads = jnp.concatenate(
                [term[half * m:(half + 1) * m] for half in range(nh) for term in terms], axis=0)
            normed = jnp.concatenate([nt_s[t0 + u] for u in range(s.tb)], axis=1)
            raw[q] += dot(grads, normed, NT).reshape(nh, 4 * m, d)
            part = dot(wt[q], grads, NN)
            for u in range(s.tb):
                piece = part[:, u * 2 * k:(u + 1) * 2 * k]
                ng[t0 + u] = ng[t0 + u] + piece if q else piece
            return carry
        lax.fori_loop(0, br // 2 // s.tb, one, 0)

    def norm_back(b):
        def one(sub, carry):
            t = b * (br // 2) + sub
            unit = unit_s[t]
            scaled = ng[t] * gain[...]
            first = jnp.mean(scaled, axis=0, keepdims=True)
            second = jnp.mean(scaled * unit, axis=0, keepdims=True)
            res = (inv_s[t] * (scaled - first - unit * second)).astype(BF16)
            for e in range(2):
                out_ref[h * rh + 2 * t + e] = dot(eye_k, res[:, e * k:(e + 1) * k], NT).astype(BF16)
            return carry
        lax.fori_loop(0, br // 2, one, 0, unroll=2)
        for step in range(1, nh):
            out_copy(b, step).start()

    for hop in range(1, nz - 1):
        for q in range(nq):
            z_hop(q, hop)
    for q in range(nq):
        z_hop(q, nz - 1)
        for step in range(1, g_n):
            lr_copy(q, step).wait_recv()

        def tri(r, carry, q=q):
            triangle(q * cq + r)
            return carry
        lax.fori_loop(0, cq, tri, 0)
        for b in range(nb):
            for step in range(1, g_n):
                g_copy(q, b, step).start()
        for side in range(2):
            for r in range(cq):
                gr[side, q * nc + me_g * cq + r] = gs[side, q * cq + r, pl.ds(row0, rh), :]
        if q:
            for b in range(nb):
                gather(q - 1, b)
            for step in range(1, nh):
                r1_copy(q - 1, step).start()
    if nq > 1:
        for q in range(nq - 1):
            r1_sum(q)
        for step in range(1, s.naz):
            r2_copy(0, step).start()
    last = nq - 1
    for b in range(nb):
        gather(last, b)
        if b == nb - 1:
            for step in range(1, nh):
                r1_copy(last, step).start()
        if b == 0 and nq > 1:
            r2_sum(0)
            for step in range(1, s.naz):
                r3_copy(0, step).start()
        if b < nb - 1:
            norm_back(b)
    r1_sum(last)
    end = len(batches) - 1
    for step in range(1, s.naz):
        r2_copy(end, step).start()
    norm_back(nb - 1)
    r2_sum(end)
    for step in range(1, s.naz):
        r3_copy(end, step).start()
    for batch in range(len(batches)):
        for step in range(1, s.naz):
            r3_copy(batch, step).wait_recv()
    found = rx3[...].reshape(s.naz * nq, s.rs, d)
    row = jnp.sum(jnp.sum(found * found, axis=0), axis=0, keepdims=True)
    sq[0] = jnp.broadcast_to(row, (8, d))
    for step in range(1, nh):
        sq_copy(step).start()
    for step in range(1, nh):
        sq_copy(step).wait()
    squares = jnp.sum(jnp.sum(sq[...], axis=0)[0:1, :], axis=1, keepdims=True)
    factor = jnp.minimum(1.0, CLIP_LIMIT * lax.rsqrt(squares + 1e-06))
    for q in range(nq):
        full = jnp.concatenate([rx3[n, q] for n in range(s.naz)], axis=0) * factor
        for w in range(4):
            wg_ref[w, q * m:(q + 1) * m, :] = full[w * m:(w + 1) * m]

    for b in range(nb):
        for step in range(1, nh):
            out_copy(b, step).wait()
    for step in range(1, nh):
        w_copy(step).wait_send()
    for batch in range(len(batches)):
        for step in range(1, s.naz):
            r2_copy(batch, step).wait_send()
            r3_copy(batch, step).wait_send()
    for q in range(nq):
        for step in range(1, nh):
            r1_copy(q, step).wait_send()
        for step in range(1, na):
            p_copy(q, step).wait_send()
        for step in range(1, g_n):
            lr_copy(q, step).wait_send()
            for b in range(nb):
                g_copy(q, b, step).wait_send()
        for hop in range(nz):
            @pl.when((z >= hop) & (z < nz - 1))
            def _(q=q, hop=hop):
                z_copy(q, z - hop, True).wait_send()

            @pl.when((z + hop < nz) & (z > 0))
            def _(q=q, hop=hop):
                z_copy(q, z + hop, False).wait_send()


def on_device(na, nz, nh, pair_rep, norm_gain, weights, residue_mask, product_grad):
    rows, cols, depth = pair_rep.shape
    ch = product_grad.shape[1]
    s = Sizes(na, nz, nh, rows, cols, depth, ch)
    vm = pl.BlockSpec(memory_space=pltpu.VMEM)
    dma = pltpu.SemaphoreType.DMA
    half = s.rh // 2
    slices = (s.naz, s.nq, s.rs, depth)
    scratch = [
        pltpu.VMEM((s.rh, cols, depth), BF16),
        pltpu.VMEM((ch, rows, cols), BF16),
        pltpu.VMEM((nz, s.cp, s.i, cols), BF16),
        pltpu.VMEM((nh, 4, ch, depth), BF16),
        pltpu.VMEM((s.nq, depth, 4 * s.nc), BF16),
        pltpu.VMEM((depth, 2 * cols), F32),
        pltpu.VMEM((half, depth, 2 * cols), F32),
        pltpu.VMEM((half, 1, 2 * cols), F32),
        pltpu.VMEM((half, depth, 2 * cols), BF16),
        pltpu.VMEM((4 * s.hid, 2 * cols), F32),
        pltpu.VMEM((half, s.nq, 4, s.nc, 2 * cols), BF16),
        pltpu.VMEM((2, max(s.br * s.sp, s.bi * s.pp), cols), F32),
        pltpu.VMEM((2, s.hid, s.rh, cols), BF16),
        pltpu.VMEM((2, s.cp, s.i, cols), BF16),
        pltpu.VMEM((2, s.cp, s.i, cols), BF16),
        pltpu.VMEM((2, s.hid, s.rh, cols), BF16),
        pltpu.VMEM((2, s.nc * s.tp, cols), F32),
        pltpu.VMEM((half, depth, 2 * cols), F32),
        pltpu.VMEM((s.nq, nh, 4 * s.m, depth), F32),
        pltpu.VMEM((s.nq, nh, 4 * s.m, depth), F32),
        pltpu.VMEM(slices, F32),
        pltpu.VMEM(slices, F32),
        pltpu.VMEM(slices, F32),
        pltpu.VMEM((nh, 8, depth), F32),
        dma(()), dma((nh,)), dma((nh,)),
        dma((s.nq, na)), dma((s.nq, na)), dma((s.nq, nz, 2)), dma((s.nq, nz)),
        dma((s.nq, s.g)), dma((s.nq, s.g)), dma((s.nq, s.nb, s.g)), dma((s.nq, s.nb, s.g)),
        dma((s.nb, nh)), dma((s.nb, nh)),
        dma((s.nq, nh)), dma((s.nq, nh)), dma((2, s.naz)), dma((2, s.naz)), dma((2, s.naz)), dma((2, s.naz)),
        dma((nh,)), dma((nh,)),
    ]
    pair_grad, found = pl.pallas_call(
        functools.partial(kernel, s),
        out_shape=(
            jax.ShapeDtypeStruct((rows, cols, depth), BF16),
            jax.ShapeDtypeStruct((4, ch, depth), F32),
        ),
        in_specs=[vm, pl.BlockSpec(memory_space=pl.ANY), vm, vm, vm, pl.BlockSpec(memory_space=pltpu.SMEM)],
        out_specs=(vm, vm),
        scratch_shapes=scratch,
        compiler_params=pltpu.CompilerParams(
            collective_id=0, has_side_effects=True, vmem_limit_bytes=VMEM_LIMIT),
    )(product_grad, pair_rep, weights.transpose(0, 2, 1), norm_gain.reshape(1, depth),
      residue_mask.reshape(nz, cols), residue_mask)
    return (pair_grad, found.transpose(0, 2, 1))


def solution(mesh):
    sizes = mesh.shape["ia"], mesh.shape["ja"], mesh.shape["col"]
    placed = (P("ia", "ja", None), P(), P(None, None, "col"), P(), P("ia", "col", "ja"))

    def step(*args):
        return on_device(*sizes, *args)

    return jax.shard_map(
        step,
        mesh=mesh,
        in_specs=placed,
        out_specs=(P("ia", "ja", None), P(None, None, "col")),
        check_vma=False,
    )
```

```python
import functools
import math

import jax
import jax.numpy as jnp
from jax import lax
from jax.experimental import pallas as pl
from jax.experimental.pallas import tpu as pltpu
from jax.sharding import PartitionSpec as P

CLIP_LIMIT = 64.0
MAX_CHUNKS = 4
ROWS_AT_ONCE = 2
VMEM_LIMIT = 66 * 1000 * 1000
MESH = pl.DeviceIdType.MESH
NT = (((1,), (1,)), ((), ()))
NN = (((1,), (0,)), ((), ()))
F32 = jnp.float32
BF16 = jnp.bfloat16


def dot(a, b, dims):
    return lax.dot_general(a, b, dims, preferred_element_type=F32)


def eye(n):
    rows = lax.broadcasted_iota(jnp.int32, (n, n), 0)
    cols = lax.broadcasted_iota(jnp.int32, (n, n), 1)
    return jnp.where(rows == cols, 1.0, 0.0).astype(BF16)


class Sizes:
    def __init__(self, na, nz, nh, rows, cols, depth, ch):
        self.na, self.nz, self.nh = na, nz, nh
        self.rb, self.k, self.d, self.ch = rows, cols, depth, ch
        self.g = na * nh
        self.naz = na * nz
        self.rh = rows // nh
        self.hid = ch * nh
        self.cp = ch // na
        self.nq = math.gcd(self.cp, MAX_CHUNKS)
        self.cq = self.cp // self.nq
        self.m = na * self.cq
        self.nc = self.g * self.cq
        self.i = na * rows
        self.br = math.gcd(self.rh, 16)
        self.nb = self.rh // self.br
        self.bi = math.gcd(self.rb, 16)
        self.sp = self.hid + 8
        self.pp = self.m + 8
        self.tp = self.br + 8
        self.tb = math.gcd(self.br // 2, ROWS_AT_ONCE)
        self.rs = 4 * self.m // self.naz
        self.q0 = self.nq - self.nq // 2 if nz > 3 else self.nq
        self.helped = max(self.nq - self.q0, 1)


def kernel(s, p_ref, x_hbm, w_ref, gain_ref, mask_ref, mask_s, out_ref, wg_ref,
           xv, pt, pg, wall, wt, gain, unit_s, inv_s, nt_s, pr, fac, relay, lrs, lrb, lrh, gs, gsh, gr, turn, ng,
           raw, rx1, mine_s, rx2, rx3, sq,
           xsem, wsend, wrecv, psend, precv, zsend, zrecv, lsend, lrecv, gsend, grecv, osend, orecv,
           r1s, r1r, r2s, r2r, r3s, r3r, qs, qr, hls, hlr, hgs, hgr):
    na, nz, nh, g_n, nq, cq, nc = s.na, s.nz, s.nh, s.g, s.nq, s.cq, s.nc
    rb, rh, k, d, ch, hid, br, nb, m = s.rb, s.rh, s.k, s.d, s.ch, s.hid, s.br, s.nb, s.m
    a, z, h = lax.axis_index("ia"), lax.axis_index("ja"), lax.axis_index("col")
    me_g = h * na + a
    me_n = a * nz + z
    row0 = a * rb + h * rh
    q0 = s.q0
    is_end = (z == 0) | (z == nz - 1)
    is_near = (z == 1) | (z == nz - 2)
    inward = jnp.where(z == 0, 1, nz - 2)
    outward = jnp.where(z == 1, 0, nz - 1)

    def plane(g):
        return (lax.rem(g, na), z, lax.div(g, na))

    def peer_g(step):
        return lax.rem(me_g + step, g_n)

    def send(src, dst, send_sem, recv_sem, device):
        return pltpu.make_async_remote_copy(
            src_ref=src, dst_ref=dst, send_sem=send_sem, recv_sem=recv_sem,
            device_id=device, device_id_type=MESH)

    barrier = pltpu.get_barrier_semaphore()
    total = s.naz * nh
    for step in range(1, total):
        to = lax.rem(me_n * nh + h + step, total)
        device = (lax.div(to, nz * nh), lax.rem(lax.div(to, nh), nz), lax.rem(to, nh))
        pl.semaphore_signal(barrier, inc=1, device_id=device, device_id_type=MESH)
    xcopy = pltpu.make_async_copy(x_hbm.at[pl.ds(h * rh, rh)], xv, xsem)
    xcopy.start()

    def p_turn(q):
        def block(ib, carry):
            slot = lax.rem(ib, 2)
            for ii in range(s.bi):
                relay[slot, ii * s.pp:ii * s.pp + m, :] = p_ref[ib * s.bi + ii, q * m:(q + 1) * m, :].astype(F32)
            for c in range(m):
                tile = relay[slot, pl.ds(c, s.bi, stride=s.pp), :]
                pt[q * m + c, pl.ds(pl.multiple_of(ib * s.bi, s.bi), s.bi), :] = tile.astype(BF16)
            return carry
        lax.fori_loop(0, rb // s.bi, block, 0)

    def p_copy(q, step):
        to = lax.rem(a + step, na)
        return send(pt.at[pl.ds(q * m + to * cq, cq)], pg.at[z, pl.ds(q * cq, cq), pl.ds(a * rb, rb)],
                    psend.at[q, step], precv.at[q, step], (to, z, h))

    def w_copy(step):
        return send(w_ref, wall.at[h], wsend.at[step], wrecv.at[step], (a, z, lax.rem(h + step, nh)))

    p_turn(0)
    pl.semaphore_wait(barrier, total - 1)
    for step in range(1, nh):
        w_copy(step).start()
    for q in range(nq):
        if q:
            p_turn(q)
        for step in range(1, na):
            p_copy(q, step).start()
    for q in range(nq):
        for r in range(cq):
            pg[z, q * cq + r, pl.ds(a * rb, rb), :] = pt[q * m + a * cq + r]

    def z_copy(q, block, up):
        ref = pg.at[block, pl.ds(q * cq, cq)]
        return send(ref, ref, zsend.at[q, block, 0 if up else 1], zrecv.at[q, block],
                    (a, z + 1 if up else z - 1, h))

    def goes_up(q):
        return z < (nz - 1 if q < q0 else nz - 2)

    def goes_down(q):
        return z > (0 if q < q0 else 1)

    def z_own(q):
        for step in range(1, na):
            p_copy(q, step).wait_recv()

        @pl.when(goes_up(q))
        def _():
            z_copy(q, z, True).start()

        @pl.when(goes_down(q))
        def _():
            z_copy(q, z, False).start()

    def z_forward(q, hop):
        @pl.when((z >= hop) & goes_up(q))
        def _():
            z_copy(q, z - hop, True).wait_recv()
            z_copy(q, z - hop, True).start()

        @pl.when((z + hop < nz) & goes_down(q))
        def _():
            z_copy(q, z + hop, False).wait_recv()
            z_copy(q, z + hop, False).start()

    def z_rest(q):
        for hop in range(1, nz):
            here = True if q < q0 else jnp.logical_not(is_end)

            @pl.when((z >= hop) & jnp.logical_not(goes_up(q)) & here)
            def _(hop=hop):
                z_copy(q, z - hop, True).wait_recv()

            @pl.when((z + hop < nz) & jnp.logical_not(goes_down(q)) & here)
            def _(hop=hop):
                z_copy(q, z + hop, False).wait_recv()

    eye_d = eye(d)
    column = jnp.transpose(jnp.broadcast_to(gain_ref[...], (k, d)))
    gain[...] = jnp.concatenate([column, column], axis=1)
    wall[h] = w_ref[...]
    for step in range(1, nh):
        w_copy(step).wait_recv()
    for q in range(nq):
        rows = [wall[half, w, q * m:(q + 1) * m, :] for half in range(nh) for w in range(4)]
        wt[q] = dot(eye_d, jnp.concatenate(rows, axis=0), NT).astype(BF16)

    xcopy.wait()
    col_valid = mask_ref[pl.ds(z, 1), :].astype(F32)

    def rows_step(t, sub):
        x2 = xv[pl.ds(2 * t, 2)].reshape(2 * k, d)
        xt = dot(eye_d, x2, NT)
        centred = xt - jnp.mean(xt, axis=0, keepdims=True)
        inv = lax.rsqrt(jnp.mean(centred * centred, axis=0, keepdims=True) + 1e-05)
        unit = centred * inv
        normed = (unit * gain[...]).astype(BF16)
        unit_s[t] = unit
        inv_s[t] = inv
        nt_s[t] = normed
        for half in range(nh):
            pr[half * 4 * ch:(half + 1) * 4 * ch, :] = dot(wall[half].reshape(4 * ch, d), normed, NN)
        valid = jnp.concatenate(
            [col_valid * mask_s[row0 + 2 * t + e].astype(F32) for e in range(2)], axis=1)
        for q in range(nq):
            for side in range(2):
                def part(w):
                    at = [half * 4 * ch + w * ch + q * m for half in range(nh)]
                    return jnp.concatenate([pr[x:x + m, :] for x in at], axis=0)
                lin = part(2 * side)
                gate = jax.nn.sigmoid(part(2 * side + 1))
                first = valid * gate
                value = first * lin
                fac[t, q, 2 * side] = first.astype(BF16)
                fac[t, q, 2 * side + 1] = (value * (1.0 - gate)).astype(BF16)
                for e in range(2):
                    at = pl.multiple_of((2 * sub + e) * s.sp, 8) + q * nc
                    relay[side, pl.ds(at, nc), :] = value[:, e * k:(e + 1) * k]

    for b in range(nb):
        def one(sub, carry, b=b):
            rows_step(b * (br // 2) + sub, sub)
            return carry
        lax.fori_loop(0, br // 2, one, 0)

        def flush(c, carry, b=b):
            for side in range(2):
                tile = relay[side, pl.ds(c, br, stride=s.sp), :]
                lrs[side, c, b * br:(b + 1) * br, :] = tile.astype(BF16)
            return carry
        lax.fori_loop(0, hid, flush, 0, unroll=4)
        if b < q0:
            z_own(b)
    for q in range(nb, q0):
        z_own(q)

    @pl.when(is_end)
    def _():
        for q in range(q0, nq):
            z_own(q)

    def lr_copy(q, step):
        return send(lrs.at[:, pl.ds(q * nc + peer_g(step) * cq, cq)],
                    lrb.at[:, pl.ds(q * cq, cq), pl.ds(row0, rh)],
                    lsend.at[q, step], lrecv.at[q, step], plane(peer_g(step)))

    for q in [*range(q0, nq), *range(q0)]:
        for step in range(1, g_n):
            lr_copy(q, step).start()
    for q in range(nq):
        for side in range(2):
            for r in range(cq):
                lrb[side, q * cq + r, pl.ds(row0, rh), :] = lrs[side, q * nc + me_g * cq + r]

    eye_k = eye(k)

    def triangle(c, lr, at, to):
        panel = jnp.concatenate([pg[b, c] for b in range(nz)], axis=1)
        left, right = lr[0, at], lr[1, at]
        to[0, at] = dot(panel, right, NN).astype(BF16).reshape(g_n, rh, k)
        left_t = dot(eye_k, left, NT).astype(BF16)
        back_t = dot(left_t, panel, NN).astype(BF16)
        back = [dot(eye_k, back_t[:, b * k:(b + 1) * k], NT).astype(BF16) for b in range(nz)]
        to[1, at] = jnp.concatenate(back, axis=0).reshape(g_n, rh, k)

    def triangles(q, lr, to, base):
        def one(r, carry):
            triangle(q * cq + r, lr, (q - base) * cq + r, to)
            return carry
        lax.fori_loop(0, cq, one, 0)

    def in_copy(q, z_to):
        return send(lrb.at[:, pl.ds(q * cq, cq)], lrh.at[:, pl.ds((q - q0) * cq, cq)],
                    hls.at[q - q0], hlr.at[q - q0], (a, z_to, h))

    def back_copy(q, b, z_to):
        return send(gsh.at[:, pl.ds((q - q0) * cq, cq), :, pl.ds(b * br, br)],
                    gs.at[:, pl.ds(q * cq, cq), :, pl.ds(b * br, br)],
                    hgs.at[q - q0, b], hgr.at[q - q0, b], (a, z_to, h))

    def g_copy(q, b, step):
        g = peer_g(step)
        place = lax.rem(g, na) * nh + lax.div(g, na)
        return send(gs.at[:, pl.ds(q * cq, cq), place, pl.ds(b * br, br)],
                    gr.at[:, pl.ds(q * nc + me_g * cq, cq), pl.ds(b * br, br)],
                    gsend.at[q, b, step], grecv.at[q, b, step], plane(g))

    def out_copy(b, step):
        ref = out_ref.at[pl.ds(h * rh + b * br, br)]
        return send(ref, ref, osend.at[b, step], orecv.at[b, step], (a, z, lax.rem(h + step, nh)))

    def r1_copy(q, step):
        to = lax.rem(h + step, nh)
        return send(raw.at[q, to], rx1.at[q, step], r1s.at[q, step], r1r.at[q, step], (a, z, to))

    def r1_sum(q):
        mine = raw[q, h]
        for step in range(1, nh):
            r1_copy(q, step).wait_recv()
            mine = mine + rx1[q, step]
        for n in range(s.naz):
            mine_s[n, q] = mine[n * s.rs:(n + 1) * s.rs]

    def peer_n(step):
        return lax.rem(me_n + step, s.naz)

    def at_n(n):
        return (lax.div(n, nz), lax.rem(n, nz), h)

    batches = [(0, nq - 1), (nq - 1, nq)] if nq > 1 else [(0, nq)]

    def r2_copy(batch, step):
        lo, hi = batches[batch]
        n = peer_n(step)
        return send(mine_s.at[n, lo:hi], rx2.at[step, lo:hi], r2s.at[batch, step], r2r.at[batch, step], at_n(n))

    def r2_sum(batch):
        lo, hi = batches[batch]
        mine = mine_s[me_n, lo:hi]
        for step in range(1, s.naz):
            r2_copy(batch, step).wait_recv()
            mine = mine + rx2[step, lo:hi]
        rx3[me_n, lo:hi] = mine

    def r3_copy(batch, step):
        lo, hi = batches[batch]
        ref = rx3.at[me_n, lo:hi]
        return send(ref, ref, r3s.at[batch, step], r3r.at[batch, step], at_n(peer_n(step)))

    def sq_copy(step):
        return send(sq.at[0], sq.at[step], qs.at[step], qr.at[step], (a, z, lax.rem(h + step, nh)))

    def gather(q, b):
        for step in range(1, g_n):
            g_copy(q, b, step).wait_recv()

        def spread(n, carry):
            for side in range(2):
                tile = gr[side, q * nc + n, b * br:(b + 1) * br, :].astype(F32)
                turn[side, pl.ds(pl.multiple_of(n * s.tp, 8), br), :] = tile
            return carry
        lax.fori_loop(0, nc, spread, 0, unroll=4)
        if b == 0:
            raw[q] = jnp.zeros((nh, 4 * m, d), F32)

        def one(sub, carry):
            t0 = b * (br // 2) + sub * s.tb
            terms = []
            for side in range(2):
                both = jnp.concatenate(
                    [turn[side, pl.ds(2 * s.tb * sub + e, nc, stride=s.tp), :] for e in range(2 * s.tb)], axis=1)
                for w in range(2):
                    factor = jnp.concatenate([fac[t0 + u, q, 2 * side + w] for u in range(s.tb)], axis=1)
                    terms.append((both * factor.astype(F32)).astype(BF16))
            grads = jnp.concatenate(
                [term[half * m:(half + 1) * m] for half in range(nh) for term in terms], axis=0)
            normed = jnp.concatenate([nt_s[t0 + u] for u in range(s.tb)], axis=1)
            raw[q] += dot(grads, normed, NT).reshape(nh, 4 * m, d)
            part = dot(wt[q], grads, NN)
            for u in range(s.tb):
                piece = part[:, u * 2 * k:(u + 1) * 2 * k]
                ng[t0 + u] = ng[t0 + u] + piece if q else piece
            return carry
        lax.fori_loop(0, br // 2 // s.tb, one, 0)

    def norm_back(b):
        def one(sub, carry):
            t = b * (br // 2) + sub
            unit = unit_s[t]
            scaled = ng[t] * gain[...]
            first = jnp.mean(scaled, axis=0, keepdims=True)
            second = jnp.mean(scaled * unit, axis=0, keepdims=True)
            res = (inv_s[t] * (scaled - first - unit * second)).astype(BF16)
            for e in range(2):
                out_ref[h * rh + 2 * t + e] = dot(eye_k, res[:, e * k:(e + 1) * k], NT).astype(BF16)
            return carry
        lax.fori_loop(0, br // 2, one, 0, unroll=2)
        for step in range(1, nh):
            out_copy(b, step).start()

    def lr_wait(q):
        for step in range(1, g_n):
            lr_copy(q, step).wait_recv()

    def g_send(q, b):
        for step in range(1, g_n):
            g_copy(q, b, step).start()
        for side in range(2):
            for r in range(cq):
                gr[side, q * nc + me_g * cq + r, b * br:(b + 1) * br, :] = gs[
                    side, q * cq + r, a * nh + h, b * br:(b + 1) * br, :]

    def make(q):
        if q < q0:
            z_rest(q)
            lr_wait(q)
            triangles(q, lrb, gs, 0)
            return

        @pl.when(is_near)
        def _():
            z_rest(q)
            in_copy(q, outward).wait_recv()
            triangles(q, lrh, gsh, q0)
            for b in range(nb):
                back_copy(q, b, outward).start()
            lr_wait(q)
            triangles(q, lrb, gs, 0)

        @pl.when(jnp.logical_not(is_near | is_end))
        def _():
            z_rest(q)
            lr_wait(q)
            triangles(q, lrb, gs, 0)

    def came_back(q, b):
        if q >= q0:
            @pl.when(is_end)
            def _():
                back_copy(q, b, outward).wait_recv()

    for hop in range(1, nz - 1):
        for q in range(q0):
            z_forward(q, hop)
        if hop == 1 and q0 < nq:
            @pl.when(jnp.logical_not(is_end))
            def _():
                z_own(q0)
    for q in range(q0, nq):
        for hop in range(1, nz - 1):
            z_forward(q, hop)
        if q + 1 < nq:
            @pl.when(jnp.logical_not(is_end))
            def _(q=q):
                z_own(q + 1)

    @pl.when(is_end)
    def _():
        for q in range(q0, nq):
            lr_wait(q)
            in_copy(q, inward).start()

    last = nq - 1
    late = 0
    before = []
    for q in range(nq):
        make(q)
        for b in range(nb):
            came_back(q, b)
            g_send(q, b)
            for _ in range(2):
                if before:
                    gather(*before.pop(0))
            if q == last and not before and b > 1:
                at = b - 2 - late
                gather(last, at)
                norm_back(at)
            elif q == last and b > 1:
                late += 1
        for task in before:
            gather(*task)
        before = [(q, b) for b in range(nb)]
        if q:
            for step in range(1, nh):
                r1_copy(q - 1, step).start()
    if nq > 1:
        for q in range(nq - 1):
            r1_sum(q)
        for step in range(1, s.naz):
            r2_copy(0, step).start()
    for b in range(max(nb - 2 - late, 0), nb):
        gather(last, b)
        if b == nb - 1:
            for step in range(1, nh):
                r1_copy(last, step).start()
            if nq > 1:
                r2_sum(0)
                for step in range(1, s.naz):
                    r3_copy(0, step).start()
        else:
            norm_back(b)
    r1_sum(last)
    end = len(batches) - 1
    for step in range(1, s.naz):
        r2_copy(end, step).start()
    norm_back(nb - 1)
    r2_sum(end)
    for step in range(1, s.naz):
        r3_copy(end, step).start()
    for batch in range(len(batches)):
        for step in range(1, s.naz):
            r3_copy(batch, step).wait_recv()
    found = rx3[...].reshape(s.naz * nq, s.rs, d)
    row = jnp.sum(jnp.sum(found * found, axis=0), axis=0, keepdims=True)
    sq[0] = jnp.broadcast_to(row, (8, d))
    for step in range(1, nh):
        sq_copy(step).start()
    for step in range(1, nh):
        sq_copy(step).wait()
    squares = jnp.sum(jnp.sum(sq[...], axis=0)[0:1, :], axis=1, keepdims=True)
    factor = jnp.minimum(1.0, CLIP_LIMIT * lax.rsqrt(squares + 1e-06))
    for q in range(nq):
        full = jnp.concatenate([rx3[n, q] for n in range(s.naz)], axis=0) * factor
        for w in range(4):
            wg_ref[w, q * m:(q + 1) * m, :] = full[w * m:(w + 1) * m]

    for b in range(nb):
        for step in range(1, nh):
            out_copy(b, step).wait()
    for step in range(1, nh):
        w_copy(step).wait_send()
    for batch in range(len(batches)):
        for step in range(1, s.naz):
            r2_copy(batch, step).wait_send()
            r3_copy(batch, step).wait_send()
    for q in range(nq):
        for step in range(1, nh):
            r1_copy(q, step).wait_send()
        for step in range(1, na):
            p_copy(q, step).wait_send()
        for step in range(1, g_n):
            lr_copy(q, step).wait_send()
            for b in range(nb):
                g_copy(q, b, step).wait_send()
        for hop in range(nz):
            @pl.when((z >= hop) & goes_up(q))
            def _(q=q, hop=hop):
                z_copy(q, z - hop, True).wait_send()

            @pl.when((z + hop < nz) & goes_down(q))
            def _(q=q, hop=hop):
                z_copy(q, z + hop, False).wait_send()
        if q >= q0:
            @pl.when(is_end)
            def _(q=q):
                in_copy(q, inward).wait_send()

            @pl.when(is_near)
            def _(q=q):
                for b in range(nb):
                    back_copy(q, b, outward).wait_send()


def on_device(na, nz, nh, pair_rep, norm_gain, weights, residue_mask, product_grad):
    rows, cols, depth = pair_rep.shape
    ch = product_grad.shape[1]
    s = Sizes(na, nz, nh, rows, cols, depth, ch)
    vm = pl.BlockSpec(memory_space=pltpu.VMEM)
    dma = pltpu.SemaphoreType.DMA
    half = s.rh // 2
    slices = (s.naz, s.nq, s.rs, depth)
    scratch = [
        pltpu.VMEM((s.rh, cols, depth), BF16),
        pltpu.VMEM((ch, rows, cols), BF16),
        pltpu.VMEM((nz, s.cp, s.i, cols), BF16),
        pltpu.VMEM((nh, 4, ch, depth), BF16),
        pltpu.VMEM((s.nq, depth, 4 * s.nc), BF16),
        pltpu.VMEM((depth, 2 * cols), F32),
        pltpu.VMEM((half, depth, 2 * cols), F32),
        pltpu.VMEM((half, 1, 2 * cols), F32),
        pltpu.VMEM((half, depth, 2 * cols), BF16),
        pltpu.VMEM((4 * s.hid, 2 * cols), F32),
        pltpu.VMEM((half, s.nq, 4, s.nc, 2 * cols), BF16),
        pltpu.VMEM((2, max(s.br * s.sp, s.bi * s.pp), cols), F32),
        pltpu.VMEM((2, s.hid, s.rh, cols), BF16),
        pltpu.VMEM((2, s.cp, s.i, cols), BF16),
        pltpu.VMEM((2, s.helped * s.cq, s.i, cols), BF16),
        pltpu.VMEM((2, s.cp, s.g, s.rh, cols), BF16),
        pltpu.VMEM((2, s.helped * s.cq, s.g, s.rh, cols), BF16),
        pltpu.VMEM((2, s.hid, s.rh, cols), BF16),
        pltpu.VMEM((2, s.nc * s.tp, cols), F32),
        pltpu.VMEM((half, depth, 2 * cols), F32),
        pltpu.VMEM((s.nq, nh, 4 * s.m, depth), F32),
        pltpu.VMEM((s.nq, nh, 4 * s.m, depth), F32),
        pltpu.VMEM(slices, F32),
        pltpu.VMEM(slices, F32),
        pltpu.VMEM(slices, F32),
        pltpu.VMEM((nh, 8, depth), F32),
        dma(()), dma((nh,)), dma((nh,)),
        dma((s.nq, na)), dma((s.nq, na)), dma((s.nq, nz, 2)), dma((s.nq, nz)),
        dma((s.nq, s.g)), dma((s.nq, s.g)), dma((s.nq, s.nb, s.g)), dma((s.nq, s.nb, s.g)),
        dma((s.nb, nh)), dma((s.nb, nh)),
        dma((s.nq, nh)), dma((s.nq, nh)), dma((2, s.naz)), dma((2, s.naz)), dma((2, s.naz)), dma((2, s.naz)),
        dma((nh,)), dma((nh,)),
        dma((s.helped,)), dma((s.helped,)), dma((s.helped, s.nb)), dma((s.helped, s.nb)),
    ]
    pair_grad, found = pl.pallas_call(
        functools.partial(kernel, s),
        out_shape=(
            jax.ShapeDtypeStruct((rows, cols, depth), BF16),
            jax.ShapeDtypeStruct((4, ch, depth), F32),
        ),
        in_specs=[vm, pl.BlockSpec(memory_space=pl.ANY), vm, vm, vm, pl.BlockSpec(memory_space=pltpu.SMEM)],
        out_specs=(vm, vm),
        scratch_shapes=scratch,
        compiler_params=pltpu.CompilerParams(
            collective_id=0, has_side_effects=True, vmem_limit_bytes=VMEM_LIMIT),
    )(product_grad, pair_rep, weights.transpose(0, 2, 1), norm_gain.reshape(1, depth),
      residue_mask.reshape(nz, cols), residue_mask)
    return (pair_grad, found.transpose(0, 2, 1))


def solution(mesh):
    sizes = mesh.shape["ia"], mesh.shape["ja"], mesh.shape["col"]
    placed = (P("ia", "ja", None), P(), P(None, None, "col"), P(), P("ia", "col", "ja"))

    def step(*args):
        return on_device(*sizes, *args)

    return jax.shard_map(
        step,
        mesh=mesh,
        in_specs=placed,
        out_specs=(P("ia", "ja", None), P(None, None, "col")),
        check_vma=False,
    )
```

```python
import functools
import math

import jax
import jax.numpy as jnp
from jax import lax
from jax.experimental import pallas as pl
from jax.experimental.pallas import tpu as pltpu
from jax.sharding import PartitionSpec as P

CLIP_LIMIT = 64.0
MAX_CHUNKS = 4
ROWS_AT_ONCE = 2
VMEM_LIMIT = 66 * 1000 * 1000
MESH = pl.DeviceIdType.MESH
NT = (((1,), (1,)), ((), ()))
NN = (((1,), (0,)), ((), ()))
F32 = jnp.float32
BF16 = jnp.bfloat16


def dot(a, b, dims):
    return lax.dot_general(a, b, dims, preferred_element_type=F32)


def eye(n):
    rows = lax.broadcasted_iota(jnp.int32, (n, n), 0)
    cols = lax.broadcasted_iota(jnp.int32, (n, n), 1)
    return jnp.where(rows == cols, 1.0, 0.0).astype(BF16)


class Sizes:
    def __init__(self, na, nz, nh, rows, cols, depth, ch):
        self.na, self.nz, self.nh = na, nz, nh
        self.rb, self.k, self.d, self.ch = rows, cols, depth, ch
        self.g = na * nh
        self.naz = na * nz
        self.rh = rows // nh
        self.hid = ch * nh
        self.cp = ch // na
        self.nq = math.gcd(self.cp, MAX_CHUNKS)
        self.cq = self.cp // self.nq
        self.m = na * self.cq
        self.nc = self.g * self.cq
        self.i = na * rows
        self.br = math.gcd(self.rh, 16)
        self.nb = self.rh // self.br
        self.bi = math.gcd(self.rb, 16)
        self.sp = self.hid + 8
        self.pp = self.m + 8
        self.tp = self.br + 8
        self.tb = math.gcd(self.br // 2, ROWS_AT_ONCE)
        self.no = math.gcd(max(4 * self.m // 8, 1), self.naz)
        self.rs = 4 * self.m // self.no
        self.per = max(self.no // na, 1)
        self.stride = na * self.per // self.no
        self.base = (nz - self.per) // 2
        self.q0 = self.nq - self.nq // 2 if nz > 3 else self.nq
        self.helped = max(self.nq - self.q0, 1)


def kernel(s, p_ref, x_hbm, w_ref, gain_ref, mask_ref, mask_s, out_hbm, wg_ref,
           xv, pt, pg, wall, wt, gain, unit_s, inv_s, nt_s, pr, fac, relay, lrs, lrb, lrh, gs, gsh, gr, turn, ng,
           outv, raw, rx1, mine_s, rx2, rx3, sq,
           xsem, wsend, wrecv, psend, precv, zsend, zrecv, lsend, lrecv, gsend, grecv, osend, orecv,
           r1s, r1r, r2s, r2r, r3s, r3r, qs, qr, keep, hls, hlr, hgs, hgr):
    na, nz, nh, g_n, nq, cq, nc = s.na, s.nz, s.nh, s.g, s.nq, s.cq, s.nc
    rb, rh, k, d, ch, hid, br, nb, m = s.rb, s.rh, s.k, s.d, s.ch, s.hid, s.br, s.nb, s.m
    a, z, h = lax.axis_index("ia"), lax.axis_index("ja"), lax.axis_index("col")
    me_g = h * na + a
    me_n = a * nz + z
    row0 = a * rb + h * rh
    q0 = s.q0
    is_end = (z == 0) | (z == nz - 1)
    is_near = (z == 1) | (z == nz - 2)
    inward = jnp.where(z == 0, 1, nz - 2)
    outward = jnp.where(z == 1, 0, nz - 1)

    def plane(g):
        return (lax.rem(g, na), z, lax.div(g, na))

    def peer_g(step):
        return lax.rem(me_g + step, g_n)

    def send(src, dst, send_sem, recv_sem, device):
        return pltpu.make_async_remote_copy(
            src_ref=src, dst_ref=dst, send_sem=send_sem, recv_sem=recv_sem,
            device_id=device, device_id_type=MESH)

    barrier = pltpu.get_barrier_semaphore()
    total = s.naz * nh
    for step in range(1, total):
        to = lax.rem(me_n * nh + h + step, total)
        device = (lax.div(to, nz * nh), lax.rem(lax.div(to, nh), nz), lax.rem(to, nh))
        pl.semaphore_signal(barrier, inc=1, device_id=device, device_id_type=MESH)
    xcopy = pltpu.make_async_copy(x_hbm.at[pl.ds(h * rh, rh)], xv, xsem)
    xcopy.start()

    def p_turn(q):
        def block(ib, carry):
            slot = lax.rem(ib, 2)
            for ii in range(s.bi):
                relay[slot, ii * s.pp:ii * s.pp + m, :] = p_ref[ib * s.bi + ii, q * m:(q + 1) * m, :].astype(F32)
            for c in range(m):
                tile = relay[slot, pl.ds(c, s.bi, stride=s.pp), :]
                pt[q * m + c, pl.ds(pl.multiple_of(ib * s.bi, s.bi), s.bi), :] = tile.astype(BF16)
            return carry
        lax.fori_loop(0, rb // s.bi, block, 0)

    def pieces(q):
        return [(q * cq + r, 1) for r in range(cq)] if q == 0 else [(q * cq, cq)]

    def p_copy(piece, step):
        c, n = piece
        to = lax.rem(a + step, na)
        return send(pt.at[pl.ds((c // cq) * m + to * cq + c % cq, n)], pg.at[z, pl.ds(c, n), pl.ds(a * rb, rb)],
                    psend.at[c, step], precv.at[c, step], (to, z, h))

    def w_copy(step):
        return send(w_ref, wall.at[h], wsend.at[step], wrecv.at[step], (a, z, lax.rem(h + step, nh)))

    p_turn(0)
    pl.semaphore_wait(barrier, total - 1)
    for step in range(1, nh):
        w_copy(step).start()
    for q in range(nq):
        if q:
            p_turn(q)
        for piece in pieces(q):
            for step in range(1, na):
                p_copy(piece, step).start()
    for q in range(nq):
        for r in range(cq):
            pg[z, q * cq + r, pl.ds(a * rb, rb), :] = pt[q * m + a * cq + r]

    def z_copy(piece, block, up):
        c, n = piece
        ref = pg.at[block, pl.ds(c, n)]
        return send(ref, ref, zsend.at[c, block, 0 if up else 1], zrecv.at[c, block],
                    (a, z + 1 if up else z - 1, h))

    def goes_up(q):
        return z < (nz - 1 if q < q0 else nz - 2)

    def goes_down(q):
        return z > (0 if q < q0 else 1)

    def z_own(q):
        for piece in pieces(q):
            for step in range(1, na):
                p_copy(piece, step).wait_recv()

            @pl.when(goes_up(q))
            def _(piece=piece):
                z_copy(piece, z, True).start()

            @pl.when(goes_down(q))
            def _(piece=piece):
                z_copy(piece, z, False).start()

    def z_forward(q, hop):
        @pl.when((z >= hop) & goes_up(q))
        def _():
            for piece in pieces(q):
                z_copy(piece, z - hop, True).wait_recv()
                z_copy(piece, z - hop, True).start()

        @pl.when((z + hop < nz) & goes_down(q))
        def _():
            for piece in pieces(q):
                z_copy(piece, z + hop, False).wait_recv()
                z_copy(piece, z + hop, False).start()

    def z_rest(q):
        for hop in range(1, nz):
            here = True if q < q0 else jnp.logical_not(is_end)

            @pl.when((z >= hop) & jnp.logical_not(goes_up(q)) & here)
            def _(hop=hop):
                for piece in pieces(q):
                    z_copy(piece, z - hop, True).wait_recv()

            @pl.when((z + hop < nz) & jnp.logical_not(goes_down(q)) & here)
            def _(hop=hop):
                for piece in pieces(q):
                    z_copy(piece, z + hop, False).wait_recv()

    eye_d = eye(d)
    column = jnp.transpose(jnp.broadcast_to(gain_ref[...], (k, d)))
    gain[...] = jnp.concatenate([column, column], axis=1)
    wall[h] = w_ref[...]
    for step in range(1, nh):
        w_copy(step).wait_recv()
    for q in range(nq):
        rows = [wall[half, w, q * m:(q + 1) * m, :] for half in range(nh) for w in range(4)]
        wt[q] = dot(eye_d, jnp.concatenate(rows, axis=0), NT).astype(BF16)

    xcopy.wait()
    col_valid = mask_ref[pl.ds(z, 1), :].astype(F32)

    def rows_step(t, sub):
        x2 = xv[pl.ds(2 * t, 2)].reshape(2 * k, d)
        xt = dot(eye_d, x2, NT)
        centred = xt - jnp.mean(xt, axis=0, keepdims=True)
        inv = lax.rsqrt(jnp.mean(centred * centred, axis=0, keepdims=True) + 1e-05)
        unit = centred * inv
        normed = (unit * gain[...]).astype(BF16)
        unit_s[t] = unit
        inv_s[t] = inv
        nt_s[t] = normed
        for half in range(nh):
            pr[half * 4 * ch:(half + 1) * 4 * ch, :] = dot(wall[half].reshape(4 * ch, d), normed, NN)
        valid = jnp.concatenate(
            [col_valid * mask_s[row0 + 2 * t + e].astype(F32) for e in range(2)], axis=1)
        for q in range(nq):
            for side in range(2):
                def part(w):
                    at = [half * 4 * ch + w * ch + q * m for half in range(nh)]
                    return jnp.concatenate([pr[x:x + m, :] for x in at], axis=0)
                lin = part(2 * side)
                gate = jax.nn.sigmoid(part(2 * side + 1))
                first = valid * gate
                value = first * lin
                fac[t, q, 2 * side] = first.astype(BF16)
                fac[t, q, 2 * side + 1] = (value * (1.0 - gate)).astype(BF16)
                for e in range(2):
                    at = pl.multiple_of((2 * sub + e) * s.sp, 8) + q * nc
                    relay[side, pl.ds(at, nc), :] = value[:, e * k:(e + 1) * k]

    for b in range(nb):
        def one(sub, carry, b=b):
            rows_step(b * (br // 2) + sub, sub)
            return carry
        lax.fori_loop(0, br // 2, one, 0)

        def flush(c, carry, b=b):
            for side in range(2):
                tile = relay[side, pl.ds(c, br, stride=s.sp), :]
                lrs[side, c, b * br:(b + 1) * br, :] = tile.astype(BF16)
            return carry
        lax.fori_loop(0, hid, flush, 0, unroll=4)
        if b < q0:
            z_own(b)
    for q in range(nb, q0):
        z_own(q)

    @pl.when(is_end)
    def _():
        for q in range(q0, nq):
            z_own(q)

    def lr_copy(q, step):
        return send(lrs.at[:, pl.ds(q * nc + peer_g(step) * cq, cq)],
                    lrb.at[:, pl.ds(q * cq, cq), pl.ds(row0, rh)],
                    lsend.at[q, step], lrecv.at[q, step], plane(peer_g(step)))

    for q in [*range(q0, nq), *range(q0)]:
        for step in range(1, g_n):
            lr_copy(q, step).start()
    for q in range(nq):
        for side in range(2):
            for r in range(cq):
                lrb[side, q * cq + r, pl.ds(row0, rh), :] = lrs[side, q * nc + me_g * cq + r]

    eye_k = eye(k)

    def triangle(c, lr, at, to):
        panel = jnp.concatenate([pg[b, c] for b in range(nz)], axis=1)
        left, right = lr[0, at], lr[1, at]
        to[0, at] = dot(panel, right, NN).astype(BF16).reshape(g_n, rh, k)
        left_t = dot(eye_k, left, NT).astype(BF16)
        back_t = dot(left_t, panel, NN).astype(BF16)
        back = [dot(eye_k, back_t[:, b * k:(b + 1) * k], NT).astype(BF16) for b in range(nz)]
        to[1, at] = jnp.concatenate(back, axis=0).reshape(g_n, rh, k)

    def triangles(q, lr, to, base):
        def one(r, carry):
            triangle(q * cq + r, lr, (q - base) * cq + r, to)
            return carry
        lax.fori_loop(0, cq, one, 0)

    def in_copy(q, z_to):
        return send(lrb.at[:, pl.ds(q * cq, cq)], lrh.at[:, pl.ds((q - q0) * cq, cq)],
                    hls.at[q - q0], hlr.at[q - q0], (a, z_to, h))

    def back_copy(q, b, z_to):
        return send(gsh.at[:, pl.ds((q - q0) * cq, cq), :, pl.ds(b * br, br)],
                    gs.at[:, pl.ds(q * cq, cq), :, pl.ds(b * br, br)],
                    hgs.at[q - q0, b], hgr.at[q - q0, b], (a, z_to, h))

    def g_copy(q, b, step):
        g = peer_g(step)
        place = lax.rem(g, na) * nh + lax.div(g, na)
        return send(gs.at[:, pl.ds(q * cq, cq), place, pl.ds(b * br, br)],
                    gr.at[:, pl.ds(q * nc + me_g * cq, cq), pl.ds(b * br, br)],
                    gsend.at[q, b, step], grecv.at[q, b, step], plane(g))

    def out_copy(b, step):
        return send(outv.at[pl.ds(b * br, br)], out_hbm.at[pl.ds(h * rh + b * br, br)],
                    osend.at[b, step], orecv.at[b, step], (a, z, lax.rem(h + step, nh)))

    def keep_copy(b):
        return pltpu.make_async_copy(
            outv.at[pl.ds(b * br, br)], out_hbm.at[pl.ds(h * rh + b * br, br)], keep.at[b])

    def r1_copy(q, step):
        to = lax.rem(h + step, nh)
        return send(raw.at[q, to], rx1.at[q, step], r1s.at[q, step], r1r.at[q, step], (a, z, to))

    def r1_sum(q):
        mine = raw[q, h]
        for step in range(1, nh):
            r1_copy(q, step).wait_recv()
            mine = mine + rx1[q, step]
        for o in range(s.no):
            mine_s[o, q] = mine[o * s.rs:(o + 1) * s.rs]

    def at_n(n):
        return (lax.div(n, nz), lax.rem(n, nz), h)

    def owner(o):
        return (o // s.per * s.stride, s.base + o % s.per)

    def other(o):
        return (a != owner(o)[0]) | (z != owner(o)[1])

    me_o = lax.div(a, s.stride) * s.per + z - s.base
    is_owner = (lax.rem(a, s.stride) == 0) & (z >= s.base) & (z < s.base + s.per)
    batches = [(0, nq - 1), (nq - 1, nq)] if nq > 1 else [(0, nq)]

    def r2_copy(batch, o, n):
        lo, hi = batches[batch]
        return send(mine_s.at[o, lo:hi], rx2.at[n, lo:hi],
                    r2s.at[batch, o], r2r.at[batch, n], (*owner(o), h))

    def r2_start(batch):
        for o in range(s.no):
            @pl.when(other(o))
            def _(o=o):
                r2_copy(batch, o, me_n).start()

    def r3_copy(batch, o, step):
        lo, hi = batches[batch]
        ref = rx3.at[o, lo:hi]
        return send(ref, ref, r3s.at[batch, step], r3r.at[batch, o], at_n(lax.rem(me_n + step, s.naz)))

    def r2_sum(batch):
        lo, hi = batches[batch]

        @pl.when(is_owner)
        def _():
            mine = mine_s[me_o, lo:hi]
            for step in range(1, s.naz):
                n = lax.rem(me_n + step, s.naz)
                r2_copy(batch, 0, n).wait_recv()
                mine = mine + rx2[n, lo:hi]
            rx3[me_o, lo:hi] = mine
            for step in range(1, s.naz):
                r3_copy(batch, me_o, step).start()

    def r3_wait(batch):
        for o in range(s.no):
            @pl.when(other(o))
            def _(o=o):
                r3_copy(batch, o, 1).wait_recv()

    def sq_copy(step):
        return send(sq.at[0], sq.at[step], qs.at[step], qr.at[step], (a, z, lax.rem(h + step, nh)))

    def gather(q, b):
        for step in range(1, g_n):
            g_copy(q, b, step).wait_recv()

        def spread(n, carry):
            for side in range(2):
                tile = gr[side, q * nc + n, b * br:(b + 1) * br, :].astype(F32)
                turn[side, pl.ds(pl.multiple_of(n * s.tp, 8), br), :] = tile
            return carry
        lax.fori_loop(0, nc, spread, 0, unroll=4)
        if b == 0:
            raw[q] = jnp.zeros((nh, 4 * m, d), F32)

        def one(sub, carry):
            t0 = b * (br // 2) + sub * s.tb
            terms = []
            for side in range(2):
                both = jnp.concatenate(
                    [turn[side, pl.ds(2 * s.tb * sub + e, nc, stride=s.tp), :] for e in range(2 * s.tb)], axis=1)
                for w in range(2):
                    factor = jnp.concatenate([fac[t0 + u, q, 2 * side + w] for u in range(s.tb)], axis=1)
                    terms.append((both * factor.astype(F32)).astype(BF16))
            grads = jnp.concatenate(
                [term[half * m:(half + 1) * m] for half in range(nh) for term in terms], axis=0)
            normed = jnp.concatenate([nt_s[t0 + u] for u in range(s.tb)], axis=1)
            raw[q] += dot(grads, normed, NT).reshape(nh, 4 * m, d)
            part = dot(wt[q], grads, NN)
            for u in range(s.tb):
                piece = part[:, u * 2 * k:(u + 1) * 2 * k]
                ng[t0 + u] = ng[t0 + u] + piece if q else piece
            return carry
        lax.fori_loop(0, br // 2 // s.tb, one, 0)

    def norm_back(b):
        def one(sub, carry):
            t = b * (br // 2) + sub
            unit = unit_s[t]
            scaled = ng[t] * gain[...]
            first = jnp.mean(scaled, axis=0, keepdims=True)
            second = jnp.mean(scaled * unit, axis=0, keepdims=True)
            res = (inv_s[t] * (scaled - first - unit * second)).astype(BF16)
            for e in range(2):
                outv[2 * t + e] = dot(eye_k, res[:, e * k:(e + 1) * k], NT).astype(BF16)
            return carry
        lax.fori_loop(0, br // 2, one, 0, unroll=2)
        keep_copy(b).start()
        for step in range(1, nh):
            out_copy(b, step).start()

    def lr_wait(q):
        for step in range(1, g_n):
            lr_copy(q, step).wait_recv()

    def g_send(q, b):
        for step in range(1, g_n):
            g_copy(q, b, step).start()
        for side in range(2):
            for r in range(cq):
                gr[side, q * nc + me_g * cq + r, b * br:(b + 1) * br, :] = gs[
                    side, q * cq + r, a * nh + h, b * br:(b + 1) * br, :]

    def make(q):
        if q < q0:
            z_rest(q)
            lr_wait(q)
            triangles(q, lrb, gs, 0)
            return

        @pl.when(is_near)
        def _():
            z_rest(q)
            in_copy(q, outward).wait_recv()
            triangles(q, lrh, gsh, q0)
            for b in range(nb):
                back_copy(q, b, outward).start()
            lr_wait(q)
            triangles(q, lrb, gs, 0)

        @pl.when(jnp.logical_not(is_near | is_end))
        def _():
            z_rest(q)
            lr_wait(q)
            triangles(q, lrb, gs, 0)

    def came_back(q, b):
        if q >= q0:
            @pl.when(is_end)
            def _():
                back_copy(q, b, outward).wait_recv()

    for hop in range(1, nz - 1):
        for q in range(q0):
            z_forward(q, hop)
        if hop == 1 and q0 < nq:
            @pl.when(jnp.logical_not(is_end))
            def _():
                z_own(q0)
    for q in range(q0, nq):
        for hop in range(1, nz - 1):
            z_forward(q, hop)
        if q + 1 < nq:
            @pl.when(jnp.logical_not(is_end))
            def _(q=q):
                z_own(q + 1)

    @pl.when(is_end)
    def _():
        for q in range(q0, nq):
            lr_wait(q)
            in_copy(q, inward).start()

    last = nq - 1
    queue = []

    def run(count):
        for _ in range(min(count, len(queue))):
            q, b = queue.pop(0)
            gather(q, b)
            if b == nb - 1:
                for step in range(1, nh):
                    r1_copy(q, step).start()

    for q in range(nq):
        make(q)
        if q > 1:
            queue += [(q - 2, b) for b in range(nb)]
        if q == last:
            queue += [(last - 1, b) for b in range(nb)] if q else []
            run(max(len(queue) - 2 * nb, 0))
        for b in range(nb):
            run(1 if q < last else 0)
            came_back(q, b)
            g_send(q, b)
            if q == last:
                run(3 if b < nb - 1 else 0)
                if b > 0:
                    queue.append((last, b - 1))
    queue.append((last, nb - 1))
    run(max(len(queue) - 1, 0))
    if nq > 1:
        for q in range(nq - 1):
            r1_sum(q)
        r2_start(0)
    run(1)
    norm_back(0)
    r1_sum(last)
    r2_start(len(batches) - 1)
    waiting = list(range(len(batches)))
    for b in range(1, nb):
        norm_back(b)
        if len(waiting) > 1:
            r2_sum(waiting.pop(0))
    for batch in waiting:
        r2_sum(batch)
    for batch in range(len(batches)):
        r3_wait(batch)
    found = rx3[...].reshape(s.no * nq, s.rs, d)
    sq[0] = jnp.sum(found * found, axis=0)
    for step in range(1, nh):
        sq_copy(step).start()
    for step in range(1, nh):
        sq_copy(step).wait()
    squares = jnp.sum(jnp.sum(jnp.sum(sq[...], axis=0), axis=0, keepdims=True), axis=1, keepdims=True)
    factor = jnp.minimum(1.0, CLIP_LIMIT * lax.rsqrt(squares + 1e-06))
    for q in range(nq):
        for o in range(s.no):
            w, at = o * s.rs // m, q * m + o * s.rs % m
            wg_ref[w, at:at + s.rs, :] = rx3[o, q] * factor

    for b in range(nb):
        keep_copy(b).wait()
        for step in range(1, nh):
            out_copy(b, step).wait()
    for step in range(1, nh):
        w_copy(step).wait_send()
    for batch in range(len(batches)):
        for o in range(s.no):
            @pl.when(other(o))
            def _(batch=batch, o=o):
                r2_copy(batch, o, me_n).wait_send()

        @pl.when(is_owner)
        def _(batch=batch):
            for step in range(1, s.naz):
                r3_copy(batch, me_o, step).wait_send()
    for q in range(nq):
        for step in range(1, nh):
            r1_copy(q, step).wait_send()
        for piece in pieces(q):
            for step in range(1, na):
                p_copy(piece, step).wait_send()
        for step in range(1, g_n):
            lr_copy(q, step).wait_send()
            for b in range(nb):
                g_copy(q, b, step).wait_send()
        for hop in range(nz):
            @pl.when((z >= hop) & goes_up(q))
            def _(q=q, hop=hop):
                for piece in pieces(q):
                    z_copy(piece, z - hop, True).wait_send()

            @pl.when((z + hop < nz) & goes_down(q))
            def _(q=q, hop=hop):
                for piece in pieces(q):
                    z_copy(piece, z + hop, False).wait_send()
        if q >= q0:
            @pl.when(is_end)
            def _(q=q):
                in_copy(q, inward).wait_send()

            @pl.when(is_near)
            def _(q=q):
                for b in range(nb):
                    back_copy(q, b, outward).wait_send()


def on_device(na, nz, nh, pair_rep, norm_gain, weights, residue_mask, product_grad):
    rows, cols, depth = pair_rep.shape
    ch = product_grad.shape[1]
    s = Sizes(na, nz, nh, rows, cols, depth, ch)
    vm = pl.BlockSpec(memory_space=pltpu.VMEM)
    dma = pltpu.SemaphoreType.DMA
    half = s.rh // 2
    scratch = [
        pltpu.VMEM((s.rh, cols, depth), BF16),
        pltpu.VMEM((ch, rows, cols), BF16),
        pltpu.VMEM((nz, s.cp, s.i, cols), BF16),
        pltpu.VMEM((nh, 4, ch, depth), BF16),
        pltpu.VMEM((s.nq, depth, 4 * s.nc), BF16),
        pltpu.VMEM((depth, 2 * cols), F32),
        pltpu.VMEM((half, depth, 2 * cols), F32),
        pltpu.VMEM((half, 1, 2 * cols), F32),
        pltpu.VMEM((half, depth, 2 * cols), BF16),
        pltpu.VMEM((4 * s.hid, 2 * cols), F32),
        pltpu.VMEM((half, s.nq, 4, s.nc, 2 * cols), BF16),
        pltpu.VMEM((2, max(s.br * s.sp, s.bi * s.pp), cols), F32),
        pltpu.VMEM((2, s.hid, s.rh, cols), BF16),
        pltpu.VMEM((2, s.cp, s.i, cols), BF16),
        pltpu.VMEM((2, s.helped * s.cq, s.i, cols), BF16),
        pltpu.VMEM((2, s.cp, s.g, s.rh, cols), BF16),
        pltpu.VMEM((2, s.helped * s.cq, s.g, s.rh, cols), BF16),
        pltpu.VMEM((2, s.hid, s.rh, cols), BF16),
        pltpu.VMEM((2, s.nc * s.tp, cols), F32),
        pltpu.VMEM((half, depth, 2 * cols), F32),
        pltpu.VMEM((s.rh, cols, depth), BF16),
        pltpu.VMEM((s.nq, nh, 4 * s.m, depth), F32),
        pltpu.VMEM((s.nq, nh, 4 * s.m, depth), F32),
        pltpu.VMEM((s.no, s.nq, s.rs, depth), F32),
        pltpu.VMEM((s.naz, s.nq, s.rs, depth), F32),
        pltpu.VMEM((s.no, s.nq, s.rs, depth), F32),
        pltpu.VMEM((nh, s.rs, depth), F32),
        dma(()), dma((nh,)), dma((nh,)),
        dma((s.cp, na)), dma((s.cp, na)), dma((s.cp, nz, 2)), dma((s.cp, nz)),
        dma((s.nq, s.g)), dma((s.nq, s.g)), dma((s.nq, s.nb, s.g)), dma((s.nq, s.nb, s.g)),
        dma((s.nb, nh)), dma((s.nb, nh)),
        dma((s.nq, nh)), dma((s.nq, nh)), dma((2, s.no)), dma((2, s.naz)), dma((2, s.naz)), dma((2, s.no)),
        dma((nh,)), dma((nh,)), dma((s.nb,)),
        dma((s.helped,)), dma((s.helped,)), dma((s.helped, s.nb)), dma((s.helped, s.nb)),
    ]
    pair_grad, found = pl.pallas_call(
        functools.partial(kernel, s),
        out_shape=(
            jax.ShapeDtypeStruct((rows, cols, depth), BF16),
            jax.ShapeDtypeStruct((4, ch, depth), F32),
        ),
        in_specs=[vm, pl.BlockSpec(memory_space=pl.ANY), vm, vm, vm, pl.BlockSpec(memory_space=pltpu.SMEM)],
        out_specs=(pl.BlockSpec(memory_space=pl.ANY), vm),
        scratch_shapes=scratch,
        compiler_params=pltpu.CompilerParams(
            collective_id=0, has_side_effects=True, vmem_limit_bytes=VMEM_LIMIT),
    )(product_grad, pair_rep, weights.transpose(0, 2, 1), norm_gain.reshape(1, depth),
      residue_mask.reshape(nz, cols), residue_mask)
    return (pair_grad, found.transpose(0, 2, 1))


def solution(mesh):
    sizes = mesh.shape["ia"], mesh.shape["ja"], mesh.shape["col"]
    placed = (P("ia", "ja", None), P(), P(None, None, "col"), P(), P("ia", "col", "ja"))

    def step(*args):
        return on_device(*sizes, *args)

    return jax.shard_map(
        step,
        mesh=mesh,
        in_specs=placed,
        out_specs=(P("ia", "ja", None), P(None, None, "col")),
        check_vma=False,
    )
```

```python
import functools
import math

import jax
import jax.numpy as jnp
from jax import lax
from jax.experimental import pallas as pl
from jax.experimental.pallas import tpu as pltpu
from jax.sharding import PartitionSpec as P

CLIP_LIMIT = 64.0
MAX_CHUNKS = 4
ROWS_AT_ONCE = 2
VMEM_LIMIT = 66 * 1000 * 1000
MESH = pl.DeviceIdType.MESH
NT = (((1,), (1,)), ((), ()))
NN = (((1,), (0,)), ((), ()))
F32 = jnp.float32
BF16 = jnp.bfloat16


def dot(a, b, dims):
    return lax.dot_general(a, b, dims, preferred_element_type=F32)


def eye(n):
    rows = lax.broadcasted_iota(jnp.int32, (n, n), 0)
    cols = lax.broadcasted_iota(jnp.int32, (n, n), 1)
    return jnp.where(rows == cols, 1.0, 0.0).astype(BF16)


class Sizes:
    def __init__(self, na, nz, nh, rows, cols, depth, ch):
        self.na, self.nz, self.nh = na, nz, nh
        self.rb, self.k, self.d, self.ch = rows, cols, depth, ch
        self.g = na * nh
        self.naz = na * nz
        self.rh = rows // nh
        self.hid = ch * nh
        self.cp = ch // na
        self.nq = math.gcd(self.cp, MAX_CHUNKS)
        self.cq = self.cp // self.nq
        self.m = na * self.cq
        self.nc = self.g * self.cq
        self.i = na * rows
        self.br = math.gcd(self.rh, 16)
        self.nb = self.rh // self.br
        self.bi = math.gcd(self.rb, 16)
        self.sp = self.hid + 8
        self.pp = self.m + 8
        self.tp = self.br + 8
        self.tb = math.gcd(self.br // 2, ROWS_AT_ONCE)
        self.no = math.gcd(max(4 * self.m // 8, 1), self.naz)
        self.rs = 4 * self.m // self.no
        self.per = max(self.no // na, 1)
        self.stride = na * self.per // self.no
        self.base = (nz - self.per) // 2
        self.q0 = self.nq - self.nq // 2 if nz > 3 else self.nq
        self.helped = max(self.nq - self.q0, 1)


def kernel(s, p_ref, x_hbm, w_ref, gain_ref, mask_ref, mask_s, out_hbm, wg_ref, sq_ref,
           xv, pt, pg, wall, wt, gain, unit_s, inv_s, nt_s, pr, fac, relay, lrs, lrb, lrh, gs, gsh, gr, turn, ng,
           outv, raw, rx1, mine_s, rx2, rx3, sq,
           xsem, wsend, wrecv, psend, precv, zsend, zrecv, lsend, lrecv, gsend, grecv, osend, orecv,
           r1s, r1r, r2s, r2r, r3s, r3r, qs, qr, keep, hls, hlr, hgs, hgr):
    na, nz, nh, g_n, nq, cq, nc = s.na, s.nz, s.nh, s.g, s.nq, s.cq, s.nc
    rb, rh, k, d, ch, hid, br, nb, m = s.rb, s.rh, s.k, s.d, s.ch, s.hid, s.br, s.nb, s.m
    a, z, h = lax.axis_index("ia"), lax.axis_index("ja"), lax.axis_index("col")
    me_g = h * na + a
    me_n = a * nz + z
    row0 = a * rb + h * rh
    q0 = s.q0
    is_end = (z == 0) | (z == nz - 1)
    is_near = (z == 1) | (z == nz - 2)
    inward = jnp.where(z == 0, 1, nz - 2)
    outward = jnp.where(z == 1, 0, nz - 1)

    def plane(g):
        return (lax.rem(g, na), z, lax.div(g, na))

    def peer_g(step):
        return lax.rem(me_g + step, g_n)

    def sent(ref, sem):
        pltpu.make_async_copy(ref, ref, sem).wait()

    def send(src, dst, send_sem, recv_sem, device):
        return pltpu.make_async_remote_copy(
            src_ref=src, dst_ref=dst, send_sem=send_sem, recv_sem=recv_sem,
            device_id=device, device_id_type=MESH)

    barrier = pltpu.get_barrier_semaphore()
    total = s.naz * nh
    for step in range(1, total):
        to = lax.rem(me_n * nh + h + step, total)
        device = (lax.div(to, nz * nh), lax.rem(lax.div(to, nh), nz), lax.rem(to, nh))
        pl.semaphore_signal(barrier, inc=1, device_id=device, device_id_type=MESH)
    xcopy = pltpu.make_async_copy(x_hbm.at[pl.ds(h * rh, rh)], xv, xsem)
    xcopy.start()

    def p_turn(q):
        def block(ib, carry):
            slot = lax.rem(ib, 2)
            for ii in range(s.bi):
                relay[slot, ii * s.pp:ii * s.pp + m, :] = p_ref[ib * s.bi + ii, q * m:(q + 1) * m, :].astype(F32)
            for c in range(m):
                tile = relay[slot, pl.ds(c, s.bi, stride=s.pp), :]
                pt[q * m + c, pl.ds(pl.multiple_of(ib * s.bi, s.bi), s.bi), :] = tile.astype(BF16)
            return carry
        lax.fori_loop(0, rb // s.bi, block, 0)

    def pieces(q):
        return [(q * cq + r, 1) for r in range(cq)] if q == 0 else [(q * cq, cq)]

    def p_copy(piece, step):
        c, n = piece
        to = lax.rem(a + step, na)
        return send(pt.at[pl.ds((c // cq) * m + to * cq + c % cq, n)], pg.at[z, pl.ds(c, n), pl.ds(a * rb, rb)],
                    psend, precv.at[c, step], (to, z, h))

    def w_copy(step):
        return send(w_ref, wall.at[h], wsend.at[step], wrecv.at[step], (a, z, lax.rem(h + step, nh)))

    p_turn(0)
    pl.semaphore_wait(barrier, total - 1)
    for step in range(1, nh):
        w_copy(step).start()
    for q in range(nq):
        if q:
            p_turn(q)
        for piece in pieces(q):
            for step in range(1, na):
                p_copy(piece, step).start()
    for q in range(nq):
        for r in range(cq):
            pg[z, q * cq + r, pl.ds(a * rb, rb), :] = pt[q * m + a * cq + r]

    def z_copy(piece, block, up):
        c, n = piece
        ref = pg.at[block, pl.ds(c, n)]
        return send(ref, ref, zsend.at[c // cq, 0 if up else 1], zrecv.at[c, block],
                    (a, z + 1 if up else z - 1, h))

    def goes_up(q):
        return z < (nz - 1 if q < q0 else nz - 2)

    def goes_down(q):
        return z > (0 if q < q0 else 1)

    def z_own(q, some=None):
        for piece in some or pieces(q):
            for step in range(1, na):
                p_copy(piece, step).wait_recv()

            @pl.when(goes_up(q))
            def _(piece=piece):
                z_copy(piece, z, True).start()

            @pl.when(goes_down(q))
            def _(piece=piece):
                z_copy(piece, z, False).start()

    def z_forward(q, hop):
        @pl.when((z >= hop) & goes_up(q))
        def _():
            for piece in pieces(q):
                z_copy(piece, z - hop, True).wait_recv()
                z_copy(piece, z - hop, True).start()

        @pl.when((z + hop < nz) & goes_down(q))
        def _():
            for piece in pieces(q):
                z_copy(piece, z + hop, False).wait_recv()
                z_copy(piece, z + hop, False).start()

    def z_rest(q):
        for hop in range(1, nz):
            here = True if q < q0 else jnp.logical_not(is_end)

            @pl.when((z >= hop) & jnp.logical_not(goes_up(q)) & here)
            def _(hop=hop):
                for piece in pieces(q):
                    z_copy(piece, z - hop, True).wait_recv()

            @pl.when((z + hop < nz) & jnp.logical_not(goes_down(q)) & here)
            def _(hop=hop):
                for piece in pieces(q):
                    z_copy(piece, z + hop, False).wait_recv()

    eye_d = eye(d)
    column = jnp.transpose(jnp.broadcast_to(gain_ref[...], (k, d)))
    gain[...] = jnp.concatenate([column, column], axis=1)
    wall[h] = w_ref[...]
    for step in range(1, nh):
        w_copy(step).wait_recv()
    for q in range(nq):
        rows = [wall[half, w, q * m:(q + 1) * m, :] for half in range(nh) for w in range(4)]
        wt[q] = dot(eye_d, jnp.concatenate(rows, axis=0), NT).astype(BF16)

    xcopy.wait()
    col_valid = mask_ref[pl.ds(z, 1), :].astype(F32)

    def rows_step(t, sub):
        x2 = xv[pl.ds(2 * t, 2)].reshape(2 * k, d)
        xt = dot(eye_d, x2, NT)
        centred = xt - jnp.mean(xt, axis=0, keepdims=True)
        inv = lax.rsqrt(jnp.mean(centred * centred, axis=0, keepdims=True) + 1e-05)
        unit = centred * inv
        normed = (unit * gain[...]).astype(BF16)
        unit_s[t] = unit
        inv_s[t] = inv
        nt_s[t] = normed
        for half in range(nh):
            pr[half * 4 * ch:(half + 1) * 4 * ch, :] = dot(wall[half].reshape(4 * ch, d), normed, NN)
        valid = jnp.concatenate(
            [col_valid * mask_s[row0 + 2 * t + e].astype(F32) for e in range(2)], axis=1)
        for q in range(nq):
            for side in range(2):
                def part(w):
                    at = [half * 4 * ch + w * ch + q * m for half in range(nh)]
                    return jnp.concatenate([pr[x:x + m, :] for x in at], axis=0)
                lin = part(2 * side)
                gate = jax.nn.sigmoid(part(2 * side + 1))
                first = valid * gate
                value = first * lin
                fac[t, q, 2 * side] = first.astype(BF16)
                fac[t, q, 2 * side + 1] = (value * (1.0 - gate)).astype(BF16)
                for e in range(2):
                    at = pl.multiple_of((2 * sub + e) * s.sp, 8) + q * nc
                    relay[side, pl.ds(at, nc), :] = value[:, e * k:(e + 1) * k]

    for b in range(nb):
        def one(sub, carry, b=b):
            rows_step(b * (br // 2) + sub, sub)
            return carry
        parts = pieces(0) if b == 0 else [None]
        each = br // 2 // len(parts)
        if each * len(parts) * 2 == br:
            for n, piece in enumerate(parts):
                lax.fori_loop(n * each, (n + 1) * each, one, 0)
                if piece:
                    z_own(0, [piece])
        else:
            lax.fori_loop(0, br // 2, one, 0)
            if b == 0:
                z_own(0)

        def flush(c, carry, b=b):
            for side in range(2):
                tile = relay[side, pl.ds(c, br, stride=s.sp), :]
                lrs[side, c, b * br:(b + 1) * br, :] = tile.astype(BF16)
            return carry
        lax.fori_loop(0, hid, flush, 0, unroll=4)
        if 0 < b < q0:
            z_own(b)
    for q in range(nb, q0):
        z_own(q)

    @pl.when(is_end)
    def _():
        for q in range(q0, nq):
            z_own(q)

    def lr_copy(q, step):
        return send(lrs.at[:, pl.ds(q * nc + peer_g(step) * cq, cq)],
                    lrb.at[:, pl.ds(q * cq, cq), pl.ds(row0, rh)],
                    lsend, lrecv.at[q, step], plane(peer_g(step)))

    for q in [*range(q0, nq), *range(q0)]:
        for step in range(1, g_n):
            lr_copy(q, step).start()
    for q in range(nq):
        for side in range(2):
            for r in range(cq):
                lrb[side, q * cq + r, pl.ds(row0, rh), :] = lrs[side, q * nc + me_g * cq + r]

    eye_k = eye(k)

    def triangle(c, lr, at, to):
        panel = jnp.concatenate([pg[b, c] for b in range(nz)], axis=1)
        left, right = lr[0, at], lr[1, at]
        to[0, at] = dot(panel, right, NN).astype(BF16).reshape(g_n, rh, k)
        left_t = dot(eye_k, left, NT).astype(BF16)
        back_t = dot(left_t, panel, NN).astype(BF16)
        back = [dot(eye_k, back_t[:, b * k:(b + 1) * k], NT).astype(BF16) for b in range(nz)]
        to[1, at] = jnp.concatenate(back, axis=0).reshape(g_n, rh, k)

    def triangles(q, lr, to, base):
        def one(r, carry):
            triangle(q * cq + r, lr, (q - base) * cq + r, to)
            return carry
        lax.fori_loop(0, cq, one, 0)

    def in_copy(q, z_to):
        return send(lrb.at[:, pl.ds(q * cq, cq)], lrh.at[:, pl.ds((q - q0) * cq, cq)],
                    hls, hlr.at[q - q0], (a, z_to, h))

    def back_copy(q, b, z_to):
        return send(gsh.at[:, pl.ds((q - q0) * cq, cq), :, pl.ds(b * br, br)],
                    gs.at[:, pl.ds(q * cq, cq), :, pl.ds(b * br, br)],
                    hgs, hgr.at[q - q0, b], (a, z_to, h))

    def g_copy(q, b, step):
        g = peer_g(step)
        place = lax.rem(g, na) * nh + lax.div(g, na)
        return send(gs.at[:, pl.ds(q * cq, cq), place, pl.ds(b * br, br)],
                    gr.at[:, pl.ds(q * nc + me_g * cq, cq), pl.ds(b * br, br)],
                    gsend.at[q], grecv.at[q, b, step], plane(g))

    def out_copy(b, step):
        return send(outv.at[pl.ds(b * br, br)], out_hbm.at[pl.ds(h * rh + b * br, br)],
                    osend.at[b, step], orecv.at[b, step], (a, z, lax.rem(h + step, nh)))

    def keep_copy(b):
        return pltpu.make_async_copy(
            outv.at[pl.ds(b * br, br)], out_hbm.at[pl.ds(h * rh + b * br, br)], keep.at[b])

    def r1_copy(q, step):
        to = lax.rem(h + step, nh)
        return send(raw.at[q, to], rx1.at[q, step], r1s.at[q, step], r1r.at[q, step], (a, z, to))

    def r1_sum(q):
        mine = raw[q, h]
        for step in range(1, nh):
            r1_copy(q, step).wait_recv()
            mine = mine + rx1[q, step]
        for o in range(s.no):
            mine_s[o, q] = mine[o * s.rs:(o + 1) * s.rs]

    def at_n(n):
        return (lax.div(n, nz), lax.rem(n, nz), h)

    def owner(o):
        return (o // s.per * s.stride, s.base + o % s.per)

    def other(o):
        return (a != owner(o)[0]) | (z != owner(o)[1])

    me_o = lax.div(a, s.stride) * s.per + z - s.base
    is_owner = (lax.rem(a, s.stride) == 0) & (z >= s.base) & (z < s.base + s.per)
    batches = [(0, nq - 1), (nq - 1, nq)] if nq > 1 else [(0, nq)]

    def r2_copy(batch, o, n):
        lo, hi = batches[batch]
        return send(mine_s.at[o, lo:hi], rx2.at[n, lo:hi],
                    r2s.at[batch], r2r.at[batch, n], (*owner(o), h))

    def r2_start(batch):
        for o in range(s.no):
            @pl.when(other(o))
            def _(o=o):
                r2_copy(batch, o, me_n).start()

    def r3_copy(batch, o, step):
        lo, hi = batches[batch]
        ref = rx3.at[o, lo:hi]
        return send(ref, ref, r3s.at[batch], r3r.at[batch, o], at_n(lax.rem(me_n + step, s.naz)))

    def r2_sum(batch):
        lo, hi = batches[batch]

        @pl.when(is_owner)
        def _():
            mine = mine_s[me_o, lo:hi]
            for step in range(1, s.naz):
                n = lax.rem(me_n + step, s.naz)
                r2_copy(batch, 0, n).wait_recv()
                mine = mine + rx2[n, lo:hi]
            rx3[me_o, lo:hi] = mine
            for step in range(1, s.naz):
                r3_copy(batch, me_o, step).start()

    def r3_wait(batch):
        for o in range(s.no):
            @pl.when(other(o))
            def _(o=o):
                r3_copy(batch, o, 1).wait_recv()

    def sq_copy(step):
        return send(sq.at[0], sq.at[step], qs.at[step], qr.at[step], (a, z, lax.rem(h + step, nh)))

    def gather(q, b):
        for step in range(1, g_n):
            g_copy(q, b, step).wait_recv()

        def spread(n, carry):
            for side in range(2):
                tile = gr[side, q * nc + n, b * br:(b + 1) * br, :].astype(F32)
                turn[side, pl.ds(pl.multiple_of(n * s.tp, 8), br), :] = tile
            return carry
        lax.fori_loop(0, nc, spread, 0, unroll=4)
        if b == 0:
            raw[q] = jnp.zeros((nh, 4 * m, d), F32)

        def one(sub, carry):
            t0 = b * (br // 2) + sub * s.tb
            terms = []
            for side in range(2):
                both = jnp.concatenate(
                    [turn[side, pl.ds(2 * s.tb * sub + e, nc, stride=s.tp), :] for e in range(2 * s.tb)], axis=1)
                for w in range(2):
                    factor = jnp.concatenate([fac[t0 + u, q, 2 * side + w] for u in range(s.tb)], axis=1)
                    terms.append((both * factor.astype(F32)).astype(BF16))
            grads = jnp.concatenate(
                [term[half * m:(half + 1) * m] for half in range(nh) for term in terms], axis=0)
            normed = jnp.concatenate([nt_s[t0 + u] for u in range(s.tb)], axis=1)
            raw[q] += dot(grads, normed, NT).reshape(nh, 4 * m, d)
            part = dot(wt[q], grads, NN)
            for u in range(s.tb):
                piece = part[:, u * 2 * k:(u + 1) * 2 * k]
                ng[t0 + u] = ng[t0 + u] + piece if q else piece
            return carry
        lax.fori_loop(0, br // 2 // s.tb, one, 0)

    def norm_back(b):
        def one(sub, carry):
            t = b * (br // 2) + sub
            unit = unit_s[t]
            scaled = ng[t] * gain[...]
            first = jnp.mean(scaled, axis=0, keepdims=True)
            second = jnp.mean(scaled * unit, axis=0, keepdims=True)
            res = (inv_s[t] * (scaled - first - unit * second)).astype(BF16)
            for e in range(2):
                outv[2 * t + e] = dot(eye_k, res[:, e * k:(e + 1) * k], NT).astype(BF16)
            return carry
        lax.fori_loop(0, br // 2, one, 0, unroll=2)
        keep_copy(b).start()
        for step in range(1, nh):
            out_copy(b, step).start()

    def lr_wait(q):
        for step in range(1, g_n):
            lr_copy(q, step).wait_recv()

    def g_send(q, b):
        for step in range(1, g_n):
            g_copy(q, b, step).start()
        for side in range(2):
            for r in range(cq):
                gr[side, q * nc + me_g * cq + r, b * br:(b + 1) * br, :] = gs[
                    side, q * cq + r, a * nh + h, b * br:(b + 1) * br, :]

    def make(q):
        if q < q0:
            z_rest(q)
            lr_wait(q)
            triangles(q, lrb, gs, 0)
            return

        @pl.when(is_near)
        def _():
            z_rest(q)
            in_copy(q, outward).wait_recv()
            triangles(q, lrh, gsh, q0)
            for b in range(nb):
                back_copy(q, b, outward).start()
            lr_wait(q)
            triangles(q, lrb, gs, 0)

        @pl.when(jnp.logical_not(is_near | is_end))
        def _():
            z_rest(q)
            lr_wait(q)
            triangles(q, lrb, gs, 0)

    def came_back(q, b):
        if q >= q0:
            @pl.when(is_end)
            def _():
                back_copy(q, b, outward).wait_recv()

    for hop in range(1, nz - 1):
        for q in range(q0):
            z_forward(q, hop)
        if hop == 1 and q0 < nq:
            @pl.when(jnp.logical_not(is_end))
            def _():
                z_own(q0)
    for q in range(q0, nq):
        for hop in range(1, nz - 1):
            z_forward(q, hop)
        if q + 1 < nq:
            @pl.when(jnp.logical_not(is_end))
            def _(q=q):
                z_own(q + 1)

    @pl.when(is_end)
    def _():
        for q in range(q0, nq):
            lr_wait(q)
            in_copy(q, inward).start()

    def drain():
        for step in range(1, nh):
            w_copy(step).wait_send()
        sent(pt.at[pl.ds(0, (na - 1) * s.cp)], psend)
        sent(lrs.at[:, pl.ds(0, (g_n - 1) * nq * cq)], lsend)
        for q in range(nq):
            for step in range(1, nh):
                r1_copy(q, step).wait_send()
            sent(gs.at[:, pl.ds(q * cq, cq), pl.ds(0, g_n - 1)], gsend.at[q])
            for count in range(1, nz):
                @pl.when((z + 1 == count) & goes_up(q))
                def _(q=q, count=count):
                    sent(pg.at[pl.ds(0, count), pl.ds(q * cq, cq)], zsend.at[q, 0])

                @pl.when((nz - z == count) & goes_down(q))
                def _(q=q, count=count):
                    sent(pg.at[pl.ds(0, count), pl.ds(q * cq, cq)], zsend.at[q, 1])
        if q0 < nq:
            @pl.when(is_end)
            def _():
                sent(lrh, hls)

            @pl.when(is_near)
            def _():
                sent(gsh, hgs)

    last = nq - 1
    queue = []

    def run(count):
        for _ in range(min(count, len(queue))):
            q, b = queue.pop(0)
            gather(q, b)
            if b == nb - 1:
                for step in range(1, nh):
                    r1_copy(q, step).start()

    for q in range(nq):
        make(q)
        if q > 1:
            queue += [(q - 2, b) for b in range(nb)]
        if q == last:
            queue += [(last - 1, b) for b in range(nb)] if q else []
            run(max(len(queue) - 2 * nb, 0))
        for b in range(nb):
            run(1 if q < last else 0)
            came_back(q, b)
            g_send(q, b)
            if q == last:
                run(3 if b < nb - 1 else 0)
                if b > 0:
                    queue.append((last, b - 1))
    queue.append((last, nb - 1))
    run(max(len(queue) - 1, 0))
    if nq > 1:
        for q in range(nq - 1):
            r1_sum(q)
        r2_start(0)
    run(1)
    norm_back(0)
    r1_sum(last)
    r2_start(len(batches) - 1)
    waiting = list(range(len(batches)))
    for b in range(1, nb):
        norm_back(b)
        if len(waiting) > 1:
            r2_sum(waiting.pop(0))
    for batch in waiting:
        r2_sum(batch)
    drain()
    for batch in range(len(batches)):
        r3_wait(batch)
    found = rx3[...].reshape(s.no * nq, s.rs, d)
    sq[0] = jnp.sum(found * found, axis=0)
    for step in range(1, nh):
        sq_copy(step).start()
    for step in range(1, nh):
        sq_copy(step).wait()
    sq_ref[...] = jnp.sum(sq[...], axis=0)
    for q in range(nq):
        for o in range(s.no):
            w, at = o * s.rs // m, q * m + o * s.rs % m
            wg_ref[w, at:at + s.rs, :] = rx3[o, q]

    for b in range(nb):
        keep_copy(b).wait()
        for step in range(1, nh):
            out_copy(b, step).wait()
    for batch, (lo, hi) in enumerate(batches):
        @pl.when(is_owner)
        def _(batch=batch, lo=lo, hi=hi):
            sent(mine_s.at[pl.ds(0, s.no - 1), lo:hi], r2s.at[batch])
            sent(rx2.at[pl.ds(0, s.naz - 1), lo:hi], r3s.at[batch])

        @pl.when(jnp.logical_not(is_owner))
        def _(batch=batch, lo=lo, hi=hi):
            sent(mine_s.at[:, lo:hi], r2s.at[batch])


def finish(blocks, from_hbm, found_ref, sq_ref, out_hbm, wg_ref, held, sem_in, sem_out):
    size = held.shape[0] // blocks

    def came(b):
        at = pl.ds(b * size, size)
        return pltpu.make_async_copy(from_hbm.at[at], held.at[at], sem_in.at[b])

    def leaves(b):
        at = pl.ds(b * size, size)
        return pltpu.make_async_copy(held.at[at], out_hbm.at[at], sem_out.at[b])

    for b in range(blocks):
        came(b).start()
    squares = jnp.sum(jnp.sum(sq_ref[...], axis=0, keepdims=True), axis=1, keepdims=True)
    factor = jnp.minimum(1.0, CLIP_LIMIT * lax.rsqrt(squares + 1e-06))
    wg_ref[...] = found_ref[...] * factor
    for b in range(blocks):
        came(b).wait()
        leaves(b).start()
    for b in range(blocks):
        leaves(b).wait()


def on_device(na, nz, nh, pair_rep, norm_gain, weights, residue_mask, product_grad):
    rows, cols, depth = pair_rep.shape
    ch = product_grad.shape[1]
    s = Sizes(na, nz, nh, rows, cols, depth, ch)
    vm = pl.BlockSpec(memory_space=pltpu.VMEM)
    dma = pltpu.SemaphoreType.DMA
    half = s.rh // 2
    scratch = [
        pltpu.VMEM((s.rh, cols, depth), BF16),
        pltpu.VMEM((ch, rows, cols), BF16),
        pltpu.VMEM((nz, s.cp, s.i, cols), BF16),
        pltpu.VMEM((nh, 4, ch, depth), BF16),
        pltpu.VMEM((s.nq, depth, 4 * s.nc), BF16),
        pltpu.VMEM((depth, 2 * cols), F32),
        pltpu.VMEM((half, depth, 2 * cols), F32),
        pltpu.VMEM((half, 1, 2 * cols), F32),
        pltpu.VMEM((half, depth, 2 * cols), BF16),
        pltpu.VMEM((4 * s.hid, 2 * cols), F32),
        pltpu.VMEM((half, s.nq, 4, s.nc, 2 * cols), BF16),
        pltpu.VMEM((2, max(s.br * s.sp, s.bi * s.pp), cols), F32),
        pltpu.VMEM((2, s.hid, s.rh, cols), BF16),
        pltpu.VMEM((2, s.cp, s.i, cols), BF16),
        pltpu.VMEM((2, s.helped * s.cq, s.i, cols), BF16),
        pltpu.VMEM((2, s.cp, s.g, s.rh, cols), BF16),
        pltpu.VMEM((2, s.helped * s.cq, s.g, s.rh, cols), BF16),
        pltpu.VMEM((2, s.hid, s.rh, cols), BF16),
        pltpu.VMEM((2, s.nc * s.tp, cols), F32),
        pltpu.VMEM((half, depth, 2 * cols), F32),
        pltpu.VMEM((s.rh, cols, depth), BF16),
        pltpu.VMEM((s.nq, nh, 4 * s.m, depth), F32),
        pltpu.VMEM((s.nq, nh, 4 * s.m, depth), F32),
        pltpu.VMEM((s.no, s.nq, s.rs, depth), F32),
        pltpu.VMEM((s.naz, s.nq, s.rs, depth), F32),
        pltpu.VMEM((s.no, s.nq, s.rs, depth), F32),
        pltpu.VMEM((nh, s.rs, depth), F32),
        dma(()), dma((nh,)), dma((nh,)),
        dma(()), dma((s.cp, na)), dma((s.nq, 2)), dma((s.cp, nz)),
        dma(()), dma((s.nq, s.g)), dma((s.nq,)), dma((s.nq, s.nb, s.g)),
        dma((s.nb, nh)), dma((s.nb, nh)),
        dma((s.nq, nh)), dma((s.nq, nh)), dma((2,)), dma((2, s.naz)), dma((2,)), dma((2, s.no)),
        dma((nh,)), dma((nh,)), dma((s.nb,)),
        dma(()), dma((s.helped,)), dma(()), dma((s.helped, s.nb)),
    ]
    grad, found, squares = pl.pallas_call(
        functools.partial(kernel, s),
        out_shape=(
            jax.ShapeDtypeStruct((rows, cols, depth), BF16),
            jax.ShapeDtypeStruct((4, ch, depth), F32),
            jax.ShapeDtypeStruct((s.rs, depth), F32),
        ),
        in_specs=[vm, pl.BlockSpec(memory_space=pl.ANY), vm, vm, vm, pl.BlockSpec(memory_space=pltpu.SMEM)],
        out_specs=(pl.BlockSpec(memory_space=pl.ANY), vm, vm),
        scratch_shapes=scratch,
        compiler_params=pltpu.CompilerParams(
            collective_id=0, has_side_effects=True, vmem_limit_bytes=VMEM_LIMIT),
    )(product_grad, pair_rep, weights.transpose(0, 2, 1), norm_gain.reshape(1, depth),
      residue_mask.reshape(nz, cols), residue_mask)
    blocks = math.gcd(rows, 8)
    pair_grad, weight_grads = pl.pallas_call(
        functools.partial(finish, blocks),
        out_shape=(
            jax.ShapeDtypeStruct((rows, cols, depth), BF16),
            jax.ShapeDtypeStruct((4, ch, depth), F32),
        ),
        in_specs=[pl.BlockSpec(memory_space=pl.ANY), vm, vm],
        out_specs=(pl.BlockSpec(memory_space=pl.ANY), vm),
        scratch_shapes=[pltpu.VMEM((rows, cols, depth), BF16), dma((blocks,)), dma((blocks,))],
    )(grad, found, squares)
    return (pair_grad, weight_grads.transpose(0, 2, 1))


def solution(mesh):
    sizes = mesh.shape["ia"], mesh.shape["ja"], mesh.shape["col"]
    placed = (P("ia", "ja", None), P(), P(None, None, "col"), P(), P("ia", "col", "ja"))

    def step(*args):
        return on_device(*sizes, *args)

    return jax.shard_map(
        step,
        mesh=mesh,
        in_specs=placed,
        out_specs=(P("ia", "ja", None), P(None, None, "col")),
        check_vma=False,
    )
```

```python
import functools
import math

import jax
import jax.numpy as jnp
from jax import lax
from jax.experimental import pallas as pl
from jax.experimental.pallas import tpu as pltpu
from jax.sharding import PartitionSpec as P

CLIP_LIMIT = 64.0
MAX_CHUNKS = 4
ROWS_AT_ONCE = 2
VMEM_LIMIT = 66 * 1000 * 1000
MESH = pl.DeviceIdType.MESH
NT = (((1,), (1,)), ((), ()))
NN = (((1,), (0,)), ((), ()))
F32 = jnp.float32
BF16 = jnp.bfloat16


def dot(a, b, dims):
    return lax.dot_general(a, b, dims, preferred_element_type=F32)


def eye(n):
    rows = lax.broadcasted_iota(jnp.int32, (n, n), 0)
    cols = lax.broadcasted_iota(jnp.int32, (n, n), 1)
    return jnp.where(rows == cols, 1.0, 0.0).astype(BF16)


class Sizes:
    def __init__(self, na, nz, nh, rows, cols, depth, ch):
        self.na, self.nz, self.nh = na, nz, nh
        self.rb, self.k, self.d, self.ch = rows, cols, depth, ch
        self.g = na * nh
        self.naz = na * nz
        self.rh = rows // nh
        self.hid = ch * nh
        self.cp = ch // na
        self.nq = math.gcd(self.cp, MAX_CHUNKS)
        self.cq = self.cp // self.nq
        self.m = na * self.cq
        self.nc = self.g * self.cq
        self.i = na * rows
        self.br = math.gcd(self.rh, 16)
        self.nb = self.rh // self.br
        self.bi = math.gcd(self.rb, 16)
        self.sp = self.hid + 8
        self.pp = self.m + 8
        self.tp = self.br + 8
        self.tb = math.gcd(self.br // 2, ROWS_AT_ONCE)
        self.no = math.gcd(max(4 * self.m // 8, 1), self.naz)
        self.rs = 4 * self.m // self.no
        self.per = max(self.no // na, 1)
        self.stride = na * self.per // self.no
        self.base = (nz - self.per) // 2
        self.q0 = self.nq - self.nq // 2 if nz > 3 else self.nq
        self.helped = max(self.nq - self.q0, 1)


def kernel(s, p_hbm, x_hbm, w_ref, gain_ref, mask_ref, mask_s, out_hbm, found_hbm, sq_hbm,
           xv, p_ref, pt, pg, wall, wt, gain, unit_s, inv_s, nt_s, pr, fac, relay, lrs, lrb, lrh, gs, gsh, gr, turn, ng,
           outv, raw, rx2, rx3, sq,
           xsem, pin, wsend, wrecv, psend, precv, zsend, zrecv, lsend, lrecv, gsend, grecv, osend, orecv,
           r2s, r2r, r3s, r3r, qs, qr, keep, leave, hls, hlr, hgs, hgr):
    na, nz, nh, g_n, nq, cq, nc = s.na, s.nz, s.nh, s.g, s.nq, s.cq, s.nc
    rb, rh, k, d, ch, hid, br, nb, m = s.rb, s.rh, s.k, s.d, s.ch, s.hid, s.br, s.nb, s.m
    a, z, h = lax.axis_index("ia"), lax.axis_index("ja"), lax.axis_index("col")
    me_g = h * na + a
    me_n = a * nz + z
    row0 = a * rb + h * rh
    q0 = s.q0
    is_end = (z == 0) | (z == nz - 1)
    is_near = (z == 1) | (z == nz - 2)
    inward = jnp.where(z == 0, 1, nz - 2)
    outward = jnp.where(z == 1, 0, nz - 1)

    def plane(g):
        return (lax.rem(g, na), z, lax.div(g, na))

    def peer_g(step):
        return lax.rem(me_g + step, g_n)

    def sent(ref, sem):
        pltpu.make_async_copy(ref, ref, sem).wait()

    def send(src, dst, send_sem, recv_sem, device):
        return pltpu.make_async_remote_copy(
            src_ref=src, dst_ref=dst, send_sem=send_sem, recv_sem=recv_sem,
            device_id=device, device_id_type=MESH)

    barrier = pltpu.get_barrier_semaphore()
    total = s.naz * nh
    me_t = me_n * nh + h

    def at_t(t):
        return (lax.div(t, nz * nh), lax.rem(lax.div(t, nh), nz), lax.rem(t, nh))

    def p_in(q):
        at = pl.ds(q * m, m)
        return pltpu.make_async_copy(p_hbm.at[:, at], p_ref.at[:, at], pin.at[q])

    for q in range(nq):
        p_in(q).start()
    for step in range(1, total):
        pl.semaphore_signal(barrier, inc=1, device_id=at_t(lax.rem(me_t + step, total)), device_id_type=MESH)
    xcopy = pltpu.make_async_copy(x_hbm.at[pl.ds(h * rh, rh)], xv, xsem)
    xcopy.start()

    def p_turn(q):
        p_in(q).wait()

        def block(ib, carry):
            slot = lax.rem(ib, 2)
            for ii in range(s.bi):
                relay[slot, ii * s.pp:ii * s.pp + m, :] = p_ref[ib * s.bi + ii, q * m:(q + 1) * m, :].astype(F32)
            for c in range(m):
                tile = relay[slot, pl.ds(c, s.bi, stride=s.pp), :]
                pt[q * m + c, pl.ds(pl.multiple_of(ib * s.bi, s.bi), s.bi), :] = tile.astype(BF16)
            return carry
        lax.fori_loop(0, rb // s.bi, block, 0)

    def pieces(q):
        return [(q * cq + r, 1) for r in range(cq)] if q == 0 else [(q * cq, cq)]

    def p_copy(piece, step):
        c, n = piece
        to = lax.rem(a + step, na)
        return send(pt.at[pl.ds((c // cq) * m + to * cq + c % cq, n)], pg.at[z, pl.ds(c, n), pl.ds(a * rb, rb)],
                    psend, precv.at[c, step], (to, z, h))

    def w_copy(step):
        return send(w_ref, wall.at[h], wsend.at[step], wrecv.at[step], (a, z, lax.rem(h + step, nh)))

    p_turn(0)
    pl.semaphore_wait(barrier, total - 1)
    for step in range(1, nh):
        w_copy(step).start()
    for q in range(nq):
        if q:
            p_turn(q)
        for piece in pieces(q):
            for step in range(1, na):
                p_copy(piece, step).start()
    for q in range(nq):
        for r in range(cq):
            pg[z, q * cq + r, pl.ds(a * rb, rb), :] = pt[q * m + a * cq + r]

    def z_copy(piece, block, up):
        c, n = piece
        ref = pg.at[block, pl.ds(c, n)]
        return send(ref, ref, zsend.at[c // cq, 0 if up else 1], zrecv.at[c, block],
                    (a, z + 1 if up else z - 1, h))

    def goes_up(q):
        return z < (nz - 1 if q < q0 else nz - 2)

    def goes_down(q):
        return z > (0 if q < q0 else 1)

    def z_own(q, some=None):
        for piece in some or pieces(q):
            for step in range(1, na):
                p_copy(piece, step).wait_recv()

            @pl.when(goes_up(q))
            def _(piece=piece):
                z_copy(piece, z, True).start()

            @pl.when(goes_down(q))
            def _(piece=piece):
                z_copy(piece, z, False).start()

    def z_forward(q, hop):
        @pl.when((z >= hop) & goes_up(q))
        def _():
            for piece in pieces(q):
                z_copy(piece, z - hop, True).wait_recv()
                z_copy(piece, z - hop, True).start()

        @pl.when((z + hop < nz) & goes_down(q))
        def _():
            for piece in pieces(q):
                z_copy(piece, z + hop, False).wait_recv()
                z_copy(piece, z + hop, False).start()

    def z_rest(q):
        for hop in range(1, nz):
            here = True if q < q0 else jnp.logical_not(is_end)

            @pl.when((z >= hop) & jnp.logical_not(goes_up(q)) & here)
            def _(hop=hop):
                for piece in pieces(q):
                    z_copy(piece, z - hop, True).wait_recv()

            @pl.when((z + hop < nz) & jnp.logical_not(goes_down(q)) & here)
            def _(hop=hop):
                for piece in pieces(q):
                    z_copy(piece, z + hop, False).wait_recv()

    eye_d = eye(d)
    column = jnp.transpose(jnp.broadcast_to(gain_ref[...], (k, d)))
    gain[...] = jnp.concatenate([column, column], axis=1)
    wall[h] = w_ref[...]
    for step in range(1, nh):
        w_copy(step).wait_recv()
    for q in range(nq):
        rows = [wall[half, w, q * m:(q + 1) * m, :] for half in range(nh) for w in range(4)]
        wt[q] = dot(eye_d, jnp.concatenate(rows, axis=0), NT).astype(BF16)

    xcopy.wait()
    col_valid = mask_ref[pl.ds(z, 1), :].astype(F32)

    def rows_step(t, sub):
        x2 = xv[pl.ds(2 * t, 2)].reshape(2 * k, d)
        xt = dot(eye_d, x2, NT)
        centred = xt - jnp.mean(xt, axis=0, keepdims=True)
        inv = lax.rsqrt(jnp.mean(centred * centred, axis=0, keepdims=True) + 1e-05)
        unit = centred * inv
        normed = (unit * gain[...]).astype(BF16)
        unit_s[t] = unit
        inv_s[t] = inv
        nt_s[t] = normed
        for half in range(nh):
            pr[half * 4 * ch:(half + 1) * 4 * ch, :] = dot(wall[half].reshape(4 * ch, d), normed, NN)
        valid = jnp.concatenate(
            [col_valid * mask_s[row0 + 2 * t + e].astype(F32) for e in range(2)], axis=1)
        for q in range(nq):
            for side in range(2):
                def part(w):
                    at = [half * 4 * ch + w * ch + q * m for half in range(nh)]
                    return jnp.concatenate([pr[x:x + m, :] for x in at], axis=0)
                lin = part(2 * side)
                gate = jax.nn.sigmoid(part(2 * side + 1))
                first = valid * gate
                value = first * lin
                fac[t, q, 2 * side] = first.astype(BF16)
                fac[t, q, 2 * side + 1] = (value * (1.0 - gate)).astype(BF16)
                for e in range(2):
                    at = pl.multiple_of((2 * sub + e) * s.sp, 8) + q * nc
                    relay[side, pl.ds(at, nc), :] = value[:, e * k:(e + 1) * k]

    for b in range(nb):
        def one(sub, carry, b=b):
            rows_step(b * (br // 2) + sub, sub)
            return carry
        parts = pieces(0) if b == 0 else [None]
        each = br // 2 // len(parts)
        if each * len(parts) * 2 == br:
            for n, piece in enumerate(parts):
                lax.fori_loop(n * each, (n + 1) * each, one, 0)
                if piece:
                    z_own(0, [piece])
        else:
            lax.fori_loop(0, br // 2, one, 0)
            if b == 0:
                z_own(0)

        def flush(c, carry, b=b):
            for side in range(2):
                tile = relay[side, pl.ds(c, br, stride=s.sp), :]
                lrs[side, c, b * br:(b + 1) * br, :] = tile.astype(BF16)
            return carry
        lax.fori_loop(0, hid, flush, 0, unroll=4)
        if 0 < b < q0:
            z_own(b)
    for q in range(nb, q0):
        z_own(q)

    @pl.when(is_end)
    def _():
        for q in range(q0, nq):
            z_own(q)

    def lr_copy(q, step):
        return send(lrs.at[:, pl.ds(q * nc + peer_g(step) * cq, cq)],
                    lrb.at[:, pl.ds(q * cq, cq), pl.ds(row0, rh)],
                    lsend, lrecv.at[q, step], plane(peer_g(step)))

    for q in [*range(q0, nq), *range(q0)]:
        for step in range(1, g_n):
            lr_copy(q, step).start()
    for q in range(nq):
        for side in range(2):
            for r in range(cq):
                lrb[side, q * cq + r, pl.ds(row0, rh), :] = lrs[side, q * nc + me_g * cq + r]

    eye_k = eye(k)

    def triangle(c, lr, at, to):
        panel = jnp.concatenate([pg[b, c] for b in range(nz)], axis=1)
        left, right = lr[0, at], lr[1, at]
        to[0, at] = dot(panel, right, NN).astype(BF16).reshape(g_n, rh, k)
        left_t = dot(eye_k, left, NT).astype(BF16)
        back_t = dot(left_t, panel, NN).astype(BF16)
        back = [dot(eye_k, back_t[:, b * k:(b + 1) * k], NT).astype(BF16) for b in range(nz)]
        to[1, at] = jnp.concatenate(back, axis=0).reshape(g_n, rh, k)

    def triangles(q, lr, to, base):
        def one(r, carry):
            triangle(q * cq + r, lr, (q - base) * cq + r, to)
            return carry
        lax.fori_loop(0, cq, one, 0)

    def in_copy(q, z_to):
        return send(lrb.at[:, pl.ds(q * cq, cq)], lrh.at[:, pl.ds((q - q0) * cq, cq)],
                    hls, hlr.at[q - q0], (a, z_to, h))

    def cuts(q):
        whole = [(b, 0, cq) for b in range(nb)]
        if q == nq - 1 and q >= q0 and cq % 2 == 0:
            return whole[:-1] + [(nb - 1, 0, cq // 2), (nb - 1, cq // 2, cq // 2)]
        return whole

    def back_copy(q, at, z_to):
        b, lo, n = cuts(q)[at]
        return send(gsh.at[:, pl.ds((q - q0) * cq + lo, n), :, pl.ds(b * br, br)],
                    gs.at[:, pl.ds(q * cq + lo, n), :, pl.ds(b * br, br)],
                    hgs, hgr.at[q - q0, at], (a, z_to, h))

    def g_copy(q, at, step):
        b, lo, n = cuts(q)[at]
        g = peer_g(step)
        place = lax.rem(g, na) * nh + lax.div(g, na)
        return send(gs.at[:, pl.ds(q * cq + lo, n), place, pl.ds(b * br, br)],
                    gr.at[:, pl.ds(q * nc + me_g * cq + lo, n), pl.ds(b * br, br)],
                    gsend.at[q], grecv.at[q, at, step], plane(g))

    def out_copy(b, step):
        return send(outv.at[pl.ds(b * br, br)], out_hbm.at[pl.ds(h * rh + b * br, br)],
                    osend.at[b, step], orecv.at[b, step], (a, z, lax.rem(h + step, nh)))

    def keep_copy(b):
        return pltpu.make_async_copy(
            outv.at[pl.ds(b * br, br)], out_hbm.at[pl.ds(h * rh + b * br, br)], keep.at[b])

    def at_n(n):
        return (lax.div(n, nz), lax.rem(n, nz), h)

    def owner(o):
        return (o // s.per * s.stride, s.base + o % s.per)

    def other(o, half=None):
        away = (a != owner(o)[0]) | (z != owner(o)[1])
        return away if half is None else away | (h != half)

    me_o = lax.div(a, s.stride) * s.per + z - s.base
    is_owner = (lax.rem(a, s.stride) == 0) & (z >= s.base) & (z < s.base + s.per)
    batches = [(0, nq - 1), (nq - 1, nq)] if nq > 1 else [(0, nq)]
    final = len(batches) - 1

    def r2_copy(batch, half, o, sender):
        lo, hi = batches[batch]
        return send(raw.at[lo:hi, half, o], rx2.at[sender, lo:hi],
                    r2s.at[batch], r2r.at[batch, sender], (*owner(o), half))

    def r2_start(batch):
        for half in range(nh):
            for o in range(s.no):
                @pl.when(other(o, half))
                def _(half=half, o=o):
                    r2_copy(batch, half, o, me_t).start()

    def r3_copy(batch, o, step):
        lo, hi = batches[batch]
        ref = rx3.at[o, lo:hi]
        return send(ref, ref, r3s.at[batch], r3r.at[batch, o], at_n(lax.rem(me_n + step, s.naz)))

    def sq_copy(slot, step):
        ref = sq.at[slot]
        return send(ref, ref, qs, qr.at[slot], at_t(lax.rem(me_t + step, total)))

    def r2_sum(batch):
        lo, hi = batches[batch]

        @pl.when(is_owner)
        def _():
            def one(step, mine):
                n = lax.rem(me_t + step, total)
                r2_copy(batch, 0, 0, n).wait_recv()
                return mine + rx2[n, lo:hi]
            rx3[me_o, lo:hi] = lax.fori_loop(1, total, one, raw[lo:hi, h, me_o])
            for step in range(1, s.naz):
                r3_copy(batch, me_o, step).start()
            if batch == final:
                slot = h * s.no + me_o
                found = rx3[me_o].reshape(nq * s.rs, d)
                sq[slot] = jnp.sum(found * found, axis=0, keepdims=True)
                for step in range(1, total):
                    sq_copy(slot, step).start()

    def r3_wait(batch):
        for o in range(s.no):
            @pl.when(other(o))
            def _(o=o):
                r3_copy(batch, o, 1).wait_recv()

    def sq_wait():
        for half in range(nh):
            for o in range(s.no):
                @pl.when(other(o, half))
                def _(slot=half * s.no + o):
                    sq_copy(slot, 1).wait_recv()

    def gather(q, b):
        for at, cut in enumerate(cuts(q)):
            for step in range(1, g_n if cut[0] == b else 1):
                g_copy(q, at, step).wait_recv()

        def spread(n, carry):
            for side in range(2):
                tile = gr[side, q * nc + n, b * br:(b + 1) * br, :].astype(F32)
                turn[side, pl.ds(pl.multiple_of(n * s.tp, 8), br), :] = tile
            return carry
        lax.fori_loop(0, nc, spread, 0, unroll=4)
        if b == 0:
            raw[q] = jnp.zeros((nh, s.no, s.rs, d), F32)

        def one(sub, carry):
            t0 = b * (br // 2) + sub * s.tb
            terms = []
            for side in range(2):
                both = jnp.concatenate(
                    [turn[side, pl.ds(2 * s.tb * sub + e, nc, stride=s.tp), :] for e in range(2 * s.tb)], axis=1)
                for w in range(2):
                    factor = jnp.concatenate([fac[t0 + u, q, 2 * side + w] for u in range(s.tb)], axis=1)
                    terms.append((both * factor.astype(F32)).astype(BF16))
            grads = jnp.concatenate(
                [term[half * m:(half + 1) * m] for half in range(nh) for term in terms], axis=0)
            normed = jnp.concatenate([nt_s[t0 + u] for u in range(s.tb)], axis=1)
            raw[q] += dot(grads, normed, NT).reshape(nh, s.no, s.rs, d)
            part = dot(wt[q], grads, NN)
            for u in range(s.tb):
                piece = part[:, u * 2 * k:(u + 1) * 2 * k]
                ng[t0 + u] = ng[t0 + u] + piece if q else piece
            return carry
        lax.fori_loop(0, br // 2 // s.tb, one, 0)

    def norm_back(b):
        def one(sub, carry):
            t = b * (br // 2) + sub
            unit = unit_s[t]
            scaled = ng[t] * gain[...]
            first = jnp.mean(scaled, axis=0, keepdims=True)
            second = jnp.mean(scaled * unit, axis=0, keepdims=True)
            res = (inv_s[t] * (scaled - first - unit * second)).astype(BF16)
            for e in range(2):
                outv[2 * t + e] = dot(eye_k, res[:, e * k:(e + 1) * k], NT).astype(BF16)
            return carry
        lax.fori_loop(0, br // 2, one, 0, unroll=2)
        keep_copy(b).start()
        for step in range(1, nh):
            out_copy(b, step).start()

    def lr_wait(q):
        for step in range(1, g_n):
            lr_copy(q, step).wait_recv()

    def g_send(q, at):
        b, lo, n = cuts(q)[at]
        for step in range(1, g_n):
            g_copy(q, at, step).start()
        for side in range(2):
            for r in range(lo, lo + n):
                gr[side, q * nc + me_g * cq + r, b * br:(b + 1) * br, :] = gs[
                    side, q * cq + r, a * nh + h, b * br:(b + 1) * br, :]

    def make(q):
        if q < q0:
            z_rest(q)
            lr_wait(q)
            triangles(q, lrb, gs, 0)
            return

        @pl.when(is_near)
        def _():
            z_rest(q)
            in_copy(q, outward).wait_recv()
            triangles(q, lrh, gsh, q0)
            for at in range(len(cuts(q))):
                back_copy(q, at, outward).start()
            lr_wait(q)
            triangles(q, lrb, gs, 0)

        @pl.when(jnp.logical_not(is_near | is_end))
        def _():
            z_rest(q)
            lr_wait(q)
            triangles(q, lrb, gs, 0)

    def came_back(q, at):
        if q >= q0:
            @pl.when(is_end)
            def _():
                back_copy(q, at, outward).wait_recv()

    for hop in range(1, nz - 1):
        for q in range(q0):
            z_forward(q, hop)
        if hop == 1 and q0 < nq:
            @pl.when(jnp.logical_not(is_end))
            def _():
                z_own(q0)
    for q in range(q0, nq):
        for hop in range(1, nz - 1):
            z_forward(q, hop)
        if q + 1 < nq:
            @pl.when(jnp.logical_not(is_end))
            def _(q=q):
                z_own(q + 1)

    @pl.when(is_end)
    def _():
        for q in range(q0, nq):
            lr_wait(q)
            in_copy(q, inward).start()

    def drain():
        for step in range(1, nh):
            w_copy(step).wait_send()
        sent(pt.at[pl.ds(0, (na - 1) * s.cp)], psend)
        sent(lrs.at[:, pl.ds(0, (g_n - 1) * nq * cq)], lsend)
        for q in range(nq):
            sent(gs.at[:, pl.ds(q * cq, cq), pl.ds(0, g_n - 1)], gsend.at[q])
            for count in range(1, nz):
                @pl.when((z + 1 == count) & goes_up(q))
                def _(q=q, count=count):
                    sent(pg.at[pl.ds(0, count), pl.ds(q * cq, cq)], zsend.at[q, 0])

                @pl.when((nz - z == count) & goes_down(q))
                def _(q=q, count=count):
                    sent(pg.at[pl.ds(0, count), pl.ds(q * cq, cq)], zsend.at[q, 1])
        if q0 < nq:
            @pl.when(is_end)
            def _():
                sent(lrh, hls)

            @pl.when(is_near)
            def _():
                sent(gsh, hgs)

    last = nq - 1
    queue = []

    def run(count):
        for _ in range(min(count, len(queue))):
            q, b = queue.pop(0)
            gather(q, b)
            if b == nb - 1 and q == last - 1:
                r2_start(0)
            if b == nb - 1 and q == last:
                r2_start(final)

    for q in range(nq):
        make(q)
        if q > 1:
            queue += [(q - 2, b) for b in range(nb)]
        if q == last:
            queue += [(last - 1, b) for b in range(nb)] if q else []
            run(max(len(queue) - 2 * nb, 0))
        ways = cuts(q)
        for at, (b, lo, n) in enumerate(ways):
            run(1 if q < last else 0)
            came_back(q, at)
            g_send(q, at)
            if q == last:
                run(3 if b < nb - 1 else 1 if at < len(ways) - 1 else 0)
                if b and not lo:
                    queue.append((last, b - 1))
    queue.append((last, nb - 1))
    run(max(len(queue) - 1, 0))
    if nb > 1:
        norm_back(0)
    run(1)
    waiting = list(range(len(batches)))
    for b in range(1 if nb > 1 else 0, nb):
        if len(waiting) > 1:
            r2_sum(waiting.pop(0))
        norm_back(b)
    for batch in waiting:
        r2_sum(batch)
    drain()
    for batch in range(len(batches)):
        r3_wait(batch)
    found_out = pltpu.make_async_copy(rx3, found_hbm, leave.at[0])
    found_out.start()
    sq_wait()
    sq_out = pltpu.make_async_copy(sq.at[pl.ds(0, nh * s.no)], sq_hbm, leave.at[1])
    sq_out.start()
    for b in range(nb):
        keep_copy(b).wait()
        for step in range(1, nh):
            out_copy(b, step).wait()
    for batch, (lo, hi) in enumerate(batches):
        @pl.when(is_owner)
        def _(batch=batch, lo=lo, hi=hi):
            sent(rx2.at[pl.ds(0, nh * s.no - 1), lo:hi], r2s.at[batch])
            sent(rx2.at[pl.ds(0, s.naz - 1), lo:hi], r3s.at[batch])

        @pl.when(jnp.logical_not(is_owner))
        def _(batch=batch, lo=lo, hi=hi):
            sent(rx2.at[pl.ds(0, nh * s.no), lo:hi], r2s.at[batch])

    @pl.when(is_owner)
    def _():
        sent(sq.at[pl.ds(0, total - 1)], qs)
    found_out.wait()
    sq_out.wait()


def finish(s, blocks, from_hbm, found_ref, sq_ref, out_hbm, wg_ref, held, sem_in, sem_out):
    size = held.shape[0] // blocks

    def came(b):
        at = pl.ds(b * size, size)
        return pltpu.make_async_copy(from_hbm.at[at], held.at[at], sem_in.at[b])

    def leaves(b):
        at = pl.ds(b * size, size)
        return pltpu.make_async_copy(held.at[at], out_hbm.at[at], sem_out.at[b])

    for b in range(blocks):
        came(b).start()
    squares = jnp.sum(jnp.sum(sq_ref[...], axis=0), axis=1, keepdims=True)
    factor = jnp.minimum(1.0, CLIP_LIMIT * lax.rsqrt(squares + 1e-06))
    for q in range(s.nq):
        for o in range(s.no):
            w, at = o * s.rs // s.m, q * s.m + o * s.rs % s.m
            wg_ref[w, at:at + s.rs, :] = found_ref[o, q] * factor
    for b in range(blocks):
        came(b).wait()
        leaves(b).start()
    for b in range(blocks):
        leaves(b).wait()


def on_device(na, nz, nh, pair_rep, norm_gain, weights, residue_mask, product_grad):
    rows, cols, depth = pair_rep.shape
    ch = product_grad.shape[1]
    s = Sizes(na, nz, nh, rows, cols, depth, ch)
    vm = pl.BlockSpec(memory_space=pltpu.VMEM)
    anywhere = pl.BlockSpec(memory_space=pl.ANY)
    dma = pltpu.SemaphoreType.DMA
    half = s.rh // 2
    scratch = [
        pltpu.VMEM((s.rh, cols, depth), BF16),
        pltpu.VMEM((rows, ch, cols), BF16),
        pltpu.VMEM((ch, rows, cols), BF16),
        pltpu.VMEM((nz, s.cp, s.i, cols), BF16),
        pltpu.VMEM((nh, 4, ch, depth), BF16),
        pltpu.VMEM((s.nq, depth, 4 * s.nc), BF16),
        pltpu.VMEM((depth, 2 * cols), F32),
        pltpu.VMEM((half, depth, 2 * cols), F32),
        pltpu.VMEM((half, 1, 2 * cols), F32),
        pltpu.VMEM((half, depth, 2 * cols), BF16),
        pltpu.VMEM((4 * s.hid, 2 * cols), F32),
        pltpu.VMEM((half, s.nq, 4, s.nc, 2 * cols), BF16),
        pltpu.VMEM((2, max(s.br * s.sp, s.bi * s.pp), cols), F32),
        pltpu.VMEM((2, s.hid, s.rh, cols), BF16),
        pltpu.VMEM((2, s.cp, s.i, cols), BF16),
        pltpu.VMEM((2, s.helped * s.cq, s.i, cols), BF16),
        pltpu.VMEM((2, s.cp, s.g, s.rh, cols), BF16),
        pltpu.VMEM((2, s.helped * s.cq, s.g, s.rh, cols), BF16),
        pltpu.VMEM((2, s.hid, s.rh, cols), BF16),
        pltpu.VMEM((2, s.nc * s.tp, cols), F32),
        pltpu.VMEM((half, depth, 2 * cols), F32),
        pltpu.VMEM((s.rh, cols, depth), BF16),
        pltpu.VMEM((s.nq, nh, s.no, s.rs, depth), F32),
        pltpu.VMEM((s.naz * nh, s.nq, s.rs, depth), F32),
        pltpu.VMEM((s.no, s.nq, s.rs, depth), F32),
        pltpu.VMEM((s.naz * nh, 1, depth), F32),
        dma(()), dma((s.nq,)), dma((nh,)), dma((nh,)),
        dma(()), dma((s.cp, na)), dma((s.nq, 2)), dma((s.cp, nz)),
        dma(()), dma((s.nq, s.g)), dma((s.nq,)), dma((s.nq, s.nb + 1, s.g)),
        dma((s.nb, nh)), dma((s.nb, nh)),
        dma((2,)), dma((2, s.naz * nh)), dma((2,)), dma((2, s.no)),
        dma(()), dma((nh * s.no,)), dma((s.nb,)), dma((2,)),
        dma(()), dma((s.helped,)), dma(()), dma((s.helped, s.nb + 1)),
    ]
    grad, found, squares = pl.pallas_call(
        functools.partial(kernel, s),
        out_shape=(
            jax.ShapeDtypeStruct((rows, cols, depth), BF16),
            jax.ShapeDtypeStruct((s.no, s.nq, s.rs, depth), F32),
            jax.ShapeDtypeStruct((nh * s.no, 1, depth), F32),
        ),
        in_specs=[anywhere, anywhere, vm, vm, vm, pl.BlockSpec(memory_space=pltpu.SMEM)],
        out_specs=(anywhere, anywhere, anywhere),
        scratch_shapes=scratch,
        compiler_params=pltpu.CompilerParams(
            collective_id=0, has_side_effects=True, vmem_limit_bytes=VMEM_LIMIT),
    )(product_grad, pair_rep, weights.transpose(0, 2, 1), norm_gain.reshape(1, depth),
      residue_mask.reshape(nz, cols), residue_mask)
    blocks = math.gcd(rows, 4)
    pair_grad, weight_grads = pl.pallas_call(
        functools.partial(finish, s, blocks),
        out_shape=(
            jax.ShapeDtypeStruct((rows, cols, depth), BF16),
            jax.ShapeDtypeStruct((4, ch, depth), F32),
        ),
        in_specs=[pl.BlockSpec(memory_space=pl.ANY), vm, vm],
        out_specs=(pl.BlockSpec(memory_space=pl.ANY), vm),
        scratch_shapes=[pltpu.VMEM((rows, cols, depth), BF16), dma((blocks,)), dma((blocks,))],
    )(grad, found, squares)
    return (pair_grad, weight_grads.transpose(0, 2, 1))


def solution(mesh):
    sizes = mesh.shape["ia"], mesh.shape["ja"], mesh.shape["col"]
    placed = (P("ia", "ja", None), P(), P(None, None, "col"), P(), P("ia", "col", "ja"))

    def step(*args):
        return on_device(*sizes, *args)

    return jax.shard_map(
        step,
        mesh=mesh,
        in_specs=placed,
        out_specs=(P("ia", "ja", None), P(None, None, "col")),
        check_vma=False,
    )
```

```python
import functools
import math

import jax
import jax.numpy as jnp
from jax import lax
from jax.experimental import pallas as pl
from jax.experimental.pallas import tpu as pltpu
from jax.sharding import PartitionSpec as P

CLIP_LIMIT = 64.0
MAX_CHUNKS = 4
ROWS_AT_ONCE = 2
VMEM_LIMIT = 66 * 1000 * 1000
MESH = pl.DeviceIdType.MESH
NT = (((1,), (1,)), ((), ()))
NN = (((1,), (0,)), ((), ()))
F32 = jnp.float32
BF16 = jnp.bfloat16


def dot(a, b, dims):
    return lax.dot_general(a, b, dims, preferred_element_type=F32)


def eye(n):
    rows = lax.broadcasted_iota(jnp.int32, (n, n), 0)
    cols = lax.broadcasted_iota(jnp.int32, (n, n), 1)
    return jnp.where(rows == cols, 1.0, 0.0).astype(BF16)


class Sizes:
    def __init__(self, na, nz, nh, rows, cols, depth, ch):
        self.na, self.nz, self.nh = na, nz, nh
        self.rb, self.k, self.d, self.ch = rows, cols, depth, ch
        self.g = na * nh
        self.naz = na * nz
        self.rh = rows // nh
        self.hid = ch * nh
        self.cp = ch // na
        self.nq = math.gcd(self.cp, MAX_CHUNKS)
        self.cq = self.cp // self.nq
        self.m = na * self.cq
        self.nc = self.g * self.cq
        self.i = na * rows
        self.br = math.gcd(self.rh, 16)
        self.nb = self.rh // self.br
        self.bi = math.gcd(self.rb, 16)
        self.sp = self.hid + 8
        self.pp = self.m + 8
        self.tp = self.br + 8
        self.tb = math.gcd(self.br // 2, ROWS_AT_ONCE)
        self.no = math.gcd(max(4 * self.m // 8, 1), self.naz)
        self.rs = 4 * self.m // self.no
        self.per = max(self.no // na, 1)
        self.stride = na * self.per // self.no
        self.base = (nz - self.per) // 2
        self.q0 = self.nq - self.nq // 2 if nz > 3 else self.nq
        self.helped = max(self.nq - self.q0, 1)


def kernel(s, p_hbm, x_hbm, w_ref, gain_ref, mask_ref, mask_s, out_hbm, found_hbm, sq_hbm,
           xv, p_ref, pt, pg, wall, wt, gain, unit_s, inv_s, nt_s, pr, fac, relay, lrs, lrb, lrh, gs, gsh, gr, turn, ng,
           outv, raw, rx2, rx3, sq,
           xsem, pin, wsend, wrecv, psend, precv, zsend, zrecv, lsend, lrecv, gsend, grecv, osend, orecv,
           r2s, r2r, r3s, r3r, qs, qr, keep, leave, hls, hlr, hgs, hgr):
    na, nz, nh, g_n, nq, cq, nc = s.na, s.nz, s.nh, s.g, s.nq, s.cq, s.nc
    rb, rh, k, d, ch, hid, br, nb, m = s.rb, s.rh, s.k, s.d, s.ch, s.hid, s.br, s.nb, s.m
    a, z, h = lax.axis_index("ia"), lax.axis_index("ja"), lax.axis_index("col")
    me_g = h * na + a
    me_n = a * nz + z
    row0 = a * rb + h * rh
    q0 = s.q0
    is_end = (z == 0) | (z == nz - 1)
    is_near = (z == 1) | (z == nz - 2)
    inward = jnp.where(z == 0, 1, nz - 2)
    outward = jnp.where(z == 1, 0, nz - 1)

    def plane(g):
        return (lax.rem(g, na), z, lax.div(g, na))

    def peer_g(step):
        return lax.rem(me_g + step, g_n)

    def sent(ref, sem):
        pltpu.make_async_copy(ref, ref, sem).wait()

    def send(src, dst, send_sem, recv_sem, device):
        return pltpu.make_async_remote_copy(
            src_ref=src, dst_ref=dst, send_sem=send_sem, recv_sem=recv_sem,
            device_id=device, device_id_type=MESH)

    barrier = pltpu.get_barrier_semaphore()
    total = s.naz * nh
    me_t = me_n * nh + h

    def at_t(t):
        return (lax.div(t, nz * nh), lax.rem(lax.div(t, nh), nz), lax.rem(t, nh))

    def p_in(q):
        at = pl.ds(q * m, m)
        return pltpu.make_async_copy(p_hbm.at[:, at], p_ref.at[:, at], pin.at[q])

    for q in range(nq):
        p_in(q).start()
    for step in range(1, total):
        pl.semaphore_signal(barrier, inc=1, device_id=at_t(lax.rem(me_t + step, total)), device_id_type=MESH)
    xcopy = pltpu.make_async_copy(x_hbm.at[pl.ds(h * rh, rh)], xv, xsem)
    xcopy.start()

    def p_turn(q):
        p_in(q).wait()

        def block(ib, carry):
            slot = lax.rem(ib, 2)
            for ii in range(s.bi):
                relay[slot, ii * s.pp:ii * s.pp + m, :] = p_ref[ib * s.bi + ii, q * m:(q + 1) * m, :].astype(F32)
            for c in range(m):
                tile = relay[slot, pl.ds(c, s.bi, stride=s.pp), :]
                pt[q * m + c, pl.ds(pl.multiple_of(ib * s.bi, s.bi), s.bi), :] = tile.astype(BF16)
            return carry
        lax.fori_loop(0, rb // s.bi, block, 0)

    def pieces(q):
        return [(q * cq + r, 1) for r in range(cq)] if q == 0 else [(q * cq, cq)]

    def spot(c):
        return c if c < cq else cq - 1 + c // cq

    def p_copy(piece, step):
        c, n = piece
        to = lax.rem(a + step, na)
        return send(pt.at[pl.ds((c // cq) * m + to * cq + c % cq, n)], pg.at[z, pl.ds(c, n), pl.ds(a * rb, rb)],
                    psend, precv.at[spot(c)], (to, z, h))

    def w_copy(step):
        return send(w_ref, wall.at[h], wsend.at[step], wrecv.at[step], (a, z, lax.rem(h + step, nh)))

    p_turn(0)
    pl.semaphore_wait(barrier, total - 1)
    for step in range(1, nh):
        w_copy(step).start()
    for q in range(nq):
        if q:
            p_turn(q)
        for piece in pieces(q):
            for step in range(1, na):
                p_copy(piece, step).start()
    for q in range(nq):
        for r in range(cq):
            pg[z, q * cq + r, pl.ds(a * rb, rb), :] = pt[q * m + a * cq + r]

    def z_copy(piece, block, up):
        c, n = piece
        ref = pg.at[block, pl.ds(c, n)]
        return send(ref, ref, zsend.at[c // cq, 0 if up else 1], zrecv.at[spot(c), block],
                    (a, z + 1 if up else z - 1, h))

    def goes_up(q):
        return z < (nz - 1 if q < q0 else nz - 2)

    def goes_down(q):
        return z > (0 if q < q0 else 1)

    def z_own(q, some=None):
        for piece in some or pieces(q):
            sent(pt.at[pl.ds(0, (na - 1) * piece[1])], precv.at[spot(piece[0])])

            @pl.when(goes_up(q))
            def _(piece=piece):
                z_copy(piece, z, True).start()

            @pl.when(goes_down(q))
            def _(piece=piece):
                z_copy(piece, z, False).start()

    def z_forward(q, hop):
        @pl.when((z >= hop) & goes_up(q))
        def _():
            for piece in pieces(q):
                z_copy(piece, z - hop, True).wait_recv()
                z_copy(piece, z - hop, True).start()

        @pl.when((z + hop < nz) & goes_down(q))
        def _():
            for piece in pieces(q):
                z_copy(piece, z + hop, False).wait_recv()
                z_copy(piece, z + hop, False).start()

    def z_rest(q):
        for hop in range(1, nz):
            here = True if q < q0 else jnp.logical_not(is_end)

            @pl.when((z >= hop) & jnp.logical_not(goes_up(q)) & here)
            def _(hop=hop):
                for piece in pieces(q):
                    z_copy(piece, z - hop, True).wait_recv()

            @pl.when((z + hop < nz) & jnp.logical_not(goes_down(q)) & here)
            def _(hop=hop):
                for piece in pieces(q):
                    z_copy(piece, z + hop, False).wait_recv()

    eye_d = eye(d)
    column = jnp.transpose(jnp.broadcast_to(gain_ref[...], (k, d)))
    gain[...] = jnp.concatenate([column, column], axis=1)
    wall[h] = w_ref[...]
    for step in range(1, nh):
        w_copy(step).wait_recv()
    for q in range(nq):
        rows = [wall[half, w, q * m:(q + 1) * m, :] for half in range(nh) for w in range(4)]
        wt[q] = dot(eye_d, jnp.concatenate(rows, axis=0), NT).astype(BF16)

    xcopy.wait()
    col_valid = mask_ref[pl.ds(z, 1), :].astype(F32)

    def rows_step(t, sub):
        x2 = xv[pl.ds(2 * t, 2)].reshape(2 * k, d)
        xt = dot(eye_d, x2, NT)
        centred = xt - jnp.mean(xt, axis=0, keepdims=True)
        inv = lax.rsqrt(jnp.mean(centred * centred, axis=0, keepdims=True) + 1e-05)
        unit = centred * inv
        normed = (unit * gain[...]).astype(BF16)
        unit_s[t] = unit
        inv_s[t] = inv
        nt_s[t] = normed
        for half in range(nh):
            pr[half * 4 * ch:(half + 1) * 4 * ch, :] = dot(wall[half].reshape(4 * ch, d), normed, NN)
        valid = jnp.concatenate(
            [col_valid * mask_s[row0 + 2 * t + e].astype(F32) for e in range(2)], axis=1)
        for q in range(nq):
            for side in range(2):
                def part(w):
                    at = [half * 4 * ch + w * ch + q * m for half in range(nh)]
                    return jnp.concatenate([pr[x:x + m, :] for x in at], axis=0)
                lin = part(2 * side)
                gate = jax.nn.sigmoid(part(2 * side + 1))
                first = valid * gate
                value = first * lin
                fac[t, q, 2 * side] = first.astype(BF16)
                fac[t, q, 2 * side + 1] = (value * (1.0 - gate)).astype(BF16)
                for e in range(2):
                    at = pl.multiple_of((2 * sub + e) * s.sp, 8) + q * nc
                    relay[side, pl.ds(at, nc), :] = value[:, e * k:(e + 1) * k]

    for b in range(nb):
        def one(sub, carry, b=b):
            rows_step(b * (br // 2) + sub, sub)
            return carry
        parts = pieces(0) if b == 0 else [None]
        each = br // 2 // len(parts)
        if each * len(parts) * 2 == br:
            for n, piece in enumerate(parts):
                lax.fori_loop(n * each, (n + 1) * each, one, 0)
                if piece:
                    z_own(0, [piece])
        else:
            lax.fori_loop(0, br // 2, one, 0)
            if b == 0:
                z_own(0)

        def flush(c, carry, b=b):
            for side in range(2):
                tile = relay[side, pl.ds(c, br, stride=s.sp), :]
                lrs[side, c, b * br:(b + 1) * br, :] = tile.astype(BF16)
            return carry
        lax.fori_loop(0, hid, flush, 0, unroll=4)
        if 0 < b < q0:
            z_own(b)
    for q in range(nb, q0):
        z_own(q)

    @pl.when(is_end)
    def _():
        for q in range(q0, nq):
            z_own(q)

    def lr_copy(q, step):
        return send(lrs.at[:, pl.ds(q * nc + peer_g(step) * cq, cq)],
                    lrb.at[:, pl.ds(q * cq, cq), pl.ds(row0, rh)],
                    lsend, lrecv.at[q], plane(peer_g(step)))

    for q in [*range(q0, nq), *range(q0)]:
        for step in range(1, g_n):
            lr_copy(q, step).start()
    for q in range(nq):
        for side in range(2):
            for r in range(cq):
                lrb[side, q * cq + r, pl.ds(row0, rh), :] = lrs[side, q * nc + me_g * cq + r]

    eye_k = eye(k)

    def triangle(c, lr, at, to):
        panel = jnp.concatenate([pg[b, c] for b in range(nz)], axis=1)
        left, right = lr[0, at], lr[1, at]
        to[0, at] = dot(panel, right, NN).astype(BF16).reshape(g_n, rh, k)
        left_t = dot(eye_k, left, NT).astype(BF16)
        back_t = dot(left_t, panel, NN).astype(BF16)
        back = [dot(eye_k, back_t[:, b * k:(b + 1) * k], NT).astype(BF16) for b in range(nz)]
        to[1, at] = jnp.concatenate(back, axis=0).reshape(g_n, rh, k)

    def triangles(q, lr, to, base):
        def one(r, carry):
            triangle(q * cq + r, lr, (q - base) * cq + r, to)
            return carry
        lax.fori_loop(0, cq, one, 0)

    def in_copy(q, z_to):
        return send(lrb.at[:, pl.ds(q * cq, cq)], lrh.at[:, pl.ds((q - q0) * cq, cq)],
                    hls, hlr.at[q - q0], (a, z_to, h))

    def g_copy(q, b, step):
        g = peer_g(step)
        place = lax.rem(g, na) * nh + lax.div(g, na)
        return send(gs.at[:, pl.ds(q * cq, cq), place, pl.ds(b * br, br)],
                    gr.at[:, pl.ds(q * nc + me_g * cq, cq), pl.ds(b * br, br)],
                    gsend.at[q], grecv.at[q, b], plane(g))

    def back_copy(q, b, z_to):
        return send(gsh.at[:, pl.ds((q - q0) * cq, cq), :, pl.ds(b * br, br)],
                    gs.at[:, pl.ds(q * cq, cq), :, pl.ds(b * br, br)],
                    hgs, hgr.at[q - q0, b], (a, z_to, h))

    def direct(q):
        return q == nq - 1 and q >= q0

    def direct_copy(q, b, step):
        g = peer_g(step)
        place = lax.rem(g, na) * nh + lax.div(g, na)
        return send(gsh.at[:, pl.ds((q - q0) * cq, cq), place, pl.ds(b * br, br)],
                    gr.at[:, pl.ds(q * nc + me_g * cq, cq), pl.ds(b * br, br)],
                    hgs, grecv.at[q, b], (lax.rem(g, na), outward, lax.div(g, na)))

    def out_copy(b, step):
        return send(outv.at[pl.ds(b * br, br)], out_hbm.at[pl.ds(h * rh + b * br, br)],
                    osend.at[b, step], orecv.at[b, step], (a, z, lax.rem(h + step, nh)))

    def keep_copy(b):
        return pltpu.make_async_copy(
            outv.at[pl.ds(b * br, br)], out_hbm.at[pl.ds(h * rh + b * br, br)], keep.at[b])

    def at_n(n):
        return (lax.div(n, nz), lax.rem(n, nz), h)

    def owner(o):
        return (o // s.per * s.stride, s.base + o % s.per)

    def other(o, half=None):
        away = (a != owner(o)[0]) | (z != owner(o)[1])
        return away if half is None else away | (h != half)

    me_o = lax.div(a, s.stride) * s.per + z - s.base
    is_owner = (lax.rem(a, s.stride) == 0) & (z >= s.base) & (z < s.base + s.per)
    batches = [(0, nq - 1), (nq - 1, nq)] if nq > 1 else [(0, nq)]
    final = len(batches) - 1

    def r2_copy(batch, half, o, sender):
        lo, hi = batches[batch]
        return send(raw.at[lo:hi, half, o], rx2.at[sender, lo:hi],
                    r2s.at[batch], r2r.at[batch], (*owner(o), half))

    def r2_start(batch):
        for half in range(nh):
            for o in range(s.no):
                @pl.when(other(o, half))
                def _(half=half, o=o):
                    r2_copy(batch, half, o, me_t).start()

    def r3_copy(batch, o, step):
        lo, hi = batches[batch]
        ref = rx3.at[o, lo:hi]
        return send(ref, ref, r3s.at[batch], r3r.at[batch], at_n(lax.rem(me_n + step, s.naz)))

    def sq_copy(slot, step):
        ref = sq.at[slot]
        return send(ref, ref, qs, qr, at_t(lax.rem(me_t + step, total)))

    def r2_sum(batch):
        lo, hi = batches[batch]

        @pl.when(is_owner)
        def _():
            def one(step, mine):
                return mine + rx2[lax.rem(me_t + step, total), lo:hi]
            sent(rx2.at[pl.ds(0, total - 1), lo:hi], r2r.at[batch])
            rx3[me_o, lo:hi] = lax.fori_loop(1, total, one, raw[lo:hi, h, me_o])
            for step in range(1, s.naz):
                r3_copy(batch, me_o, step).start()
            if batch == final:
                slot = h * s.no + me_o
                found = rx3[me_o].reshape(nq * s.rs, d)
                sq[slot] = jnp.sum(found * found, axis=0, keepdims=True)
                for step in range(1, total):
                    sq_copy(slot, step).start()

    def at_role(wait):
        @pl.when(is_owner)
        def _():
            wait(1)

        @pl.when(jnp.logical_not(is_owner))
        def _():
            wait(0)

    def r3_wait(batch):
        lo, hi = batches[batch]
        at_role(lambda own: sent(rx2.at[pl.ds(0, s.no - own), lo:hi], r3r.at[batch]))

    def sq_wait():
        at_role(lambda own: sent(sq.at[pl.ds(0, nh * s.no - own)], qr))

    def gather(q, b):
        def came(count):
            sent(gr.at[:, pl.ds(0, count * cq), pl.ds(0, br)], grecv.at[q, b])

        if direct(q):
            @pl.when(is_end)
            def _():
                came(g_n)

            @pl.when(jnp.logical_not(is_end))
            def _():
                came(g_n - 1)
        else:
            came(g_n - 1)

        def spread(n, carry):
            for side in range(2):
                tile = gr[side, q * nc + n, b * br:(b + 1) * br, :].astype(F32)
                turn[side, pl.ds(pl.multiple_of(n * s.tp, 8), br), :] = tile
            return carry
        lax.fori_loop(0, nc, spread, 0, unroll=4)
        if b == 0:
            raw[q] = jnp.zeros((nh, s.no, s.rs, d), F32)

        def one(sub, carry):
            t0 = b * (br // 2) + sub * s.tb
            terms = []
            for side in range(2):
                both = jnp.concatenate(
                    [turn[side, pl.ds(2 * s.tb * sub + e, nc, stride=s.tp), :] for e in range(2 * s.tb)], axis=1)
                for w in range(2):
                    factor = jnp.concatenate([fac[t0 + u, q, 2 * side + w] for u in range(s.tb)], axis=1)
                    terms.append((both * factor.astype(F32)).astype(BF16))
            grads = jnp.concatenate(
                [term[half * m:(half + 1) * m] for half in range(nh) for term in terms], axis=0)
            normed = jnp.concatenate([nt_s[t0 + u] for u in range(s.tb)], axis=1)
            raw[q] += dot(grads, normed, NT).reshape(nh, s.no, s.rs, d)
            part = dot(wt[q], grads, NN)
            for u in range(s.tb):
                piece = part[:, u * 2 * k:(u + 1) * 2 * k]
                ng[t0 + u] = ng[t0 + u] + piece if q else piece
            return carry
        lax.fori_loop(0, br // 2 // s.tb, one, 0)

    def norm_back(b):
        def one(sub, carry):
            t = b * (br // 2) + sub
            unit = unit_s[t]
            scaled = ng[t] * gain[...]
            first = jnp.mean(scaled, axis=0, keepdims=True)
            second = jnp.mean(scaled * unit, axis=0, keepdims=True)
            res = (inv_s[t] * (scaled - first - unit * second)).astype(BF16)
            for e in range(2):
                outv[2 * t + e] = dot(eye_k, res[:, e * k:(e + 1) * k], NT).astype(BF16)
            return carry
        lax.fori_loop(0, br // 2, one, 0, unroll=2)
        keep_copy(b).start()
        for step in range(1, nh):
            out_copy(b, step).start()

    def lr_wait(q):
        sent(lrs.at[:, pl.ds(0, (g_n - 1) * cq)], lrecv.at[q])

    def g_out(q, b):
        for step in range(1, g_n):
            g_copy(q, b, step).start()
        for side in range(2):
            for r in range(cq):
                gr[side, q * nc + me_g * cq + r, b * br:(b + 1) * br, :] = gs[
                    side, q * cq + r, a * nh + h, b * br:(b + 1) * br, :]

    def g_send(q, b):
        if direct(q):
            @pl.when(jnp.logical_not(is_end))
            def _():
                g_out(q, b)
        else:
            g_out(q, b)

    def make(q):
        if q < q0:
            z_rest(q)
            lr_wait(q)
            triangles(q, lrb, gs, 0)
            return

        @pl.when(is_near)
        def _():
            z_rest(q)
            in_copy(q, outward).wait_recv()
            triangles(q, lrh, gsh, q0)
            for b in range(nb):
                if direct(q):
                    for step in range(g_n):
                        direct_copy(q, b, step).start()
                else:
                    back_copy(q, b, outward).start()
            lr_wait(q)
            triangles(q, lrb, gs, 0)

        @pl.when(jnp.logical_not(is_near | is_end))
        def _():
            z_rest(q)
            lr_wait(q)
            triangles(q, lrb, gs, 0)

    def came_back(q, b):
        if q >= q0 and not direct(q):
            @pl.when(is_end)
            def _():
                back_copy(q, b, outward).wait_recv()

    for hop in range(1, nz - 1):
        for q in range(q0):
            z_forward(q, hop)
        if hop == 1 and q0 < nq:
            @pl.when(jnp.logical_not(is_end))
            def _():
                z_own(q0)
    for q in range(q0, nq):
        for hop in range(1, nz - 1):
            z_forward(q, hop)
        if q + 1 < nq:
            @pl.when(jnp.logical_not(is_end))
            def _(q=q):
                z_own(q + 1)

    @pl.when(is_end)
    def _():
        for q in range(q0, nq):
            lr_wait(q)
            in_copy(q, inward).start()

    def drain():
        for step in range(1, nh):
            w_copy(step).wait_send()
        sent(pt.at[pl.ds(0, (na - 1) * s.cp)], psend)
        sent(lrs.at[:, pl.ds(0, (g_n - 1) * nq * cq)], lsend)
        for q in range(nq):
            if direct(q):
                @pl.when(jnp.logical_not(is_end))
                def _(q=q):
                    sent(gs.at[:, pl.ds(q * cq, cq), pl.ds(0, g_n - 1)], gsend.at[q])
            else:
                sent(gs.at[:, pl.ds(q * cq, cq), pl.ds(0, g_n - 1)], gsend.at[q])
            for count in range(1, nz):
                @pl.when((z + 1 == count) & goes_up(q))
                def _(q=q, count=count):
                    sent(pg.at[pl.ds(0, count), pl.ds(q * cq, cq)], zsend.at[q, 0])

                @pl.when((nz - z == count) & goes_down(q))
                def _(q=q, count=count):
                    sent(pg.at[pl.ds(0, count), pl.ds(q * cq, cq)], zsend.at[q, 1])
        if q0 < nq:
            @pl.when(is_end)
            def _():
                sent(lrh, hls)

            @pl.when(is_near)
            def _():
                sent(gsh, hgs)

    last = nq - 1
    queue = []

    def run(count):
        for _ in range(min(count, len(queue))):
            q, b = queue.pop(0)
            gather(q, b)
            if b == nb - 1 and q == last - 1:
                r2_start(0)
            if b == nb - 1 and q == last:
                r2_start(final)

    for q in range(nq):
        make(q)
        if q > 1:
            queue += [(q - 2, b) for b in range(nb)]
        if q == last:
            queue += [(last - 1, b) for b in range(nb)] if q else []
            run(max(len(queue) - 2 * nb, 0))
        for b in range(nb):
            run(1 if q < last else 0)
            came_back(q, b)
            g_send(q, b)
            if q == last:
                run(3 if b < nb - 1 else 0)
                if b:
                    queue.append((last, b - 1))
    queue.append((last, nb - 1))
    run(max(len(queue) - 1, 0))
    if nb > 1:
        norm_back(0)
    run(1)
    waiting = list(range(len(batches)))
    for b in range(1 if nb > 1 else 0, nb):
        if len(waiting) > 1:
            r2_sum(waiting.pop(0))
        norm_back(b)
    for batch in waiting:
        r2_sum(batch)
    drain()
    for batch in range(len(batches)):
        r3_wait(batch)
    found_out = pltpu.make_async_copy(rx3, found_hbm, leave.at[0])
    found_out.start()
    sq_wait()
    sq_out = pltpu.make_async_copy(sq.at[pl.ds(0, nh * s.no)], sq_hbm, leave.at[1])
    sq_out.start()
    for b in range(nb):
        keep_copy(b).wait()
        for step in range(1, nh):
            out_copy(b, step).wait()
    for batch, (lo, hi) in enumerate(batches):
        @pl.when(is_owner)
        def _(batch=batch, lo=lo, hi=hi):
            sent(rx2.at[pl.ds(0, nh * s.no - 1), lo:hi], r2s.at[batch])
            sent(rx2.at[pl.ds(0, s.naz - 1), lo:hi], r3s.at[batch])

        @pl.when(jnp.logical_not(is_owner))
        def _(batch=batch, lo=lo, hi=hi):
            sent(rx2.at[pl.ds(0, nh * s.no), lo:hi], r2s.at[batch])

    @pl.when(is_owner)
    def _():
        sent(sq.at[pl.ds(0, total - 1)], qs)
    found_out.wait()
    sq_out.wait()


def finish(s, blocks, from_hbm, found_ref, sq_ref, out_hbm, wg_ref, held, sem_in, sem_out):
    size = held.shape[0] // blocks

    def came(b):
        at = pl.ds(b * size, size)
        return pltpu.make_async_copy(from_hbm.at[at], held.at[at], sem_in.at[b])

    def leaves(b):
        at = pl.ds(b * size, size)
        return pltpu.make_async_copy(held.at[at], out_hbm.at[at], sem_out.at[b])

    for b in range(blocks):
        came(b).start()
    squares = jnp.sum(jnp.sum(sq_ref[...], axis=0), axis=1, keepdims=True)
    factor = jnp.minimum(1.0, CLIP_LIMIT * lax.rsqrt(squares + 1e-06))
    for q in range(s.nq):
        for o in range(s.no):
            w, at = o * s.rs // s.m, q * s.m + o * s.rs % s.m
            wg_ref[w, at:at + s.rs, :] = found_ref[o, q] * factor
    for b in range(blocks):
        came(b).wait()
        leaves(b).start()
    for b in range(blocks):
        leaves(b).wait()


def on_device(na, nz, nh, pair_rep, norm_gain, weights, residue_mask, product_grad):
    rows, cols, depth = pair_rep.shape
    ch = product_grad.shape[1]
    s = Sizes(na, nz, nh, rows, cols, depth, ch)
    vm = pl.BlockSpec(memory_space=pltpu.VMEM)
    anywhere = pl.BlockSpec(memory_space=pl.ANY)
    dma = pltpu.SemaphoreType.DMA
    half = s.rh // 2
    scratch = [
        pltpu.VMEM((s.rh, cols, depth), BF16),
        pltpu.VMEM((rows, ch, cols), BF16),
        pltpu.VMEM((ch, rows, cols), BF16),
        pltpu.VMEM((nz, s.cp, s.i, cols), BF16),
        pltpu.VMEM((nh, 4, ch, depth), BF16),
        pltpu.VMEM((s.nq, depth, 4 * s.nc), BF16),
        pltpu.VMEM((depth, 2 * cols), F32),
        pltpu.VMEM((half, depth, 2 * cols), F32),
        pltpu.VMEM((half, 1, 2 * cols), F32),
        pltpu.VMEM((half, depth, 2 * cols), BF16),
        pltpu.VMEM((4 * s.hid, 2 * cols), F32),
        pltpu.VMEM((half, s.nq, 4, s.nc, 2 * cols), BF16),
        pltpu.VMEM((2, max(s.br * s.sp, s.bi * s.pp), cols), F32),
        pltpu.VMEM((2, s.hid, s.rh, cols), BF16),
        pltpu.VMEM((2, s.cp, s.i, cols), BF16),
        pltpu.VMEM((2, s.helped * s.cq, s.i, cols), BF16),
        pltpu.VMEM((2, s.cp, s.g, s.rh, cols), BF16),
        pltpu.VMEM((2, s.helped * s.cq, s.g, s.rh, cols), BF16),
        pltpu.VMEM((2, s.hid, s.rh, cols), BF16),
        pltpu.VMEM((2, s.nc * s.tp, cols), F32),
        pltpu.VMEM((half, depth, 2 * cols), F32),
        pltpu.VMEM((s.rh, cols, depth), BF16),
        pltpu.VMEM((s.nq, nh, s.no, s.rs, depth), F32),
        pltpu.VMEM((s.naz * nh, s.nq, s.rs, depth), F32),
        pltpu.VMEM((s.no, s.nq, s.rs, depth), F32),
        pltpu.VMEM((s.naz * nh, 1, depth), F32),
        dma(()), dma((s.nq,)), dma((nh,)), dma((nh,)),
        dma(()), dma((s.cq + s.nq,)), dma((s.nq, 2)), dma((s.cq + s.nq, nz)),
        dma(()), dma((s.nq,)), dma((s.nq,)), dma((s.nq, s.nb)),
        dma((s.nb, nh)), dma((s.nb, nh)),
        dma((2,)), dma((2,)), dma((2,)), dma((2,)),
        dma(()), dma(()), dma((s.nb,)), dma((2,)),
        dma(()), dma((s.helped,)), dma(()), dma((s.helped, s.nb)),
    ]
    grad, found, squares = pl.pallas_call(
        functools.partial(kernel, s),
        out_shape=(
            jax.ShapeDtypeStruct((rows, cols, depth), BF16),
            jax.ShapeDtypeStruct((s.no, s.nq, s.rs, depth), F32),
            jax.ShapeDtypeStruct((nh * s.no, 1, depth), F32),
        ),
        in_specs=[anywhere, anywhere, vm, vm, vm, pl.BlockSpec(memory_space=pltpu.SMEM)],
        out_specs=(anywhere, anywhere, anywhere),
        scratch_shapes=scratch,
        compiler_params=pltpu.CompilerParams(
            collective_id=0, has_side_effects=True, vmem_limit_bytes=VMEM_LIMIT),
    )(product_grad, pair_rep, weights.transpose(0, 2, 1), norm_gain.reshape(1, depth),
      residue_mask.reshape(nz, cols), residue_mask)
    blocks = math.gcd(rows, 4)
    pair_grad, weight_grads = pl.pallas_call(
        functools.partial(finish, s, blocks),
        out_shape=(
            jax.ShapeDtypeStruct((rows, cols, depth), BF16),
            jax.ShapeDtypeStruct((4, ch, depth), F32),
        ),
        in_specs=[pl.BlockSpec(memory_space=pl.ANY), vm, vm],
        out_specs=(pl.BlockSpec(memory_space=pl.ANY), vm),
        scratch_shapes=[pltpu.VMEM((rows, cols, depth), BF16), dma((blocks,)), dma((blocks,))],
    )(grad, found, squares)
    return (pair_grad, weight_grads.transpose(0, 2, 1))


def solution(mesh):
    sizes = mesh.shape["ia"], mesh.shape["ja"], mesh.shape["col"]
    placed = (P("ia", "ja", None), P(), P(None, None, "col"), P(), P("ia", "col", "ja"))

    def step(*args):
        return on_device(*sizes, *args)

    return jax.shard_map(
        step,
        mesh=mesh,
        in_specs=placed,
        out_specs=(P("ia", "ja", None), P(None, None, "col")),
        check_vma=False,
    )
```

```python
import functools
import math

import jax
import jax.numpy as jnp
from jax import lax
from jax.experimental import pallas as pl
from jax.experimental.pallas import tpu as pltpu
from jax.sharding import PartitionSpec as P

CLIP_LIMIT = 64.0
MAX_CHUNKS = 4
ROWS_AT_ONCE = 2
VMEM_LIMIT = 66 * 1000 * 1000
MESH = pl.DeviceIdType.MESH
NT = (((1,), (1,)), ((), ()))
NN = (((1,), (0,)), ((), ()))
F32 = jnp.float32
BF16 = jnp.bfloat16


def dot(a, b, dims):
    return lax.dot_general(a, b, dims, preferred_element_type=F32)


def eye(n):
    rows = lax.broadcasted_iota(jnp.int32, (n, n), 0)
    cols = lax.broadcasted_iota(jnp.int32, (n, n), 1)
    return jnp.where(rows == cols, 1.0, 0.0).astype(BF16)


class Sizes:
    def __init__(self, na, nz, nh, rows, cols, depth, ch):
        self.na, self.nz, self.nh = na, nz, nh
        self.rb, self.k, self.d, self.ch = rows, cols, depth, ch
        self.g = na * nh
        self.naz = na * nz
        self.rh = rows // nh
        self.hid = ch * nh
        self.cp = ch // na
        self.nq = math.gcd(self.cp, MAX_CHUNKS)
        self.cq = self.cp // self.nq
        self.m = na * self.cq
        self.nc = self.g * self.cq
        self.i = na * rows
        self.br = math.gcd(self.rh, 16)
        self.nb = self.rh // self.br
        self.bi = math.gcd(self.rb, 16)
        self.sp = self.hid + 8
        self.pp = self.m + 8
        self.tp = self.br + 8
        self.tb = math.gcd(self.br // 2, ROWS_AT_ONCE)
        self.no = math.gcd(max(4 * self.m // 8, 1), self.naz)
        self.rs = 4 * self.m // self.no
        self.per = max(self.no // na, 1)
        self.stride = na * self.per // self.no
        self.base = (nz - self.per) // 2
        self.q0 = self.nq - self.nq // 2 if nz > 3 else self.nq
        self.helped = max(self.nq - self.q0, 1)


def kernel(s, p_hbm, x_hbm, w_ref, gain_ref, mask_ref, mask_s, out_hbm, found_hbm, sq_hbm,
           xv, p_ref, pt, pg, wall, wt, gain, unit_s, inv_s, nt_s, pr, fac, relay, lrs, lrb, lrh, gs, gsh, gr, turn, ng,
           outv, raw, rx2, rx3, sq,
           xsem, pin, wsend, wrecv, psend, precv, zsend, zrecv, lsend, lrecv, gsend, grecv, osend, orecv,
           r2s, r2r, r3s, r3r, qs, qr, keep, leave, hls, hlr, hgs, hgr):
    na, nz, nh, g_n, nq, cq, nc = s.na, s.nz, s.nh, s.g, s.nq, s.cq, s.nc
    rb, rh, k, d, ch, hid, br, nb, m = s.rb, s.rh, s.k, s.d, s.ch, s.hid, s.br, s.nb, s.m
    a, z, h = lax.axis_index("ia"), lax.axis_index("ja"), lax.axis_index("col")
    me_g = h * na + a
    me_n = a * nz + z
    row0 = a * rb + h * rh
    q0 = s.q0
    is_end = (z == 0) | (z == nz - 1)
    is_near = (z == 1) | (z == nz - 2)
    inward = jnp.where(z == 0, 1, nz - 2)
    outward = jnp.where(z == 1, 0, nz - 1)

    def plane(g):
        return (lax.rem(g, na), z, lax.div(g, na))

    def peer_g(step):
        return lax.rem(me_g + step, g_n)

    def sent(ref, sem):
        pltpu.make_async_copy(ref, ref, sem).wait()

    def send(src, dst, send_sem, recv_sem, device):
        return pltpu.make_async_remote_copy(
            src_ref=src, dst_ref=dst, send_sem=send_sem, recv_sem=recv_sem,
            device_id=device, device_id_type=MESH)

    barrier = pltpu.get_barrier_semaphore()
    total = s.naz * nh
    me_t = me_n * nh + h

    def at_t(t):
        return (lax.div(t, nz * nh), lax.rem(lax.div(t, nh), nz), lax.rem(t, nh))

    def p_in(q):
        at = pl.ds(q * m, m)
        return pltpu.make_async_copy(p_hbm.at[:, at], p_ref.at[:, at], pin.at[q])

    for q in range(nq):
        p_in(q).start()
    for step in range(1, total):
        pl.semaphore_signal(barrier, inc=1, device_id=at_t(lax.rem(me_t + step, total)), device_id_type=MESH)
    xcopy = pltpu.make_async_copy(x_hbm.at[pl.ds(h * rh, rh)], xv, xsem)
    xcopy.start()

    def p_turn(q):
        p_in(q).wait()

        def block(ib, carry):
            slot = lax.rem(ib, 2)
            for ii in range(s.bi):
                relay[slot, ii * s.pp:ii * s.pp + m, :] = p_ref[ib * s.bi + ii, q * m:(q + 1) * m, :].astype(F32)
            for c in range(m):
                tile = relay[slot, pl.ds(c, s.bi, stride=s.pp), :]
                pt[q * m + c, pl.ds(pl.multiple_of(ib * s.bi, s.bi), s.bi), :] = tile.astype(BF16)
            return carry
        lax.fori_loop(0, rb // s.bi, block, 0)

    def pieces(q):
        return [(q * cq + r, 1) for r in range(cq)] if q == 0 else [(q * cq, cq)]

    def spot(c):
        return c if c < cq else cq - 1 + c // cq

    def p_copy(piece, step):
        c, n = piece
        to = lax.rem(a + step, na)
        return send(pt.at[pl.ds((c // cq) * m + to * cq + c % cq, n)], pg.at[z, pl.ds(c, n), pl.ds(a * rb, rb)],
                    psend, precv.at[spot(c)], (to, z, h))

    def w_copy(step):
        return send(w_ref, wall.at[h], wsend.at[step], wrecv.at[step], (a, z, lax.rem(h + step, nh)))

    p_turn(0)
    pl.semaphore_wait(barrier, total - 1)
    for step in range(1, nh):
        w_copy(step).start()
    for q in range(nq):
        if q:
            p_turn(q)
        for piece in pieces(q):
            for step in range(1, na):
                p_copy(piece, step).start()
    for q in range(nq):
        for r in range(cq):
            pg[z, q * cq + r, pl.ds(a * rb, rb), :] = pt[q * m + a * cq + r]

    def z_copy(piece, block, up):
        c, n = piece
        ref = pg.at[block, pl.ds(c, n)]
        return send(ref, ref, zsend.at[c // cq, 0 if up else 1], zrecv.at[spot(c), block],
                    (a, z + 1 if up else z - 1, h))

    def goes_up(q):
        return z < (nz - 1 if q < q0 else nz - 2)

    def goes_down(q):
        return z > (0 if q < q0 else 1)

    def z_own(q, some=None):
        for piece in some or pieces(q):
            sent(pt.at[pl.ds(0, (na - 1) * piece[1])], precv.at[spot(piece[0])])

            @pl.when(goes_up(q))
            def _(piece=piece):
                z_copy(piece, z, True).start()

            @pl.when(goes_down(q))
            def _(piece=piece):
                z_copy(piece, z, False).start()

    def z_forward(q, hop):
        @pl.when((z >= hop) & goes_up(q))
        def _():
            for piece in pieces(q):
                z_copy(piece, z - hop, True).wait_recv()
                z_copy(piece, z - hop, True).start()

        @pl.when((z + hop < nz) & goes_down(q))
        def _():
            for piece in pieces(q):
                z_copy(piece, z + hop, False).wait_recv()
                z_copy(piece, z + hop, False).start()

    def z_rest(q):
        for hop in range(1, nz):
            here = True if q < q0 else jnp.logical_not(is_end)

            @pl.when((z >= hop) & jnp.logical_not(goes_up(q)) & here)
            def _(hop=hop):
                for piece in pieces(q):
                    z_copy(piece, z - hop, True).wait_recv()

            @pl.when((z + hop < nz) & jnp.logical_not(goes_down(q)) & here)
            def _(hop=hop):
                for piece in pieces(q):
                    z_copy(piece, z + hop, False).wait_recv()

    eye_d = eye(d)
    column = jnp.transpose(jnp.broadcast_to(gain_ref[...], (k, d)))
    gain[...] = jnp.concatenate([column, column], axis=1)
    wall[h] = w_ref[...]
    for step in range(1, nh):
        w_copy(step).wait_recv()
    for q in range(nq):
        rows = [wall[half, w, q * m:(q + 1) * m, :] for half in range(nh) for w in range(4)]
        wt[q] = dot(eye_d, jnp.concatenate(rows, axis=0), NT).astype(BF16)

    xcopy.wait()
    col_valid = mask_ref[pl.ds(z, 1), :].astype(F32)

    def rows_step(t, sub):
        x2 = xv[pl.ds(2 * t, 2)].reshape(2 * k, d)
        xt = dot(eye_d, x2, NT)
        centred = xt - jnp.mean(xt, axis=0, keepdims=True)
        inv = lax.rsqrt(jnp.mean(centred * centred, axis=0, keepdims=True) + 1e-05)
        unit = centred * inv
        normed = (unit * gain[...]).astype(BF16)
        unit_s[t] = unit
        inv_s[t] = inv
        nt_s[t] = normed
        for half in range(nh):
            pr[half * 4 * ch:(half + 1) * 4 * ch, :] = dot(wall[half].reshape(4 * ch, d), normed, NN)
        valid = jnp.concatenate(
            [col_valid * mask_s[row0 + 2 * t + e].astype(F32) for e in range(2)], axis=1)
        for q in range(nq):
            for side in range(2):
                def part(w):
                    at = [half * 4 * ch + w * ch + q * m for half in range(nh)]
                    return jnp.concatenate([pr[x:x + m, :] for x in at], axis=0)
                lin = part(2 * side)
                gate = jax.nn.sigmoid(part(2 * side + 1))
                first = valid * gate
                value = first * lin
                fac[t, q, 2 * side] = first.astype(BF16)
                fac[t, q, 2 * side + 1] = (value * (1.0 - gate)).astype(BF16)
                for e in range(2):
                    at = pl.multiple_of((2 * sub + e) * s.sp, 8) + q * nc
                    relay[side, pl.ds(at, nc), :] = value[:, e * k:(e + 1) * k]

    for b in range(nb):
        def one(sub, carry, b=b):
            rows_step(b * (br // 2) + sub, sub)
            return carry
        parts = pieces(0) if b == 0 else [None]
        each = br // 2 // len(parts)
        if each * len(parts) * 2 == br:
            for n, piece in enumerate(parts):
                lax.fori_loop(n * each, (n + 1) * each, one, 0)
                if piece:
                    z_own(0, [piece])
        else:
            lax.fori_loop(0, br // 2, one, 0)
            if b == 0:
                z_own(0)

        def flush(c, carry, b=b):
            for side in range(2):
                tile = relay[side, pl.ds(c, br, stride=s.sp), :]
                lrs[side, c, b * br:(b + 1) * br, :] = tile.astype(BF16)
            return carry
        lax.fori_loop(0, hid, flush, 0, unroll=4)
        if 0 < b < q0:
            z_own(b)
    for q in range(nb, q0):
        z_own(q)

    if q0 < nq:
        @pl.when(is_end)
        def _():
            z_own(q0)

    def lr_copy(q, step):
        return send(lrs.at[:, pl.ds(q * nc + peer_g(step) * cq, cq)],
                    lrb.at[:, pl.ds(q * cq, cq), pl.ds(row0, rh)],
                    lsend, lrecv.at[q], plane(peer_g(step)))

    for q in [*range(q0, nq), *range(q0)]:
        for step in range(1, g_n):
            lr_copy(q, step).start()
    for q in range(nq):
        for side in range(2):
            for r in range(cq):
                lrb[side, q * cq + r, pl.ds(row0, rh), :] = lrs[side, q * nc + me_g * cq + r]

    eye_k = eye(k)

    def triangle(c, lr, at, to):
        panel = jnp.concatenate([pg[b, c] for b in range(nz)], axis=1)
        left, right = lr[0, at], lr[1, at]
        to[0, at] = dot(panel, right, NN).astype(BF16).reshape(g_n, rh, k)
        left_t = dot(eye_k, left, NT).astype(BF16)
        back_t = dot(left_t, panel, NN).astype(BF16)
        back = [dot(eye_k, back_t[:, b * k:(b + 1) * k], NT).astype(BF16) for b in range(nz)]
        to[1, at] = jnp.concatenate(back, axis=0).reshape(g_n, rh, k)

    def triangles(q, lr, to, base):
        def one(r, carry):
            triangle(q * cq + r, lr, (q - base) * cq + r, to)
            return carry
        lax.fori_loop(0, cq, one, 0)

    def in_copy(q, z_to):
        return send(lrb.at[:, pl.ds(q * cq, cq)], lrh.at[:, pl.ds((q - q0) * cq, cq)],
                    hls, hlr.at[q - q0], (a, z_to, h))

    def g_copy(q, b, step):
        g = peer_g(step)
        place = lax.rem(g, na) * nh + lax.div(g, na)
        return send(gs.at[:, pl.ds(q * cq, cq), place, pl.ds(b * br, br)],
                    gr.at[:, pl.ds(q * nc + me_g * cq, cq), pl.ds(b * br, br)],
                    gsend.at[q], grecv.at[q, b], plane(g))

    def back_copy(q, b, z_to):
        return send(gsh.at[:, pl.ds((q - q0) * cq, cq), :, pl.ds(b * br, br)],
                    gs.at[:, pl.ds(q * cq, cq), :, pl.ds(b * br, br)],
                    hgs, hgr.at[q - q0, b], (a, z_to, h))

    def direct(q):
        return q == nq - 1 and q >= q0

    def direct_copy(q, b, step):
        g = peer_g(step)
        place = lax.rem(g, na) * nh + lax.div(g, na)
        return send(gsh.at[:, pl.ds((q - q0) * cq, cq), place, pl.ds(b * br, br)],
                    gr.at[:, pl.ds(q * nc + me_g * cq, cq), pl.ds(b * br, br)],
                    hgs, grecv.at[q, b], (lax.rem(g, na), outward, lax.div(g, na)))

    def out_copy(b, step):
        return send(outv.at[pl.ds(b * br, br)], out_hbm.at[pl.ds(h * rh + b * br, br)],
                    osend.at[b, step], orecv.at[b, step], (a, z, lax.rem(h + step, nh)))

    def keep_copy(b):
        return pltpu.make_async_copy(
            outv.at[pl.ds(b * br, br)], out_hbm.at[pl.ds(h * rh + b * br, br)], keep.at[b])

    def at_n(n):
        return (lax.div(n, nz), lax.rem(n, nz), h)

    def owner(o):
        return (o // s.per * s.stride, s.base + o % s.per)

    def other(o, half=None):
        away = (a != owner(o)[0]) | (z != owner(o)[1])
        return away if half is None else away | (h != half)

    me_o = lax.div(a, s.stride) * s.per + z - s.base
    is_owner = (lax.rem(a, s.stride) == 0) & (z >= s.base) & (z < s.base + s.per)
    batches = [(0, nq - 1), (nq - 1, nq)] if nq > 1 else [(0, nq)]
    final = len(batches) - 1

    def r2_copy(batch, half, o, sender):
        lo, hi = batches[batch]
        return send(raw.at[lo:hi, half, o], rx2.at[sender, lo:hi],
                    r2s.at[batch], r2r.at[batch], (*owner(o), half))

    def r2_start(batch):
        for half in range(nh):
            for o in range(s.no):
                @pl.when(other(o, half))
                def _(half=half, o=o):
                    r2_copy(batch, half, o, me_t).start()

    def r3_copy(batch, o, step):
        lo, hi = batches[batch]
        ref = rx3.at[o, lo:hi]
        return send(ref, ref, r3s.at[batch], r3r.at[batch], at_n(lax.rem(me_n + step, s.naz)))

    def sq_copy(slot, step):
        ref = sq.at[slot]
        return send(ref, ref, qs, qr, at_t(lax.rem(me_t + step, total)))

    def r2_sum(batch):
        lo, hi = batches[batch]

        @pl.when(is_owner)
        def _():
            def one(step, mine):
                return mine + rx2[lax.rem(me_t + step, total), lo:hi]
            sent(rx2.at[pl.ds(0, total - 1), lo:hi], r2r.at[batch])
            rx3[me_o, lo:hi] = lax.fori_loop(1, total, one, raw[lo:hi, h, me_o])
            for step in range(1, s.naz):
                r3_copy(batch, me_o, step).start()
            if batch == final:
                slot = h * s.no + me_o
                found = rx3[me_o].reshape(nq * s.rs, d)
                sq[slot] = jnp.sum(found * found, axis=0, keepdims=True)
                for step in range(1, total):
                    sq_copy(slot, step).start()

    def at_role(wait):
        @pl.when(is_owner)
        def _():
            wait(1)

        @pl.when(jnp.logical_not(is_owner))
        def _():
            wait(0)

    def r3_wait(batch):
        lo, hi = batches[batch]
        at_role(lambda own: sent(rx2.at[pl.ds(0, s.no - own), lo:hi], r3r.at[batch]))

    def sq_wait():
        at_role(lambda own: sent(sq.at[pl.ds(0, nh * s.no - own)], qr))

    def gather(q, b):
        def came(count):
            sent(gr.at[:, pl.ds(0, count * cq), pl.ds(0, br)], grecv.at[q, b])

        if direct(q):
            @pl.when(is_end)
            def _():
                came(g_n)

            @pl.when(jnp.logical_not(is_end))
            def _():
                came(g_n - 1)
        else:
            came(g_n - 1)

        def spread(n, carry):
            for side in range(2):
                tile = gr[side, q * nc + n, b * br:(b + 1) * br, :].astype(F32)
                turn[side, pl.ds(pl.multiple_of(n * s.tp, 8), br), :] = tile
            return carry
        lax.fori_loop(0, nc, spread, 0, unroll=4)
        if b == 0:
            raw[q] = jnp.zeros((nh, s.no, s.rs, d), F32)

        def one(sub, carry):
            t0 = b * (br // 2) + sub * s.tb
            terms = []
            for side in range(2):
                both = jnp.concatenate(
                    [turn[side, pl.ds(2 * s.tb * sub + e, nc, stride=s.tp), :] for e in range(2 * s.tb)], axis=1)
                for w in range(2):
                    factor = jnp.concatenate([fac[t0 + u, q, 2 * side + w] for u in range(s.tb)], axis=1)
                    terms.append((both * factor.astype(F32)).astype(BF16))
            grads = jnp.concatenate(
                [term[half * m:(half + 1) * m] for half in range(nh) for term in terms], axis=0)
            normed = jnp.concatenate([nt_s[t0 + u] for u in range(s.tb)], axis=1)
            raw[q] += dot(grads, normed, NT).reshape(nh, s.no, s.rs, d)
            part = dot(wt[q], grads, NN)
            for u in range(s.tb):
                piece = part[:, u * 2 * k:(u + 1) * 2 * k]
                ng[t0 + u] = ng[t0 + u] + piece if q else piece
            return carry
        lax.fori_loop(0, br // 2 // s.tb, one, 0)

    def norm_back(b):
        def one(sub, carry):
            t = b * (br // 2) + sub
            unit = unit_s[t]
            scaled = ng[t] * gain[...]
            first = jnp.mean(scaled, axis=0, keepdims=True)
            second = jnp.mean(scaled * unit, axis=0, keepdims=True)
            res = (inv_s[t] * (scaled - first - unit * second)).astype(BF16)
            for e in range(2):
                outv[2 * t + e] = dot(eye_k, res[:, e * k:(e + 1) * k], NT).astype(BF16)
            return carry
        lax.fori_loop(0, br // 2, one, 0, unroll=2)
        keep_copy(b).start()
        for step in range(1, nh):
            out_copy(b, step).start()

    def lr_wait(q):
        sent(lrs.at[:, pl.ds(0, (g_n - 1) * cq)], lrecv.at[q])

    def g_out(q, b):
        for step in range(1, g_n):
            g_copy(q, b, step).start()
        for side in range(2):
            for r in range(cq):
                gr[side, q * nc + me_g * cq + r, b * br:(b + 1) * br, :] = gs[
                    side, q * cq + r, a * nh + h, b * br:(b + 1) * br, :]

    def g_send(q, b):
        if direct(q):
            @pl.when(jnp.logical_not(is_end))
            def _():
                g_out(q, b)
        else:
            g_out(q, b)

    def help_end(q):
        @pl.when(is_near)
        def _():
            z_rest(q)
            in_copy(q, outward).wait_recv()
            triangles(q, lrh, gsh, q0)
            for b in range(nb):
                if direct(q):
                    for step in range(g_n):
                        direct_copy(q, b, step).start()
                else:
                    back_copy(q, b, outward).start()

    def make(q):
        if q < q0:
            z_rest(q)
            lr_wait(q)
            triangles(q, lrb, gs, 0)
            return

        @pl.when(jnp.logical_not(is_near | is_end))
        def _():
            z_rest(q)

        @pl.when(jnp.logical_not(is_end))
        def _():
            lr_wait(q)
            triangles(q, lrb, gs, 0)

    def came_back(q, b):
        if q >= q0 and not direct(q):
            @pl.when(is_end)
            def _():
                back_copy(q, b, outward).wait_recv()

    for hop in range(1, nz - 1):
        for q in range(q0):
            z_forward(q, hop)
        if hop == 1 and q0 < nq:
            @pl.when(jnp.logical_not(is_end))
            def _():
                z_own(q0)
    for q in range(q0, nq):
        for hop in range(1, nz - 1):
            z_forward(q, hop)
        if q + 1 < nq:
            @pl.when(jnp.logical_not(is_end))
            def _(q=q):
                z_own(q + 1)

    @pl.when(is_end)
    def _():
        for q in range(q0, nq):
            lr_wait(q)
            in_copy(q, inward).start()
            if q + 1 < nq:
                z_own(q + 1)

    def drain():
        for step in range(1, nh):
            w_copy(step).wait_send()
        sent(pt.at[pl.ds(0, (na - 1) * s.cp)], psend)
        sent(lrs.at[:, pl.ds(0, (g_n - 1) * nq * cq)], lsend)
        for q in range(nq):
            if direct(q):
                @pl.when(jnp.logical_not(is_end))
                def _(q=q):
                    sent(gs.at[:, pl.ds(q * cq, cq), pl.ds(0, g_n - 1)], gsend.at[q])
            else:
                sent(gs.at[:, pl.ds(q * cq, cq), pl.ds(0, g_n - 1)], gsend.at[q])
            for count in range(1, nz):
                @pl.when((z + 1 == count) & goes_up(q))
                def _(q=q, count=count):
                    sent(pg.at[pl.ds(0, count), pl.ds(q * cq, cq)], zsend.at[q, 0])

                @pl.when((nz - z == count) & goes_down(q))
                def _(q=q, count=count):
                    sent(pg.at[pl.ds(0, count), pl.ds(q * cq, cq)], zsend.at[q, 1])
        if q0 < nq:
            @pl.when(is_end)
            def _():
                sent(lrh, hls)

            @pl.when(is_near)
            def _():
                sent(gsh, hgs)

    last = nq - 1
    queue = []

    def run(count):
        for _ in range(min(count, len(queue))):
            q, b = queue.pop(0)
            gather(q, b)
            if b == nb - 1 and q == last - 1:
                r2_start(0)
            if b == nb - 1 and q == last:
                r2_start(final)

    for q in range(nq):
        if q == q0 - 1 and q0 < nq:
            help_end(q0)
        elif q > q0:
            help_end(q)
        make(q)
        if q > 1:
            queue += [(q - 2, b) for b in range(nb)]
        if q == last:
            queue += [(last - 1, b) for b in range(nb)] if q else []
            run(max(len(queue) - 2 * nb, 0))
        for b in range(nb):
            run(1 if q < last else 0)
            came_back(q, b)
            g_send(q, b)
            if q == last:
                run(3 if b < nb - 1 else 0)
                if b:
                    queue.append((last, b - 1))
    queue.append((last, nb - 1))
    run(max(len(queue) - 1, 0))
    if nb > 1:
        norm_back(0)
    run(1)
    waiting = list(range(len(batches)))
    for b in range(1 if nb > 1 else 0, nb):
        if len(waiting) > 1:
            r2_sum(waiting.pop(0))
        norm_back(b)
    for batch in waiting:
        r2_sum(batch)
    drain()
    for batch in range(len(batches)):
        r3_wait(batch)
    found_out = pltpu.make_async_copy(rx3, found_hbm, leave.at[0])
    found_out.start()
    sq_wait()
    sq_out = pltpu.make_async_copy(sq.at[pl.ds(0, nh * s.no)], sq_hbm, leave.at[1])
    sq_out.start()
    for b in range(nb):
        keep_copy(b).wait()
        for step in range(1, nh):
            out_copy(b, step).wait()
    for batch, (lo, hi) in enumerate(batches):
        @pl.when(is_owner)
        def _(batch=batch, lo=lo, hi=hi):
            sent(rx2.at[pl.ds(0, nh * s.no - 1), lo:hi], r2s.at[batch])
            sent(rx2.at[pl.ds(0, s.naz - 1), lo:hi], r3s.at[batch])

        @pl.when(jnp.logical_not(is_owner))
        def _(batch=batch, lo=lo, hi=hi):
            sent(rx2.at[pl.ds(0, nh * s.no), lo:hi], r2s.at[batch])

    @pl.when(is_owner)
    def _():
        sent(sq.at[pl.ds(0, total - 1)], qs)
    found_out.wait()
    sq_out.wait()


def finish(s, blocks, from_hbm, found_ref, sq_ref, out_hbm, wg_ref, held, sem_in, sem_out):
    size = held.shape[0] // blocks

    def came(b):
        at = pl.ds(b * size, size)
        return pltpu.make_async_copy(from_hbm.at[at], held.at[at], sem_in.at[b])

    def leaves(b):
        at = pl.ds(b * size, size)
        return pltpu.make_async_copy(held.at[at], out_hbm.at[at], sem_out.at[b])

    for b in range(blocks):
        came(b).start()
    squares = jnp.sum(jnp.sum(sq_ref[...], axis=0), axis=1, keepdims=True)
    factor = jnp.minimum(1.0, CLIP_LIMIT * lax.rsqrt(squares + 1e-06))
    for q in range(s.nq):
        for o in range(s.no):
            w, at = o * s.rs // s.m, q * s.m + o * s.rs % s.m
            wg_ref[w, at:at + s.rs, :] = found_ref[o, q] * factor
    for b in range(blocks):
        came(b).wait()
        leaves(b).start()
    for b in range(blocks):
        leaves(b).wait()


def on_device(na, nz, nh, pair_rep, norm_gain, weights, residue_mask, product_grad):
    rows, cols, depth = pair_rep.shape
    ch = product_grad.shape[1]
    s = Sizes(na, nz, nh, rows, cols, depth, ch)
    vm = pl.BlockSpec(memory_space=pltpu.VMEM)
    anywhere = pl.BlockSpec(memory_space=pl.ANY)
    dma = pltpu.SemaphoreType.DMA
    half = s.rh // 2
    scratch = [
        pltpu.VMEM((s.rh, cols, depth), BF16),
        pltpu.VMEM((rows, ch, cols), BF16),
        pltpu.VMEM((ch, rows, cols), BF16),
        pltpu.VMEM((nz, s.cp, s.i, cols), BF16),
        pltpu.VMEM((nh, 4, ch, depth), BF16),
        pltpu.VMEM((s.nq, depth, 4 * s.nc), BF16),
        pltpu.VMEM((depth, 2 * cols), F32),
        pltpu.VMEM((half, depth, 2 * cols), F32),
        pltpu.VMEM((half, 1, 2 * cols), F32),
        pltpu.VMEM((half, depth, 2 * cols), BF16),
        pltpu.VMEM((4 * s.hid, 2 * cols), F32),
        pltpu.VMEM((half, s.nq, 4, s.nc, 2 * cols), BF16),
        pltpu.VMEM((2, max(s.br * s.sp, s.bi * s.pp), cols), F32),
        pltpu.VMEM((2, s.hid, s.rh, cols), BF16),
        pltpu.VMEM((2, s.cp, s.i, cols), BF16),
        pltpu.VMEM((2, s.helped * s.cq, s.i, cols), BF16),
        pltpu.VMEM((2, s.cp, s.g, s.rh, cols), BF16),
        pltpu.VMEM((2, s.helped * s.cq, s.g, s.rh, cols), BF16),
        pltpu.VMEM((2, s.hid, s.rh, cols), BF16),
        pltpu.VMEM((2, s.nc * s.tp, cols), F32),
        pltpu.VMEM((half, depth, 2 * cols), F32),
        pltpu.VMEM((s.rh, cols, depth), BF16),
        pltpu.VMEM((s.nq, nh, s.no, s.rs, depth), F32),
        pltpu.VMEM((s.naz * nh, s.nq, s.rs, depth), F32),
        pltpu.VMEM((s.no, s.nq, s.rs, depth), F32),
        pltpu.VMEM((s.naz * nh, 1, depth), F32),
        dma(()), dma((s.nq,)), dma((nh,)), dma((nh,)),
        dma(()), dma((s.cq + s.nq,)), dma((s.nq, 2)), dma((s.cq + s.nq, nz)),
        dma(()), dma((s.nq,)), dma((s.nq,)), dma((s.nq, s.nb)),
        dma((s.nb, nh)), dma((s.nb, nh)),
        dma((2,)), dma((2,)), dma((2,)), dma((2,)),
        dma(()), dma(()), dma((s.nb,)), dma((2,)),
        dma(()), dma((s.helped,)), dma(()), dma((s.helped, s.nb)),
    ]
    grad, found, squares = pl.pallas_call(
        functools.partial(kernel, s),
        out_shape=(
            jax.ShapeDtypeStruct((rows, cols, depth), BF16),
            jax.ShapeDtypeStruct((s.no, s.nq, s.rs, depth), F32),
            jax.ShapeDtypeStruct((nh * s.no, 1, depth), F32),
        ),
        in_specs=[anywhere, anywhere, vm, vm, vm, pl.BlockSpec(memory_space=pltpu.SMEM)],
        out_specs=(anywhere, anywhere, anywhere),
        scratch_shapes=scratch,
        compiler_params=pltpu.CompilerParams(
            collective_id=0, has_side_effects=True, vmem_limit_bytes=VMEM_LIMIT),
    )(product_grad, pair_rep, weights.transpose(0, 2, 1), norm_gain.reshape(1, depth),
      residue_mask.reshape(nz, cols), residue_mask)
    blocks = math.gcd(rows, 4)
    pair_grad, weight_grads = pl.pallas_call(
        functools.partial(finish, s, blocks),
        out_shape=(
            jax.ShapeDtypeStruct((rows, cols, depth), BF16),
            jax.ShapeDtypeStruct((4, ch, depth), F32),
        ),
        in_specs=[pl.BlockSpec(memory_space=pl.ANY), vm, vm],
        out_specs=(pl.BlockSpec(memory_space=pl.ANY), vm),
        scratch_shapes=[pltpu.VMEM((rows, cols, depth), BF16), dma((blocks,)), dma((blocks,))],
    )(grad, found, squares)
    return (pair_grad, weight_grads.transpose(0, 2, 1))


def solution(mesh):
    sizes = mesh.shape["ia"], mesh.shape["ja"], mesh.shape["col"]
    placed = (P("ia", "ja", None), P(), P(None, None, "col"), P(), P("ia", "col", "ja"))

    def step(*args):
        return on_device(*sizes, *args)

    return jax.shard_map(
        step,
        mesh=mesh,
        in_specs=placed,
        out_specs=(P("ia", "ja", None), P(None, None, "col")),
        check_vma=False,
    )
```

```python
import functools
import math

import jax
import jax.numpy as jnp
from jax import lax
from jax.experimental import pallas as pl
from jax.experimental.pallas import tpu as pltpu
from jax.sharding import PartitionSpec as P

CLIP_LIMIT = 64.0
MAX_CHUNKS = 4
ROWS_AT_ONCE = 2
VMEM_LIMIT = 66 * 1000 * 1000
MESH = pl.DeviceIdType.MESH
NT = (((1,), (1,)), ((), ()))
NN = (((1,), (0,)), ((), ()))
F32 = jnp.float32
BF16 = jnp.bfloat16


def dot(a, b, dims):
    return lax.dot_general(a, b, dims, preferred_element_type=F32)


def eye(n):
    rows = lax.broadcasted_iota(jnp.int32, (n, n), 0)
    cols = lax.broadcasted_iota(jnp.int32, (n, n), 1)
    return jnp.where(rows == cols, 1.0, 0.0).astype(BF16)


class Sizes:
    def __init__(self, na, nz, nh, rows, cols, depth, ch):
        self.na, self.nz, self.nh = na, nz, nh
        self.rb, self.k, self.d, self.ch = rows, cols, depth, ch
        self.g = na * nh
        self.naz = na * nz
        self.rh = rows // nh
        self.hid = ch * nh
        self.cp = ch // na
        self.nq = math.gcd(self.cp, MAX_CHUNKS)
        self.cq = self.cp // self.nq
        self.m = na * self.cq
        self.nc = self.g * self.cq
        self.i = na * rows
        self.br = math.gcd(self.rh, 16)
        self.nb = self.rh // self.br
        self.bi = math.gcd(self.rb, 16)
        self.sp = self.hid + 8
        self.pp = self.m + 8
        self.tp = self.br + 8
        self.tb = math.gcd(self.br // 2, ROWS_AT_ONCE)
        self.no = math.gcd(max(4 * self.m // 8, 1), self.naz)
        self.rs = 4 * self.m // self.no
        self.per = max(self.no // na, 1)
        self.stride = na * self.per // self.no
        self.base = (nz - self.per) // 2
        self.q0 = self.nq - self.nq // 2 if nz > 3 else self.nq
        self.helped = max(self.nq - self.q0, 1)


def kernel(s, p_hbm, x_hbm, w_ref, gain_ref, mask_ref, mask_s, out_hbm, found_hbm, sq_hbm,
           xv, p_ref, pt, pg, wall, wt, gain, unit_s, inv_s, nt_s, pr, fac, relay, lrs, lrb, lrh, gs, gsh, gr, turn, ng,
           outv, raw, rx2, rx3, sq,
           xsem, pin, wsend, wrecv, psend, precv, zsend, zrecv, lsend, lrecv, gsend, grecv, osend, orecv,
           r2s, r2r, r3s, r3r, qs, qr, keep, leave, hls, hlr, hgs, hgr):
    na, nz, nh, g_n, nq, cq, nc = s.na, s.nz, s.nh, s.g, s.nq, s.cq, s.nc
    rb, rh, k, d, ch, hid, br, nb, m = s.rb, s.rh, s.k, s.d, s.ch, s.hid, s.br, s.nb, s.m
    a, z, h = lax.axis_index("ia"), lax.axis_index("ja"), lax.axis_index("col")
    me_g = h * na + a
    me_n = a * nz + z
    row0 = a * rb + h * rh
    q0 = s.q0
    is_end = (z == 0) | (z == nz - 1)
    is_near = (z == 1) | (z == nz - 2)
    inward = jnp.where(z == 0, 1, nz - 2)
    outward = jnp.where(z == 1, 0, nz - 1)

    def plane(g):
        return (lax.rem(g, na), z, lax.div(g, na))

    def peer_g(step):
        return lax.rem(me_g + step, g_n)

    def sent(ref, sem):
        pltpu.make_async_copy(ref, ref, sem).wait()

    def send(src, dst, send_sem, recv_sem, device):
        return pltpu.make_async_remote_copy(
            src_ref=src, dst_ref=dst, send_sem=send_sem, recv_sem=recv_sem,
            device_id=device, device_id_type=MESH)

    barrier = pltpu.get_barrier_semaphore()
    total = s.naz * nh
    me_t = me_n * nh + h

    def at_t(t):
        return (lax.div(t, nz * nh), lax.rem(lax.div(t, nh), nz), lax.rem(t, nh))

    def p_in(q):
        at = pl.ds(q * m, m)
        return pltpu.make_async_copy(p_hbm.at[:, at], p_ref.at[:, at], pin.at[q])

    for q in range(nq):
        p_in(q).start()
    for step in range(1, total):
        pl.semaphore_signal(barrier, inc=1, device_id=at_t(lax.rem(me_t + step, total)), device_id_type=MESH)
    xcopy = pltpu.make_async_copy(x_hbm.at[pl.ds(h * rh, rh)], xv, xsem)
    xcopy.start()

    def p_turn(q):
        p_in(q).wait()

        def block(ib, carry):
            slot = lax.rem(ib, 2)
            for ii in range(s.bi):
                relay[slot, ii * s.pp:ii * s.pp + m, :] = p_ref[ib * s.bi + ii, q * m:(q + 1) * m, :].astype(F32)
            for c in range(m):
                tile = relay[slot, pl.ds(c, s.bi, stride=s.pp), :]
                pt[q * m + c, pl.ds(pl.multiple_of(ib * s.bi, s.bi), s.bi), :] = tile.astype(BF16)
            return carry
        lax.fori_loop(0, rb // s.bi, block, 0)

    def pieces(q):
        return [(q * cq + r, 1) for r in range(cq)] if q == 0 else [(q * cq, cq)]

    def spot(c):
        return c if c < cq else cq - 1 + c // cq

    def p_copy(piece, step):
        c, n = piece
        to = lax.rem(a + step, na)
        return send(pt.at[pl.ds((c // cq) * m + to * cq + c % cq, n)], pg.at[z, pl.ds(c, n), pl.ds(a * rb, rb)],
                    psend, precv.at[spot(c)], (to, z, h))

    def w_copy(step):
        return send(w_ref, wall.at[h], wsend.at[step], wrecv.at[step], (a, z, lax.rem(h + step, nh)))

    p_turn(0)
    pl.semaphore_wait(barrier, total - 1)
    for step in range(1, nh):
        w_copy(step).start()
    for q in range(nq):
        if q:
            p_turn(q)
        for piece in pieces(q):
            for step in range(1, na):
                p_copy(piece, step).start()
    for q in range(nq):
        for r in range(cq):
            pg[z, q * cq + r, pl.ds(a * rb, rb), :] = pt[q * m + a * cq + r]

    def z_copy(piece, block, up):
        c, n = piece
        ref = pg.at[block, pl.ds(c, n)]
        return send(ref, ref, zsend.at[c // cq, 0 if up else 1], zrecv.at[spot(c), block],
                    (a, z + 1 if up else z - 1, h))

    def goes_up(q):
        return z < (nz - 1 if q < q0 else nz - 2)

    def goes_down(q):
        return z > (0 if q < q0 else 1)

    def z_own(q, some=None):
        for piece in some or pieces(q):
            sent(pt.at[pl.ds(0, (na - 1) * piece[1])], precv.at[spot(piece[0])])

            @pl.when(goes_up(q))
            def _(piece=piece):
                z_copy(piece, z, True).start()

            @pl.when(goes_down(q))
            def _(piece=piece):
                z_copy(piece, z, False).start()

    def z_forward(q, hop):
        @pl.when((z >= hop) & goes_up(q))
        def _():
            for piece in pieces(q):
                z_copy(piece, z - hop, True).wait_recv()
                z_copy(piece, z - hop, True).start()

        @pl.when((z + hop < nz) & goes_down(q))
        def _():
            for piece in pieces(q):
                z_copy(piece, z + hop, False).wait_recv()
                z_copy(piece, z + hop, False).start()

    def z_rest(q):
        for hop in range(1, nz):
            here = True if q < q0 else jnp.logical_not(is_end)

            @pl.when((z >= hop) & jnp.logical_not(goes_up(q)) & here)
            def _(hop=hop):
                for piece in pieces(q):
                    z_copy(piece, z - hop, True).wait_recv()

            @pl.when((z + hop < nz) & jnp.logical_not(goes_down(q)) & here)
            def _(hop=hop):
                for piece in pieces(q):
                    z_copy(piece, z + hop, False).wait_recv()

    eye_d = eye(d)
    column = jnp.transpose(jnp.broadcast_to(gain_ref[...], (k, d)))
    gain[...] = jnp.concatenate([column, column], axis=1)
    wall[h] = w_ref[...]
    for step in range(1, nh):
        w_copy(step).wait_recv()
    for q in range(nq):
        rows = [wall[half, w, q * m:(q + 1) * m, :] for half in range(nh) for w in range(4)]
        wt[q] = dot(eye_d, jnp.concatenate(rows, axis=0), NT).astype(BF16)

    xcopy.wait()
    col_valid = mask_ref[pl.ds(z, 1), :].astype(F32)

    def rows_step(t, sub):
        x2 = xv[pl.ds(2 * t, 2)].reshape(2 * k, d)
        xt = dot(eye_d, x2, NT)
        centred = xt - jnp.mean(xt, axis=0, keepdims=True)
        inv = lax.rsqrt(jnp.mean(centred * centred, axis=0, keepdims=True) + 1e-05)
        unit = centred * inv
        normed = (unit * gain[...]).astype(BF16)
        unit_s[t] = unit
        inv_s[t] = inv
        nt_s[t] = normed
        for half in range(nh):
            pr[half * 4 * ch:(half + 1) * 4 * ch, :] = dot(wall[half].reshape(4 * ch, d), normed, NN)
        valid = jnp.concatenate(
            [col_valid * mask_s[row0 + 2 * t + e].astype(F32) for e in range(2)], axis=1)
        for q in range(nq):
            for side in range(2):
                def part(w):
                    at = [half * 4 * ch + w * ch + q * m for half in range(nh)]
                    return jnp.concatenate([pr[x:x + m, :] for x in at], axis=0)
                lin = part(2 * side)
                gate = jax.nn.sigmoid(part(2 * side + 1))
                first = valid * gate
                value = first * lin
                fac[t, q, 2 * side] = first.astype(BF16)
                fac[t, q, 2 * side + 1] = (value * (1.0 - gate)).astype(BF16)
                for e in range(2):
                    at = pl.multiple_of((2 * sub + e) * s.sp, 8) + q * nc
                    relay[side, pl.ds(at, nc), :] = value[:, e * k:(e + 1) * k]

    for b in range(nb):
        def one(sub, carry, b=b):
            rows_step(b * (br // 2) + sub, sub)
            return carry
        parts = pieces(0) if b == 0 else [None]
        each = br // 2 // len(parts)
        if each * len(parts) * 2 == br:
            for n, piece in enumerate(parts):
                lax.fori_loop(n * each, (n + 1) * each, one, 0)
                if piece:
                    z_own(0, [piece])
        else:
            lax.fori_loop(0, br // 2, one, 0)
            if b == 0:
                z_own(0)

        def flush(c, carry, b=b):
            for side in range(2):
                tile = relay[side, pl.ds(c, br, stride=s.sp), :]
                lrs[side, c, b * br:(b + 1) * br, :] = tile.astype(BF16)
            return carry
        lax.fori_loop(0, hid, flush, 0, unroll=4)
        if 0 < b < q0:
            z_own(b)
    for q in range(nb, q0):
        z_own(q)

    if q0 < nq:
        @pl.when(is_end)
        def _():
            z_own(q0)

    def lr_copy(q, step):
        return send(lrs.at[:, pl.ds(q * nc + peer_g(step) * cq, cq)],
                    lrb.at[:, pl.ds(q * cq, cq), pl.ds(row0, rh)],
                    lsend, lrecv.at[q], plane(peer_g(step)))

    for q in [*range(q0, nq), *range(q0)]:
        for step in range(1, g_n):
            lr_copy(q, step).start()
    for q in range(nq):
        for side in range(2):
            for r in range(cq):
                lrb[side, q * cq + r, pl.ds(row0, rh), :] = lrs[side, q * nc + me_g * cq + r]

    eye_k = eye(k)

    def triangle(c, lr, at, to):
        panel = jnp.concatenate([pg[b, c] for b in range(nz)], axis=1)
        left, right = lr[0, at], lr[1, at]
        to[0, at] = dot(panel, right, NN).astype(BF16).reshape(g_n, rh, k)
        left_t = dot(eye_k, left, NT).astype(BF16)
        back_t = dot(left_t, panel, NN).astype(BF16)
        back = [dot(eye_k, back_t[:, b * k:(b + 1) * k], NT).astype(BF16) for b in range(nz)]
        to[1, at] = jnp.concatenate(back, axis=0).reshape(g_n, rh, k)

    def triangles(q, lr, to, base):
        def one(r, carry):
            triangle(q * cq + r, lr, (q - base) * cq + r, to)
            return carry
        lax.fori_loop(0, cq, one, 0)

    def in_copy(q, z_to):
        return send(lrb.at[:, pl.ds(q * cq, cq)], lrh.at[:, pl.ds((q - q0) * cq, cq)],
                    hls, hlr.at[q - q0], (a, z_to, h))

    def g_copy(q, b, step):
        g = peer_g(step)
        place = lax.rem(g, na) * nh + lax.div(g, na)
        return send(gs.at[:, pl.ds(q * cq, cq), place, pl.ds(b * br, br)],
                    gr.at[:, pl.ds(q * nc + me_g * cq, cq), pl.ds(b * br, br)],
                    gsend.at[q], grecv.at[q, b], plane(g))

    def back_copy(q, b, z_to):
        return send(gsh.at[:, pl.ds((q - q0) * cq, cq), :, pl.ds(b * br, br)],
                    gs.at[:, pl.ds(q * cq, cq), :, pl.ds(b * br, br)],
                    hgs, hgr.at[q - q0, b], (a, z_to, h))

    def direct(q):
        return q == nq - 1 and q >= q0

    def direct_copy(q, b, step):
        g = peer_g(step)
        place = lax.rem(g, na) * nh + lax.div(g, na)
        return send(gsh.at[:, pl.ds((q - q0) * cq, cq), place, pl.ds(b * br, br)],
                    gr.at[:, pl.ds(q * nc + me_g * cq, cq), pl.ds(b * br, br)],
                    hgs, grecv.at[q, b], (lax.rem(g, na), outward, lax.div(g, na)))

    def out_copy(b, step):
        return send(outv.at[pl.ds(b * br, br)], out_hbm.at[pl.ds(h * rh + b * br, br)],
                    osend.at[b, step], orecv.at[b, step], (a, z, lax.rem(h + step, nh)))

    def keep_copy(b):
        return pltpu.make_async_copy(
            outv.at[pl.ds(b * br, br)], out_hbm.at[pl.ds(h * rh + b * br, br)], keep.at[b])

    def at_n(n):
        return (lax.div(n, nz), lax.rem(n, nz), h)

    def owner(o):
        return (o // s.per * s.stride, s.base + o % s.per)

    def other(o, half=None):
        away = (a != owner(o)[0]) | (z != owner(o)[1])
        return away if half is None else away | (h != half)

    me_o = lax.div(a, s.stride) * s.per + z - s.base
    is_owner = (lax.rem(a, s.stride) == 0) & (z >= s.base) & (z < s.base + s.per)
    batches = [(0, nq - 1), (nq - 1, nq)] if nq > 1 else [(0, nq)]
    final = len(batches) - 1

    def r2_copy(batch, half, o, sender):
        lo, hi = batches[batch]
        return send(raw.at[lo:hi, half, o], rx2.at[sender, lo:hi],
                    r2s.at[batch], r2r.at[batch], (*owner(o), half))

    def r2_start(batch):
        for half in range(nh):
            for o in range(s.no):
                @pl.when(other(o, half))
                def _(half=half, o=o):
                    r2_copy(batch, half, o, me_t).start()

    def r3_copy(batch, o, step):
        lo, hi = batches[batch]
        ref = rx3.at[o, lo:hi]
        return send(ref, ref, r3s.at[batch], r3r.at[batch], at_n(lax.rem(me_n + step, s.naz)))

    def sq_copy(slot, step):
        ref = sq.at[slot]
        return send(ref, ref, qs, qr, at_t(lax.rem(me_t + step, total)))

    def r2_sum(batch):
        lo, hi = batches[batch]

        @pl.when(is_owner)
        def _():
            def one(step, mine):
                return mine + rx2[lax.rem(me_t + step, total), lo:hi]
            sent(rx2.at[pl.ds(0, total - 1), lo:hi], r2r.at[batch])
            rx3[me_o, lo:hi] = lax.fori_loop(1, total, one, raw[lo:hi, h, me_o])
            for step in range(1, s.naz):
                r3_copy(batch, me_o, step).start()
            if batch == final:
                slot = h * s.no + me_o
                found = rx3[me_o].reshape(nq * s.rs, d)
                sq[slot] = jnp.sum(found * found, axis=0, keepdims=True)
                for step in range(1, total):
                    sq_copy(slot, step).start()

    def at_role(wait):
        @pl.when(is_owner)
        def _():
            wait(1)

        @pl.when(jnp.logical_not(is_owner))
        def _():
            wait(0)

    def r3_wait(batch):
        lo, hi = batches[batch]
        at_role(lambda own: sent(rx2.at[pl.ds(0, s.no - own), lo:hi], r3r.at[batch]))

    def sq_wait():
        at_role(lambda own: sent(sq.at[pl.ds(0, nh * s.no - own)], qr))

    def gather(q, b):
        def came(count):
            sent(gr.at[:, pl.ds(0, count * cq), pl.ds(0, br)], grecv.at[q, b])

        if direct(q):
            @pl.when(is_end)
            def _():
                came(g_n)

            @pl.when(jnp.logical_not(is_end))
            def _():
                came(g_n - 1)
        else:
            came(g_n - 1)

        def spread(n, carry):
            for side in range(2):
                tile = gr[side, q * nc + n, b * br:(b + 1) * br, :].astype(F32)
                turn[side, pl.ds(pl.multiple_of(n * s.tp, 8), br), :] = tile
            return carry
        lax.fori_loop(0, nc, spread, 0, unroll=4)
        if b == 0:
            raw[q] = jnp.zeros((nh, s.no, s.rs, d), F32)

        def one(sub, carry):
            t0 = b * (br // 2) + sub * s.tb
            terms = []
            for side in range(2):
                both = jnp.concatenate(
                    [turn[side, pl.ds(2 * s.tb * sub + e, nc, stride=s.tp), :] for e in range(2 * s.tb)], axis=1)
                for w in range(2):
                    factor = jnp.concatenate([fac[t0 + u, q, 2 * side + w] for u in range(s.tb)], axis=1)
                    terms.append((both * factor.astype(F32)).astype(BF16))
            grads = jnp.concatenate(
                [term[half * m:(half + 1) * m] for half in range(nh) for term in terms], axis=0)
            normed = jnp.concatenate([nt_s[t0 + u] for u in range(s.tb)], axis=1)
            raw[q] += dot(grads, normed, NT).reshape(nh, s.no, s.rs, d)
            part = dot(wt[q], grads, NN)
            for u in range(s.tb):
                piece = part[:, u * 2 * k:(u + 1) * 2 * k]
                ng[t0 + u] = ng[t0 + u] + piece if q else piece
            return carry
        lax.fori_loop(0, br // 2 // s.tb, one, 0)

    def norm_back(b):
        def one(sub, carry):
            t = b * (br // 2) + sub
            unit = unit_s[t]
            scaled = ng[t] * gain[...]
            first = jnp.mean(scaled, axis=0, keepdims=True)
            second = jnp.mean(scaled * unit, axis=0, keepdims=True)
            res = (inv_s[t] * (scaled - first - unit * second)).astype(BF16)
            for e in range(2):
                outv[2 * t + e] = dot(eye_k, res[:, e * k:(e + 1) * k], NT).astype(BF16)
            return carry
        lax.fori_loop(0, br // 2, one, 0, unroll=2)
        keep_copy(b).start()
        for step in range(1, nh):
            out_copy(b, step).start()

    def lr_wait(q):
        sent(lrs.at[:, pl.ds(0, (g_n - 1) * cq)], lrecv.at[q])

    def g_out(q, b):
        for step in range(1, g_n):
            g_copy(q, b, step).start()
        for side in range(2):
            for r in range(cq):
                gr[side, q * nc + me_g * cq + r, b * br:(b + 1) * br, :] = gs[
                    side, q * cq + r, a * nh + h, b * br:(b + 1) * br, :]

    def g_send(q, b):
        if direct(q):
            @pl.when(jnp.logical_not(is_end))
            def _():
                g_out(q, b)
        else:
            g_out(q, b)

    def help_end(q):
        @pl.when(is_near)
        def _():
            z_rest(q)
            in_copy(q, outward).wait_recv()
            triangles(q, lrh, gsh, q0)
            for b in range(nb):
                if direct(q):
                    for step in range(g_n):
                        direct_copy(q, b, step).start()
                else:
                    back_copy(q, b, outward).start()

    def make(q):
        if q < q0:
            z_rest(q)
            lr_wait(q)
            triangles(q, lrb, gs, 0)
            return

        @pl.when(jnp.logical_not(is_near | is_end))
        def _():
            z_rest(q)

        @pl.when(jnp.logical_not(is_end))
        def _():
            lr_wait(q)
            triangles(q, lrb, gs, 0)

    def came_back(q, b):
        if q >= q0 and not direct(q):
            @pl.when(is_end)
            def _():
                back_copy(q, b, outward).wait_recv()

    for hop in range(1, nz - 1):
        for q in range(q0):
            z_forward(q, hop)
        if hop == 1 and q0 < nq:
            @pl.when(jnp.logical_not(is_end))
            def _():
                z_own(q0)
    def relay_on(q):
        if q >= nq:
            return
        for hop in range(1, nz - 1):
            z_forward(q, hop)
        if q + 1 < nq:
            @pl.when(jnp.logical_not(is_end))
            def _():
                z_own(q + 1)

    relay_on(q0)

    @pl.when(is_end)
    def _():
        for q in range(q0, nq):
            lr_wait(q)
            in_copy(q, inward).start()
            if q + 1 < nq:
                z_own(q + 1)

    def drain():
        for step in range(1, nh):
            w_copy(step).wait_send()
        sent(pt.at[pl.ds(0, (na - 1) * s.cp)], psend)
        sent(lrs.at[:, pl.ds(0, (g_n - 1) * nq * cq)], lsend)
        for q in range(nq):
            if direct(q):
                @pl.when(jnp.logical_not(is_end))
                def _(q=q):
                    sent(gs.at[:, pl.ds(q * cq, cq), pl.ds(0, g_n - 1)], gsend.at[q])
            else:
                sent(gs.at[:, pl.ds(q * cq, cq), pl.ds(0, g_n - 1)], gsend.at[q])
            for count in range(1, nz):
                @pl.when((z + 1 == count) & goes_up(q))
                def _(q=q, count=count):
                    sent(pg.at[pl.ds(0, count), pl.ds(q * cq, cq)], zsend.at[q, 0])

                @pl.when((nz - z == count) & goes_down(q))
                def _(q=q, count=count):
                    sent(pg.at[pl.ds(0, count), pl.ds(q * cq, cq)], zsend.at[q, 1])
        if q0 < nq:
            @pl.when(is_end)
            def _():
                sent(lrh, hls)

            @pl.when(is_near)
            def _():
                sent(gsh, hgs)

    last = nq - 1
    queue = []

    def run(count):
        for _ in range(min(count, len(queue))):
            q, b = queue.pop(0)
            gather(q, b)
            if b == nb - 1 and q == last - 1:
                r2_start(0)
            if b == nb - 1 and q == last:
                r2_start(final)

    for q in range(nq):
        if q == q0 - 1 and q0 < nq:
            help_end(q0)
            relay_on(q0 + 1)
        elif q > q0:
            help_end(q)
            relay_on(q + 1)
        make(q)
        if q > 1:
            queue += [(q - 2, b) for b in range(nb)]
        if q == last:
            queue += [(last - 1, b) for b in range(nb)] if q else []
            run(max(len(queue) - 2 * nb, 0))
        for b in range(nb):
            run(1 if q < last else 0)
            came_back(q, b)
            g_send(q, b)
            if q == last:
                run(3 if b < nb - 1 else 0)
                if b:
                    queue.append((last, b - 1))
    queue.append((last, nb - 1))
    run(max(len(queue) - 1, 0))
    if nb > 1:
        norm_back(0)
    run(1)
    waiting = list(range(len(batches)))
    for b in range(1 if nb > 1 else 0, nb):
        if len(waiting) > 1:
            r2_sum(waiting.pop(0))
        norm_back(b)
    for batch in waiting:
        r2_sum(batch)
    drain()
    for batch in range(len(batches)):
        r3_wait(batch)
    found_out = pltpu.make_async_copy(rx3, found_hbm, leave.at[0])
    found_out.start()
    sq_wait()
    sq_out = pltpu.make_async_copy(sq.at[pl.ds(0, nh * s.no)], sq_hbm, leave.at[1])
    sq_out.start()
    for b in range(nb):
        keep_copy(b).wait()
        for step in range(1, nh):
            out_copy(b, step).wait()
    for batch, (lo, hi) in enumerate(batches):
        @pl.when(is_owner)
        def _(batch=batch, lo=lo, hi=hi):
            sent(rx2.at[pl.ds(0, nh * s.no - 1), lo:hi], r2s.at[batch])
            sent(rx2.at[pl.ds(0, s.naz - 1), lo:hi], r3s.at[batch])

        @pl.when(jnp.logical_not(is_owner))
        def _(batch=batch, lo=lo, hi=hi):
            sent(rx2.at[pl.ds(0, nh * s.no), lo:hi], r2s.at[batch])

    @pl.when(is_owner)
    def _():
        sent(sq.at[pl.ds(0, total - 1)], qs)
    found_out.wait()
    sq_out.wait()


def finish(s, blocks, from_hbm, found_ref, sq_ref, out_hbm, wg_ref, held, sem_in, sem_out):
    size = held.shape[0] // blocks

    def came(b):
        at = pl.ds(b * size, size)
        return pltpu.make_async_copy(from_hbm.at[at], held.at[at], sem_in.at[b])

    def leaves(b):
        at = pl.ds(b * size, size)
        return pltpu.make_async_copy(held.at[at], out_hbm.at[at], sem_out.at[b])

    for b in range(blocks):
        came(b).start()
    squares = jnp.sum(jnp.sum(sq_ref[...], axis=0), axis=1, keepdims=True)
    factor = jnp.minimum(1.0, CLIP_LIMIT * lax.rsqrt(squares + 1e-06))
    for q in range(s.nq):
        for o in range(s.no):
            w, at = o * s.rs // s.m, q * s.m + o * s.rs % s.m
            wg_ref[w, at:at + s.rs, :] = found_ref[o, q] * factor
    for b in range(blocks):
        came(b).wait()
        leaves(b).start()
    for b in range(blocks):
        leaves(b).wait()


def on_device(na, nz, nh, pair_rep, norm_gain, weights, residue_mask, product_grad):
    rows, cols, depth = pair_rep.shape
    ch = product_grad.shape[1]
    s = Sizes(na, nz, nh, rows, cols, depth, ch)
    vm = pl.BlockSpec(memory_space=pltpu.VMEM)
    anywhere = pl.BlockSpec(memory_space=pl.ANY)
    dma = pltpu.SemaphoreType.DMA
    half = s.rh // 2
    scratch = [
        pltpu.VMEM((s.rh, cols, depth), BF16),
        pltpu.VMEM((rows, ch, cols), BF16),
        pltpu.VMEM((ch, rows, cols), BF16),
        pltpu.VMEM((nz, s.cp, s.i, cols), BF16),
        pltpu.VMEM((nh, 4, ch, depth), BF16),
        pltpu.VMEM((s.nq, depth, 4 * s.nc), BF16),
        pltpu.VMEM((depth, 2 * cols), F32),
        pltpu.VMEM((half, depth, 2 * cols), F32),
        pltpu.VMEM((half, 1, 2 * cols), F32),
        pltpu.VMEM((half, depth, 2 * cols), BF16),
        pltpu.VMEM((4 * s.hid, 2 * cols), F32),
        pltpu.VMEM((half, s.nq, 4, s.nc, 2 * cols), BF16),
        pltpu.VMEM((2, max(s.br * s.sp, s.bi * s.pp), cols), F32),
        pltpu.VMEM((2, s.hid, s.rh, cols), BF16),
        pltpu.VMEM((2, s.cp, s.i, cols), BF16),
        pltpu.VMEM((2, s.helped * s.cq, s.i, cols), BF16),
        pltpu.VMEM((2, s.cp, s.g, s.rh, cols), BF16),
        pltpu.VMEM((2, s.helped * s.cq, s.g, s.rh, cols), BF16),
        pltpu.VMEM((2, s.hid, s.rh, cols), BF16),
        pltpu.VMEM((2, s.nc * s.tp, cols), F32),
        pltpu.VMEM((half, depth, 2 * cols), F32),
        pltpu.VMEM((s.rh, cols, depth), BF16),
        pltpu.VMEM((s.nq, nh, s.no, s.rs, depth), F32),
        pltpu.VMEM((s.naz * nh, s.nq, s.rs, depth), F32),
        pltpu.VMEM((s.no, s.nq, s.rs, depth), F32),
        pltpu.VMEM((s.naz * nh, 1, depth), F32),
        dma(()), dma((s.nq,)), dma((nh,)), dma((nh,)),
        dma(()), dma((s.cq + s.nq,)), dma((s.nq, 2)), dma((s.cq + s.nq, nz)),
        dma(()), dma((s.nq,)), dma((s.nq,)), dma((s.nq, s.nb)),
        dma((s.nb, nh)), dma((s.nb, nh)),
        dma((2,)), dma((2,)), dma((2,)), dma((2,)),
        dma(()), dma(()), dma((s.nb,)), dma((2,)),
        dma(()), dma((s.helped,)), dma(()), dma((s.helped, s.nb)),
    ]
    grad, found, squares = pl.pallas_call(
        functools.partial(kernel, s),
        out_shape=(
            jax.ShapeDtypeStruct((rows, cols, depth), BF16),
            jax.ShapeDtypeStruct((s.no, s.nq, s.rs, depth), F32),
            jax.ShapeDtypeStruct((nh * s.no, 1, depth), F32),
        ),
        in_specs=[anywhere, anywhere, vm, vm, vm, pl.BlockSpec(memory_space=pltpu.SMEM)],
        out_specs=(anywhere, anywhere, anywhere),
        scratch_shapes=scratch,
        compiler_params=pltpu.CompilerParams(
            collective_id=0, has_side_effects=True, vmem_limit_bytes=VMEM_LIMIT),
    )(product_grad, pair_rep, weights.transpose(0, 2, 1), norm_gain.reshape(1, depth),
      residue_mask.reshape(nz, cols), residue_mask)
    blocks = math.gcd(rows, 4)
    pair_grad, weight_grads = pl.pallas_call(
        functools.partial(finish, s, blocks),
        out_shape=(
            jax.ShapeDtypeStruct((rows, cols, depth), BF16),
            jax.ShapeDtypeStruct((4, ch, depth), F32),
        ),
        in_specs=[pl.BlockSpec(memory_space=pl.ANY), vm, vm],
        out_specs=(pl.BlockSpec(memory_space=pl.ANY), vm),
        scratch_shapes=[pltpu.VMEM((rows, cols, depth), BF16), dma((blocks,)), dma((blocks,))],
    )(grad, found, squares)
    return (pair_grad, weight_grads.transpose(0, 2, 1))


def solution(mesh):
    sizes = mesh.shape["ia"], mesh.shape["ja"], mesh.shape["col"]
    placed = (P("ia", "ja", None), P(), P(None, None, "col"), P(), P("ia", "col", "ja"))

    def step(*args):
        return on_device(*sizes, *args)

    return jax.shard_map(
        step,
        mesh=mesh,
        in_specs=placed,
        out_specs=(P("ia", "ja", None), P(None, None, "col")),
        check_vma=False,
    )
```

```python
import functools
import math

import jax
import jax.numpy as jnp
from jax import lax
from jax.experimental import pallas as pl
from jax.experimental.pallas import tpu as pltpu
from jax.sharding import PartitionSpec as P

CLIP_LIMIT = 64.0
MAX_CHUNKS = 4
ROWS_AT_ONCE = 2
VMEM_LIMIT = 66 * 1000 * 1000
MESH = pl.DeviceIdType.MESH
NT = (((1,), (1,)), ((), ()))
NN = (((1,), (0,)), ((), ()))
F32 = jnp.float32
BF16 = jnp.bfloat16


def dot(a, b, dims):
    return lax.dot_general(a, b, dims, preferred_element_type=F32)


def eye(n):
    rows = lax.broadcasted_iota(jnp.int32, (n, n), 0)
    cols = lax.broadcasted_iota(jnp.int32, (n, n), 1)
    return jnp.where(rows == cols, 1.0, 0.0).astype(BF16)


class Sizes:
    def __init__(self, na, nz, nh, rows, cols, depth, ch):
        self.na, self.nz, self.nh = na, nz, nh
        self.rb, self.k, self.d, self.ch = rows, cols, depth, ch
        self.g = na * nh
        self.naz = na * nz
        self.rh = rows // nh
        self.hid = ch * nh
        self.cp = ch // na
        self.nq = math.gcd(self.cp, MAX_CHUNKS)
        self.cq = self.cp // self.nq
        self.m = na * self.cq
        self.nc = self.g * self.cq
        self.i = na * rows
        self.br = math.gcd(self.rh, 16)
        self.nb = self.rh // self.br
        self.bi = math.gcd(self.rb, 16)
        self.sp = self.hid + 8
        self.pp = self.m + 8
        self.tp = self.br + 8
        self.tb = math.gcd(self.br // 2, ROWS_AT_ONCE)
        self.no = math.gcd(max(4 * self.m // 8, 1), self.naz)
        self.rs = 4 * self.m // self.no
        self.per = max(self.no // na, 1)
        self.stride = na * self.per // self.no
        self.base = (nz - self.per) // 2
        self.q0 = self.nq - self.nq // 2 if nz > 3 else self.nq
        self.helped = max(self.nq - self.q0, 1)


def kernel(s, p_hbm, x_hbm, w_ref, gain_ref, mask_ref, mask_s, out_hbm, found_hbm, sq_hbm,
           xv, p_ref, pt, pg, wall, wt, gain, unit_s, inv_s, nt_s, pr, fac, relay, lrs, lrb, lrh, gs, gsh, gr, turn, ng,
           outv, raw, rx2, rx3, sq,
           xsem, pin, wsend, wrecv, psend, precv, zsend, zrecv, lsend, lrecv, gsend, grecv, osend, orecv,
           r2s, r2r, r3s, r3r, qs, qr, keep, leave, hls, hlr, hgs, hgr):
    na, nz, nh, g_n, nq, cq, nc = s.na, s.nz, s.nh, s.g, s.nq, s.cq, s.nc
    rb, rh, k, d, ch, hid, br, nb, m = s.rb, s.rh, s.k, s.d, s.ch, s.hid, s.br, s.nb, s.m
    a, z, h = lax.axis_index("ia"), lax.axis_index("ja"), lax.axis_index("col")
    me_g = h * na + a
    me_n = a * nz + z
    row0 = a * rb + h * rh
    q0 = s.q0
    is_end = (z == 0) | (z == nz - 1)
    is_near = (z == 1) | (z == nz - 2)
    inward = jnp.where(z == 0, 1, nz - 2)
    outward = jnp.where(z == 1, 0, nz - 1)

    def plane(g):
        return (lax.rem(g, na), z, lax.div(g, na))

    def peer_g(step):
        return lax.rem(me_g + step, g_n)

    def sent(ref, sem):
        pltpu.make_async_copy(ref, ref, sem).wait()

    def send(src, dst, send_sem, recv_sem, device):
        return pltpu.make_async_remote_copy(
            src_ref=src, dst_ref=dst, send_sem=send_sem, recv_sem=recv_sem,
            device_id=device, device_id_type=MESH)

    barrier = pltpu.get_barrier_semaphore()
    total = s.naz * nh
    me_t = me_n * nh + h

    def at_t(t):
        return (lax.div(t, nz * nh), lax.rem(lax.div(t, nh), nz), lax.rem(t, nh))

    def p_in(q):
        at = pl.ds(q * m, m)
        return pltpu.make_async_copy(p_hbm.at[:, at], p_ref.at[:, at], pin.at[q])

    for q in range(nq):
        p_in(q).start()
    for step in range(1, total):
        pl.semaphore_signal(barrier, inc=1, device_id=at_t(lax.rem(me_t + step, total)), device_id_type=MESH)
    xcopy = pltpu.make_async_copy(x_hbm.at[pl.ds(h * rh, rh)], xv, xsem)
    xcopy.start()

    def p_turn(q):
        p_in(q).wait()

        def block(ib, carry):
            slot = lax.rem(ib, 2)
            for ii in range(s.bi):
                relay[slot, ii * s.pp:ii * s.pp + m, :] = p_ref[ib * s.bi + ii, q * m:(q + 1) * m, :].astype(F32)
            for c in range(m):
                tile = relay[slot, pl.ds(c, s.bi, stride=s.pp), :]
                pt[q * m + c, pl.ds(pl.multiple_of(ib * s.bi, s.bi), s.bi), :] = tile.astype(BF16)
            return carry
        lax.fori_loop(0, rb // s.bi, block, 0)

    def pieces(q):
        return [(q * cq + r, 1) for r in range(cq)] if q in (0, q0) else [(q * cq, cq)]

    starts = [piece[0] for q in range(nq) for piece in pieces(q)]

    def spot(c):
        return starts.index(c)

    def p_copy(piece, step):
        c, n = piece
        to = lax.rem(a + step, na)
        return send(pt.at[pl.ds((c // cq) * m + to * cq + c % cq, n)], pg.at[z, pl.ds(c, n), pl.ds(a * rb, rb)],
                    psend, precv.at[spot(c)], (to, z, h))

    def w_copy(step):
        return send(w_ref, wall.at[h], wsend.at[step], wrecv.at[step], (a, z, lax.rem(h + step, nh)))

    p_turn(0)
    pl.semaphore_wait(barrier, total - 1)
    for step in range(1, nh):
        w_copy(step).start()
    for q in range(nq):
        if q:
            p_turn(q)
        for piece in pieces(q):
            for step in range(1, na):
                p_copy(piece, step).start()
    for q in range(nq):
        for r in range(cq):
            pg[z, q * cq + r, pl.ds(a * rb, rb), :] = pt[q * m + a * cq + r]

    def z_copy(piece, block, up):
        c, n = piece
        ref = pg.at[block, pl.ds(c, n)]
        return send(ref, ref, zsend.at[c // cq, 0 if up else 1], zrecv.at[spot(c), block],
                    (a, z + 1 if up else z - 1, h))

    def goes_up(q):
        return z < (nz - 1 if q < q0 else nz - 2)

    def goes_down(q):
        return z > (0 if q < q0 else 1)

    def z_own(q, some=None):
        for piece in some or pieces(q):
            sent(pt.at[pl.ds(0, (na - 1) * piece[1])], precv.at[spot(piece[0])])

            @pl.when(goes_up(q))
            def _(piece=piece):
                z_copy(piece, z, True).start()

            @pl.when(goes_down(q))
            def _(piece=piece):
                z_copy(piece, z, False).start()

    def z_forward(q, hop):
        @pl.when((z >= hop) & goes_up(q))
        def _():
            for piece in pieces(q):
                z_copy(piece, z - hop, True).wait_recv()
                z_copy(piece, z - hop, True).start()

        @pl.when((z + hop < nz) & goes_down(q))
        def _():
            for piece in pieces(q):
                z_copy(piece, z + hop, False).wait_recv()
                z_copy(piece, z + hop, False).start()

    def z_rest(q, some=None):
        for hop in range(1, nz):
            here = True if q < q0 else jnp.logical_not(is_end)

            @pl.when((z >= hop) & jnp.logical_not(goes_up(q)) & here)
            def _(hop=hop):
                for piece in some or pieces(q):
                    z_copy(piece, z - hop, True).wait_recv()

            @pl.when((z + hop < nz) & jnp.logical_not(goes_down(q)) & here)
            def _(hop=hop):
                for piece in some or pieces(q):
                    z_copy(piece, z + hop, False).wait_recv()

    eye_d = eye(d)
    column = jnp.transpose(jnp.broadcast_to(gain_ref[...], (k, d)))
    gain[...] = jnp.concatenate([column, column], axis=1)
    wall[h] = w_ref[...]
    for step in range(1, nh):
        w_copy(step).wait_recv()
    for q in range(nq):
        rows = [wall[half, w, q * m:(q + 1) * m, :] for half in range(nh) for w in range(4)]
        wt[q] = dot(eye_d, jnp.concatenate(rows, axis=0), NT).astype(BF16)

    xcopy.wait()
    col_valid = mask_ref[pl.ds(z, 1), :].astype(F32)

    def rows_step(t, sub):
        x2 = xv[pl.ds(2 * t, 2)].reshape(2 * k, d)
        xt = dot(eye_d, x2, NT)
        centred = xt - jnp.mean(xt, axis=0, keepdims=True)
        inv = lax.rsqrt(jnp.mean(centred * centred, axis=0, keepdims=True) + 1e-05)
        unit = centred * inv
        normed = (unit * gain[...]).astype(BF16)
        unit_s[t] = unit
        inv_s[t] = inv
        nt_s[t] = normed
        for half in range(nh):
            pr[half * 4 * ch:(half + 1) * 4 * ch, :] = dot(wall[half].reshape(4 * ch, d), normed, NN)
        valid = jnp.concatenate(
            [col_valid * mask_s[row0 + 2 * t + e].astype(F32) for e in range(2)], axis=1)
        for q in range(nq):
            for side in range(2):
                def part(w):
                    at = [half * 4 * ch + w * ch + q * m for half in range(nh)]
                    return jnp.concatenate([pr[x:x + m, :] for x in at], axis=0)
                lin = part(2 * side)
                gate = jax.nn.sigmoid(part(2 * side + 1))
                first = valid * gate
                value = first * lin
                fac[t, q, 2 * side] = first.astype(BF16)
                fac[t, q, 2 * side + 1] = (value * (1.0 - gate)).astype(BF16)
                for e in range(2):
                    at = pl.multiple_of((2 * sub + e) * s.sp, 8) + q * nc
                    relay[side, pl.ds(at, nc), :] = value[:, e * k:(e + 1) * k]

    for b in range(nb):
        def one(sub, carry, b=b):
            rows_step(b * (br // 2) + sub, sub)
            return carry
        parts = pieces(0) if b == 0 else [None]
        each = br // 2 // len(parts)
        if each * len(parts) * 2 == br:
            for n, piece in enumerate(parts):
                lax.fori_loop(n * each, (n + 1) * each, one, 0)
                if piece:
                    z_own(0, [piece])
        else:
            lax.fori_loop(0, br // 2, one, 0)
            if b == 0:
                z_own(0)

        def flush(c, carry, b=b):
            for side in range(2):
                tile = relay[side, pl.ds(c, br, stride=s.sp), :]
                lrs[side, c, b * br:(b + 1) * br, :] = tile.astype(BF16)
            return carry
        lax.fori_loop(0, hid, flush, 0, unroll=4)
        if 0 < b < q0:
            z_own(b)
    for q in range(nb, q0):
        z_own(q)

    if q0 < nq:
        @pl.when(is_end)
        def _():
            z_own(q0)

    def lr_copy(q, step):
        return send(lrs.at[:, pl.ds(q * nc + peer_g(step) * cq, cq)],
                    lrb.at[:, pl.ds(q * cq, cq), pl.ds(row0, rh)],
                    lsend, lrecv.at[q], plane(peer_g(step)))

    for q in [*range(q0, nq), *range(q0)]:
        for step in range(1, g_n):
            lr_copy(q, step).start()
    for q in range(nq):
        for side in range(2):
            for r in range(cq):
                lrb[side, q * cq + r, pl.ds(row0, rh), :] = lrs[side, q * nc + me_g * cq + r]

    eye_k = eye(k)

    def triangle(c, lr, at, to):
        panel = jnp.concatenate([pg[b, c] for b in range(nz)], axis=1)
        left, right = lr[0, at], lr[1, at]
        to[0, at] = dot(panel, right, NN).astype(BF16).reshape(g_n, rh, k)
        left_t = dot(eye_k, left, NT).astype(BF16)
        back_t = dot(left_t, panel, NN).astype(BF16)
        back = [dot(eye_k, back_t[:, b * k:(b + 1) * k], NT).astype(BF16) for b in range(nz)]
        to[1, at] = jnp.concatenate(back, axis=0).reshape(g_n, rh, k)

    def triangles(q, lr, to, base):
        def one(r, carry):
            triangle(q * cq + r, lr, (q - base) * cq + r, to)
            return carry
        lax.fori_loop(0, cq, one, 0)

    def in_copy(q, r, z_to):
        at = (q - q0) * cq + r
        return send(lrb.at[:, pl.ds(q * cq + r, 1)], lrh.at[:, pl.ds(at, 1)], hls, hlr.at[at], (a, z_to, h))

    def g_copy(q, b, step):
        g = peer_g(step)
        place = lax.rem(g, na) * nh + lax.div(g, na)
        return send(gs.at[:, pl.ds(q * cq, cq), place, pl.ds(b * br, br)],
                    gr.at[:, pl.ds(q * nc + me_g * cq, cq), pl.ds(b * br, br)],
                    gsend.at[q], grecv.at[q, b], plane(g))

    def back_copy(q, b, z_to):
        return send(gsh.at[:, pl.ds((q - q0) * cq, cq), :, pl.ds(b * br, br)],
                    gs.at[:, pl.ds(q * cq, cq), :, pl.ds(b * br, br)],
                    hgs, hgr.at[q - q0, b], (a, z_to, h))

    def direct(q):
        return q == nq - 1 and q >= q0

    def direct_copy(q, b, step):
        g = peer_g(step)
        place = lax.rem(g, na) * nh + lax.div(g, na)
        return send(gsh.at[:, pl.ds((q - q0) * cq, cq), place, pl.ds(b * br, br)],
                    gr.at[:, pl.ds(q * nc + me_g * cq, cq), pl.ds(b * br, br)],
                    hgs, grecv.at[q, b], (lax.rem(g, na), outward, lax.div(g, na)))

    def out_copy(b, step):
        return send(outv.at[pl.ds(b * br, br)], out_hbm.at[pl.ds(h * rh + b * br, br)],
                    osend.at[b, step], orecv.at[b, step], (a, z, lax.rem(h + step, nh)))

    def keep_copy(b):
        return pltpu.make_async_copy(
            outv.at[pl.ds(b * br, br)], out_hbm.at[pl.ds(h * rh + b * br, br)], keep.at[b])

    def at_n(n):
        return (lax.div(n, nz), lax.rem(n, nz), h)

    def owner(o):
        return (o // s.per * s.stride, s.base + o % s.per)

    def other(o, half=None):
        away = (a != owner(o)[0]) | (z != owner(o)[1])
        return away if half is None else away | (h != half)

    me_o = lax.div(a, s.stride) * s.per + z - s.base
    is_owner = (lax.rem(a, s.stride) == 0) & (z >= s.base) & (z < s.base + s.per)
    batches = [(0, nq - 1), (nq - 1, nq)] if nq > 1 else [(0, nq)]
    final = len(batches) - 1

    def r2_copy(batch, half, o, sender):
        lo, hi = batches[batch]
        return send(raw.at[lo:hi, half, o], rx2.at[sender, lo:hi],
                    r2s.at[batch], r2r.at[batch], (*owner(o), half))

    def r2_start(batch):
        for half in range(nh):
            for o in range(s.no):
                @pl.when(other(o, half))
                def _(half=half, o=o):
                    r2_copy(batch, half, o, me_t).start()

    def r3_copy(batch, o, step):
        lo, hi = batches[batch]
        ref = rx3.at[o, lo:hi]
        return send(ref, ref, r3s.at[batch], r3r.at[batch], at_n(lax.rem(me_n + step, s.naz)))

    def sq_copy(slot, step):
        ref = sq.at[slot]
        return send(ref, ref, qs, qr, at_t(lax.rem(me_t + step, total)))

    def r2_sum(batch):
        lo, hi = batches[batch]

        @pl.when(is_owner)
        def _():
            def one(step, mine):
                return mine + rx2[lax.rem(me_t + step, total), lo:hi]
            sent(rx2.at[pl.ds(0, total - 1), lo:hi], r2r.at[batch])
            rx3[me_o, lo:hi] = lax.fori_loop(1, total, one, raw[lo:hi, h, me_o])
            for step in range(1, s.naz):
                r3_copy(batch, me_o, step).start()
            if batch == final:
                slot = h * s.no + me_o
                found = rx3[me_o].reshape(nq * s.rs, d)
                sq[slot] = jnp.sum(found * found, axis=0, keepdims=True)
                for step in range(1, total):
                    sq_copy(slot, step).start()

    def at_role(wait):
        @pl.when(is_owner)
        def _():
            wait(1)

        @pl.when(jnp.logical_not(is_owner))
        def _():
            wait(0)

    def r3_wait(batch):
        lo, hi = batches[batch]
        at_role(lambda own: sent(rx2.at[pl.ds(0, s.no - own), lo:hi], r3r.at[batch]))

    def sq_wait():
        at_role(lambda own: sent(sq.at[pl.ds(0, nh * s.no - own)], qr))

    def gather(q, b):
        def came(count):
            sent(gr.at[:, pl.ds(0, count * cq), pl.ds(0, br)], grecv.at[q, b])

        if direct(q):
            @pl.when(is_end)
            def _():
                came(g_n)

            @pl.when(jnp.logical_not(is_end))
            def _():
                came(g_n - 1)
        else:
            came(g_n - 1)

        def spread(n, carry):
            for side in range(2):
                tile = gr[side, q * nc + n, b * br:(b + 1) * br, :].astype(F32)
                turn[side, pl.ds(pl.multiple_of(n * s.tp, 8), br), :] = tile
            return carry
        lax.fori_loop(0, nc, spread, 0, unroll=4)
        if b == 0:
            raw[q] = jnp.zeros((nh, s.no, s.rs, d), F32)

        def one(sub, carry):
            t0 = b * (br // 2) + sub * s.tb
            terms = []
            for side in range(2):
                both = jnp.concatenate(
                    [turn[side, pl.ds(2 * s.tb * sub + e, nc, stride=s.tp), :] for e in range(2 * s.tb)], axis=1)
                for w in range(2):
                    factor = jnp.concatenate([fac[t0 + u, q, 2 * side + w] for u in range(s.tb)], axis=1)
                    terms.append((both * factor.astype(F32)).astype(BF16))
            grads = jnp.concatenate(
                [term[half * m:(half + 1) * m] for half in range(nh) for term in terms], axis=0)
            normed = jnp.concatenate([nt_s[t0 + u] for u in range(s.tb)], axis=1)
            raw[q] += dot(grads, normed, NT).reshape(nh, s.no, s.rs, d)
            part = dot(wt[q], grads, NN)
            for u in range(s.tb):
                piece = part[:, u * 2 * k:(u + 1) * 2 * k]
                ng[t0 + u] = ng[t0 + u] + piece if q else piece
            return carry
        lax.fori_loop(0, br // 2 // s.tb, one, 0)

    def norm_back(b):
        def one(sub, carry):
            t = b * (br // 2) + sub
            unit = unit_s[t]
            scaled = ng[t] * gain[...]
            first = jnp.mean(scaled, axis=0, keepdims=True)
            second = jnp.mean(scaled * unit, axis=0, keepdims=True)
            res = (inv_s[t] * (scaled - first - unit * second)).astype(BF16)
            for e in range(2):
                outv[2 * t + e] = dot(eye_k, res[:, e * k:(e + 1) * k], NT).astype(BF16)
            return carry
        lax.fori_loop(0, br // 2, one, 0, unroll=2)
        keep_copy(b).start()
        for step in range(1, nh):
            out_copy(b, step).start()

    def lr_wait(q):
        sent(lrs.at[:, pl.ds(0, (g_n - 1) * cq)], lrecv.at[q])

    def g_out(q, b):
        for step in range(1, g_n):
            g_copy(q, b, step).start()
        for side in range(2):
            for r in range(cq):
                gr[side, q * nc + me_g * cq + r, b * br:(b + 1) * br, :] = gs[
                    side, q * cq + r, a * nh + h, b * br:(b + 1) * br, :]

    def g_send(q, b):
        if direct(q):
            @pl.when(jnp.logical_not(is_end))
            def _():
                g_out(q, b)
        else:
            g_out(q, b)

    def help_end(q):
        @pl.when(is_near)
        def _():
            if q != q0:
                z_rest(q)
            for r in range(cq):
                if q == q0:
                    z_rest(q, [pieces(q)[r]])
                in_copy(q, r, outward).wait_recv()
                triangle(q * cq + r, lrh, (q - q0) * cq + r, gsh)
            for b in range(nb):
                if direct(q):
                    for step in range(g_n):
                        direct_copy(q, b, step).start()
                else:
                    back_copy(q, b, outward).start()

    def make(q):
        if q < q0:
            z_rest(q)
            lr_wait(q)
            triangles(q, lrb, gs, 0)
            return

        @pl.when(jnp.logical_not(is_near | is_end))
        def _():
            z_rest(q)

        @pl.when(jnp.logical_not(is_end))
        def _():
            lr_wait(q)
            triangles(q, lrb, gs, 0)

    def came_back(q, b):
        if q >= q0 and not direct(q):
            @pl.when(is_end)
            def _():
                back_copy(q, b, outward).wait_recv()

    for hop in range(1, nz - 1):
        for q in range(q0):
            z_forward(q, hop)
        if hop == 1 and q0 < nq:
            @pl.when(jnp.logical_not(is_end))
            def _():
                z_own(q0)
    def relay_on(q):
        if q >= nq:
            return
        for hop in range(1, nz - 1):
            z_forward(q, hop)
        if q + 1 < nq:
            @pl.when(jnp.logical_not(is_end))
            def _():
                z_own(q + 1)

    relay_on(q0)

    @pl.when(is_end)
    def _():
        for q in range(q0, nq):
            lr_wait(q)
            for r in range(cq):
                in_copy(q, r, inward).start()
            if q + 1 < nq:
                z_own(q + 1)

    def drain():
        for step in range(1, nh):
            w_copy(step).wait_send()
        sent(pt.at[pl.ds(0, (na - 1) * s.cp)], psend)
        sent(lrs.at[:, pl.ds(0, (g_n - 1) * nq * cq)], lsend)
        for q in range(nq):
            if direct(q):
                @pl.when(jnp.logical_not(is_end))
                def _(q=q):
                    sent(gs.at[:, pl.ds(q * cq, cq), pl.ds(0, g_n - 1)], gsend.at[q])
            else:
                sent(gs.at[:, pl.ds(q * cq, cq), pl.ds(0, g_n - 1)], gsend.at[q])
            for count in range(1, nz):
                @pl.when((z + 1 == count) & goes_up(q))
                def _(q=q, count=count):
                    sent(pg.at[pl.ds(0, count), pl.ds(q * cq, cq)], zsend.at[q, 0])

                @pl.when((nz - z == count) & goes_down(q))
                def _(q=q, count=count):
                    sent(pg.at[pl.ds(0, count), pl.ds(q * cq, cq)], zsend.at[q, 1])
        if q0 < nq:
            @pl.when(is_end)
            def _():
                sent(lrh, hls)

            @pl.when(is_near)
            def _():
                sent(gsh, hgs)

    last = nq - 1
    queue = []

    def run(count):
        for _ in range(min(count, len(queue))):
            q, b = queue.pop(0)
            gather(q, b)
            if b == nb - 1 and q == last - 1:
                r2_start(0)
            if b == nb - 1 and q == last:
                r2_start(final)

    for q in range(nq):
        if q == q0 - 1 and q0 < nq:
            help_end(q0)
            relay_on(q0 + 1)
        elif q > q0:
            help_end(q)
            relay_on(q + 1)
        make(q)
        if q > 1:
            queue += [(q - 2, b) for b in range(nb)]
        if q == last:
            queue += [(last - 1, b) for b in range(nb)] if q else []
            run(max(len(queue) - 2 * nb, 0))
        for b in range(nb):
            run(1 if q < last else 0)
            came_back(q, b)
            g_send(q, b)
            if q == last:
                run(3 if b < nb - 1 else 0)
                if b:
                    queue.append((last, b - 1))
    queue.append((last, nb - 1))
    run(max(len(queue) - 1, 0))
    if nb > 1:
        norm_back(0)
    run(1)
    waiting = list(range(len(batches)))
    for b in range(1 if nb > 1 else 0, nb):
        if len(waiting) > 1:
            r2_sum(waiting.pop(0))
        norm_back(b)
    for batch in waiting:
        r2_sum(batch)
    drain()
    for batch in range(len(batches)):
        r3_wait(batch)
    found_out = pltpu.make_async_copy(rx3, found_hbm, leave.at[0])
    found_out.start()
    sq_wait()
    sq_out = pltpu.make_async_copy(sq.at[pl.ds(0, nh * s.no)], sq_hbm, leave.at[1])
    sq_out.start()
    for b in range(nb):
        keep_copy(b).wait()
        for step in range(1, nh):
            out_copy(b, step).wait()
    for batch, (lo, hi) in enumerate(batches):
        @pl.when(is_owner)
        def _(batch=batch, lo=lo, hi=hi):
            sent(rx2.at[pl.ds(0, nh * s.no - 1), lo:hi], r2s.at[batch])
            sent(rx2.at[pl.ds(0, s.naz - 1), lo:hi], r3s.at[batch])

        @pl.when(jnp.logical_not(is_owner))
        def _(batch=batch, lo=lo, hi=hi):
            sent(rx2.at[pl.ds(0, nh * s.no), lo:hi], r2s.at[batch])

    @pl.when(is_owner)
    def _():
        sent(sq.at[pl.ds(0, total - 1)], qs)
    found_out.wait()
    sq_out.wait()


def finish(s, blocks, from_hbm, found_ref, sq_ref, out_hbm, wg_ref, held, sem_in, sem_out):
    size = held.shape[0] // blocks

    def came(b):
        at = pl.ds(b * size, size)
        return pltpu.make_async_copy(from_hbm.at[at], held.at[at], sem_in.at[b])

    def leaves(b):
        at = pl.ds(b * size, size)
        return pltpu.make_async_copy(held.at[at], out_hbm.at[at], sem_out.at[b])

    for b in range(blocks):
        came(b).start()
    squares = jnp.sum(jnp.sum(sq_ref[...], axis=0), axis=1, keepdims=True)
    factor = jnp.minimum(1.0, CLIP_LIMIT * lax.rsqrt(squares + 1e-06))
    for q in range(s.nq):
        for o in range(s.no):
            w, at = o * s.rs // s.m, q * s.m + o * s.rs % s.m
            wg_ref[w, at:at + s.rs, :] = found_ref[o, q] * factor
    for b in range(blocks):
        came(b).wait()
        leaves(b).start()
    for b in range(blocks):
        leaves(b).wait()


def on_device(na, nz, nh, pair_rep, norm_gain, weights, residue_mask, product_grad):
    rows, cols, depth = pair_rep.shape
    ch = product_grad.shape[1]
    s = Sizes(na, nz, nh, rows, cols, depth, ch)
    vm = pl.BlockSpec(memory_space=pltpu.VMEM)
    anywhere = pl.BlockSpec(memory_space=pl.ANY)
    dma = pltpu.SemaphoreType.DMA
    half = s.rh // 2
    scratch = [
        pltpu.VMEM((s.rh, cols, depth), BF16),
        pltpu.VMEM((rows, ch, cols), BF16),
        pltpu.VMEM((ch, rows, cols), BF16),
        pltpu.VMEM((nz, s.cp, s.i, cols), BF16),
        pltpu.VMEM((nh, 4, ch, depth), BF16),
        pltpu.VMEM((s.nq, depth, 4 * s.nc), BF16),
        pltpu.VMEM((depth, 2 * cols), F32),
        pltpu.VMEM((half, depth, 2 * cols), F32),
        pltpu.VMEM((half, 1, 2 * cols), F32),
        pltpu.VMEM((half, depth, 2 * cols), BF16),
        pltpu.VMEM((4 * s.hid, 2 * cols), F32),
        pltpu.VMEM((half, s.nq, 4, s.nc, 2 * cols), BF16),
        pltpu.VMEM((2, max(s.br * s.sp, s.bi * s.pp), cols), F32),
        pltpu.VMEM((2, s.hid, s.rh, cols), BF16),
        pltpu.VMEM((2, s.cp, s.i, cols), BF16),
        pltpu.VMEM((2, s.helped * s.cq, s.i, cols), BF16),
        pltpu.VMEM((2, s.cp, s.g, s.rh, cols), BF16),
        pltpu.VMEM((2, s.helped * s.cq, s.g, s.rh, cols), BF16),
        pltpu.VMEM((2, s.hid, s.rh, cols), BF16),
        pltpu.VMEM((2, s.nc * s.tp, cols), F32),
        pltpu.VMEM((half, depth, 2 * cols), F32),
        pltpu.VMEM((s.rh, cols, depth), BF16),
        pltpu.VMEM((s.nq, nh, s.no, s.rs, depth), F32),
        pltpu.VMEM((s.naz * nh, s.nq, s.rs, depth), F32),
        pltpu.VMEM((s.no, s.nq, s.rs, depth), F32),
        pltpu.VMEM((s.naz * nh, 1, depth), F32),
        dma(()), dma((s.nq,)), dma((nh,)), dma((nh,)),
        dma(()), dma((2 * s.cq + s.nq,)), dma((s.nq, 2)), dma((2 * s.cq + s.nq, nz)),
        dma(()), dma((s.nq,)), dma((s.nq,)), dma((s.nq, s.nb)),
        dma((s.nb, nh)), dma((s.nb, nh)),
        dma((2,)), dma((2,)), dma((2,)), dma((2,)),
        dma(()), dma(()), dma((s.nb,)), dma((2,)),
        dma(()), dma((s.helped * s.cq,)), dma(()), dma((s.helped, s.nb)),
    ]
    grad, found, squares = pl.pallas_call(
        functools.partial(kernel, s),
        out_shape=(
            jax.ShapeDtypeStruct((rows, cols, depth), BF16),
            jax.ShapeDtypeStruct((s.no, s.nq, s.rs, depth), F32),
            jax.ShapeDtypeStruct((nh * s.no, 1, depth), F32),
        ),
        in_specs=[anywhere, anywhere, vm, vm, vm, pl.BlockSpec(memory_space=pltpu.SMEM)],
        out_specs=(anywhere, anywhere, anywhere),
        scratch_shapes=scratch,
        compiler_params=pltpu.CompilerParams(
            collective_id=0, has_side_effects=True, vmem_limit_bytes=VMEM_LIMIT),
    )(product_grad, pair_rep, weights.transpose(0, 2, 1), norm_gain.reshape(1, depth),
      residue_mask.reshape(nz, cols), residue_mask)
    blocks = math.gcd(rows, 4)
    pair_grad, weight_grads = pl.pallas_call(
        functools.partial(finish, s, blocks),
        out_shape=(
            jax.ShapeDtypeStruct((rows, cols, depth), BF16),
            jax.ShapeDtypeStruct((4, ch, depth), F32),
        ),
        in_specs=[pl.BlockSpec(memory_space=pl.ANY), vm, vm],
        out_specs=(pl.BlockSpec(memory_space=pl.ANY), vm),
        scratch_shapes=[pltpu.VMEM((rows, cols, depth), BF16), dma((blocks,)), dma((blocks,))],
    )(grad, found, squares)
    return (pair_grad, weight_grads.transpose(0, 2, 1))


def solution(mesh):
    sizes = mesh.shape["ia"], mesh.shape["ja"], mesh.shape["col"]
    placed = (P("ia", "ja", None), P(), P(None, None, "col"), P(), P("ia", "col", "ja"))

    def step(*args):
        return on_device(*sizes, *args)

    return jax.shard_map(
        step,
        mesh=mesh,
        in_specs=placed,
        out_specs=(P("ia", "ja", None), P(None, None, "col")),
        check_vma=False,
    )
```

```python
import functools
import math

import jax
import jax.numpy as jnp
from jax import lax
from jax.experimental import pallas as pl
from jax.experimental.pallas import tpu as pltpu
from jax.sharding import PartitionSpec as P

CLIP_LIMIT = 64.0
MAX_CHUNKS = 4
ROWS_AT_ONCE = 4
VMEM_LIMIT = 66 * 1000 * 1000
MESH = pl.DeviceIdType.MESH
NT = (((1,), (1,)), ((), ()))
NN = (((1,), (0,)), ((), ()))
F32 = jnp.float32
BF16 = jnp.bfloat16


def dot(a, b, dims):
    return lax.dot_general(a, b, dims, preferred_element_type=F32)


def eye(n):
    rows = lax.broadcasted_iota(jnp.int32, (n, n), 0)
    cols = lax.broadcasted_iota(jnp.int32, (n, n), 1)
    return jnp.where(rows == cols, 1.0, 0.0).astype(BF16)


class Sizes:
    def __init__(self, na, nz, nh, rows, cols, depth, ch):
        self.na, self.nz, self.nh = na, nz, nh
        self.rb, self.k, self.d, self.ch = rows, cols, depth, ch
        self.g = na * nh
        self.naz = na * nz
        self.rh = rows // nh
        self.hid = ch * nh
        self.cp = ch // na
        self.nq = math.gcd(self.cp, MAX_CHUNKS)
        self.cq = self.cp // self.nq
        self.m = na * self.cq
        self.nc = self.g * self.cq
        self.i = na * rows
        self.br = math.gcd(self.rh, 16)
        self.nb = self.rh // self.br
        self.bi = math.gcd(self.rb, 16)
        self.sp = self.hid + 8
        self.pp = self.m + 8
        self.tp = self.br + 8
        self.tb = math.gcd(self.br // 2, ROWS_AT_ONCE)
        self.no = math.gcd(max(4 * self.m // 8, 1), self.naz)
        self.rs = 4 * self.m // self.no
        self.per = max(self.no // na, 1)
        self.stride = na * self.per // self.no
        self.base = (nz - self.per) // 2
        self.q0 = self.nq - self.nq // 2 if nz > 3 else self.nq
        self.helped = max(self.nq - self.q0, 1)


def kernel(s, p_hbm, x_hbm, w_ref, gain_ref, mask_ref, mask_s, out_hbm, found_hbm, sq_hbm,
           xv, p_ref, pt, pg, wall, wt, gain, unit_s, inv_s, nt_s, pr, fac, relay, lrs, lrb, lrh, gs, gsh, gr, turn, ng,
           outv, raw, rx2, rx3, sq,
           xsem, pin, wsend, wrecv, psend, precv, zsend, zrecv, lsend, lrecv, gsend, grecv, osend, orecv,
           r2s, r2r, r3s, r3r, qs, qr, keep, leave, hls, hlr, hgs, hgr):
    na, nz, nh, g_n, nq, cq, nc = s.na, s.nz, s.nh, s.g, s.nq, s.cq, s.nc
    rb, rh, k, d, ch, hid, br, nb, m = s.rb, s.rh, s.k, s.d, s.ch, s.hid, s.br, s.nb, s.m
    a, z, h = lax.axis_index("ia"), lax.axis_index("ja"), lax.axis_index("col")
    me_g = h * na + a
    me_n = a * nz + z
    row0 = a * rb + h * rh
    q0 = s.q0
    is_end = (z == 0) | (z == nz - 1)
    is_near = (z == 1) | (z == nz - 2)
    inward = jnp.where(z == 0, 1, nz - 2)
    outward = jnp.where(z == 1, 0, nz - 1)

    def plane(g):
        return (lax.rem(g, na), z, lax.div(g, na))

    def peer_g(step):
        return lax.rem(me_g + step, g_n)

    def sent(ref, sem):
        pltpu.make_async_copy(ref, ref, sem).wait()

    def send(src, dst, send_sem, recv_sem, device):
        return pltpu.make_async_remote_copy(
            src_ref=src, dst_ref=dst, send_sem=send_sem, recv_sem=recv_sem,
            device_id=device, device_id_type=MESH)

    barrier = pltpu.get_barrier_semaphore()
    total = s.naz * nh
    me_t = me_n * nh + h

    def at_t(t):
        return (lax.div(t, nz * nh), lax.rem(lax.div(t, nh), nz), lax.rem(t, nh))

    def p_in(q):
        at = pl.ds(q * m, m)
        return pltpu.make_async_copy(p_hbm.at[:, at], p_ref.at[:, at], pin.at[q])

    for q in range(nq):
        p_in(q).start()
    for step in range(1, total):
        pl.semaphore_signal(barrier, inc=1, device_id=at_t(lax.rem(me_t + step, total)), device_id_type=MESH)
    xcopy = pltpu.make_async_copy(x_hbm.at[pl.ds(h * rh, rh)], xv, xsem)
    xcopy.start()

    def p_turn(q):
        p_in(q).wait()

        def block(ib, carry):
            slot = lax.rem(ib, 2)
            for ii in range(s.bi):
                relay[slot, ii * s.pp:ii * s.pp + m, :] = p_ref[ib * s.bi + ii, q * m:(q + 1) * m, :].astype(F32)
            for c in range(m):
                tile = relay[slot, pl.ds(c, s.bi, stride=s.pp), :]
                pt[q * m + c, pl.ds(pl.multiple_of(ib * s.bi, s.bi), s.bi), :] = tile.astype(BF16)
            return carry
        lax.fori_loop(0, rb // s.bi, block, 0)

    def pieces(q):
        return [(q * cq + r, 1) for r in range(cq)] if q in (0, q0) else [(q * cq, cq)]

    starts = [piece[0] for q in range(nq) for piece in pieces(q)]

    def spot(c):
        return starts.index(c)

    def p_copy(piece, step):
        c, n = piece
        to = lax.rem(a + step, na)
        return send(pt.at[pl.ds((c // cq) * m + to * cq + c % cq, n)], pg.at[z, pl.ds(c, n), pl.ds(a * rb, rb)],
                    psend, precv.at[spot(c)], (to, z, h))

    def w_copy(step):
        return send(w_ref, wall.at[h], wsend.at[step], wrecv.at[step], (a, z, lax.rem(h + step, nh)))

    p_turn(0)
    pl.semaphore_wait(barrier, total - 1)
    for step in range(1, nh):
        w_copy(step).start()
    for q in range(nq):
        if q:
            p_turn(q)
        for piece in pieces(q):
            for step in range(1, na):
                p_copy(piece, step).start()
    for q in range(nq):
        for r in range(cq):
            pg[z, q * cq + r, pl.ds(a * rb, rb), :] = pt[q * m + a * cq + r]

    def z_copy(piece, block, up):
        c, n = piece
        ref = pg.at[block, pl.ds(c, n)]
        return send(ref, ref, zsend.at[c // cq, 0 if up else 1], zrecv.at[spot(c), block],
                    (a, z + 1 if up else z - 1, h))

    def goes_up(q):
        return z < (nz - 1 if q < q0 else nz - 2)

    def goes_down(q):
        return z > (0 if q < q0 else 1)

    def z_own(q, some=None):
        for piece in some or pieces(q):
            sent(pt.at[pl.ds(0, (na - 1) * piece[1])], precv.at[spot(piece[0])])

            @pl.when(goes_up(q))
            def _(piece=piece):
                z_copy(piece, z, True).start()

            @pl.when(goes_down(q))
            def _(piece=piece):
                z_copy(piece, z, False).start()

    def z_forward(q, hop):
        @pl.when((z >= hop) & goes_up(q))
        def _():
            for piece in pieces(q):
                z_copy(piece, z - hop, True).wait_recv()
                z_copy(piece, z - hop, True).start()

        @pl.when((z + hop < nz) & goes_down(q))
        def _():
            for piece in pieces(q):
                z_copy(piece, z + hop, False).wait_recv()
                z_copy(piece, z + hop, False).start()

    def z_rest(q, some=None):
        for hop in range(1, nz):
            here = True if q < q0 else jnp.logical_not(is_end)

            @pl.when((z >= hop) & jnp.logical_not(goes_up(q)) & here)
            def _(hop=hop):
                for piece in some or pieces(q):
                    z_copy(piece, z - hop, True).wait_recv()

            @pl.when((z + hop < nz) & jnp.logical_not(goes_down(q)) & here)
            def _(hop=hop):
                for piece in some or pieces(q):
                    z_copy(piece, z + hop, False).wait_recv()

    eye_d = eye(d)
    column = jnp.transpose(jnp.broadcast_to(gain_ref[...], (k, d)))
    gain[...] = jnp.concatenate([column, column], axis=1)
    wall[h] = w_ref[...]
    for step in range(1, nh):
        w_copy(step).wait_recv()
    for q in range(nq):
        rows = [wall[half, w, q * m:(q + 1) * m, :] for half in range(nh) for w in range(4)]
        wt[q] = dot(eye_d, jnp.concatenate(rows, axis=0), NT).astype(BF16)

    xcopy.wait()
    col_valid = mask_ref[pl.ds(z, 1), :].astype(F32)

    def rows_step(t, sub):
        x2 = xv[pl.ds(2 * t, 2)].reshape(2 * k, d)
        xt = dot(eye_d, x2, NT)
        centred = xt - jnp.mean(xt, axis=0, keepdims=True)
        inv = lax.rsqrt(jnp.mean(centred * centred, axis=0, keepdims=True) + 1e-05)
        unit = centred * inv
        normed = (unit * gain[...]).astype(BF16)
        unit_s[t] = unit
        inv_s[t] = inv
        nt_s[t] = normed
        for half in range(nh):
            pr[half * 4 * ch:(half + 1) * 4 * ch, :] = dot(wall[half].reshape(4 * ch, d), normed, NN)
        valid = jnp.concatenate(
            [col_valid * mask_s[row0 + 2 * t + e].astype(F32) for e in range(2)], axis=1)
        for q in range(nq):
            for side in range(2):
                def part(w):
                    at = [half * 4 * ch + w * ch + q * m for half in range(nh)]
                    return jnp.concatenate([pr[x:x + m, :] for x in at], axis=0)
                lin = part(2 * side)
                gate = jax.nn.sigmoid(part(2 * side + 1))
                first = valid * gate
                value = first * lin
                fac[t, q, 2 * side] = first.astype(BF16)
                fac[t, q, 2 * side + 1] = (value * (1.0 - gate)).astype(BF16)
                for e in range(2):
                    at = pl.multiple_of((2 * sub + e) * s.sp, 8) + q * nc
                    relay[side, pl.ds(at, nc), :] = value[:, e * k:(e + 1) * k]

    for b in range(nb):
        def one(sub, carry, b=b):
            rows_step(b * (br // 2) + sub, sub)
            return carry
        parts = pieces(0) if b == 0 else [None]
        each = br // 2 // len(parts)
        if each * len(parts) * 2 == br:
            for n, piece in enumerate(parts):
                lax.fori_loop(n * each, (n + 1) * each, one, 0)
                if piece:
                    z_own(0, [piece])
        else:
            lax.fori_loop(0, br // 2, one, 0)
            if b == 0:
                z_own(0)

        def flush(c, carry, b=b):
            for side in range(2):
                tile = relay[side, pl.ds(c, br, stride=s.sp), :]
                lrs[side, c, b * br:(b + 1) * br, :] = tile.astype(BF16)
            return carry
        lax.fori_loop(0, hid, flush, 0, unroll=4)
        if 0 < b < q0:
            z_own(b)
    for q in range(nb, q0):
        z_own(q)

    if q0 < nq:
        @pl.when(is_end)
        def _():
            z_own(q0)

    def lr_copy(q, step):
        return send(lrs.at[:, pl.ds(q * nc + peer_g(step) * cq, cq)],
                    lrb.at[:, pl.ds(q * cq, cq), pl.ds(row0, rh)],
                    lsend, lrecv.at[q], plane(peer_g(step)))

    for q in [*range(q0, nq), *range(q0)]:
        for step in range(1, g_n):
            lr_copy(q, step).start()
    for q in range(nq):
        for side in range(2):
            for r in range(cq):
                lrb[side, q * cq + r, pl.ds(row0, rh), :] = lrs[side, q * nc + me_g * cq + r]

    eye_k = eye(k)

    def triangle(c, lr, at, to):
        panel = jnp.concatenate([pg[b, c] for b in range(nz)], axis=1)
        left, right = lr[0, at], lr[1, at]
        to[0, at] = dot(panel, right, NN).astype(BF16).reshape(g_n, rh, k)
        left_t = dot(eye_k, left, NT).astype(BF16)
        back_t = dot(left_t, panel, NN).astype(BF16)
        back = [dot(eye_k, back_t[:, b * k:(b + 1) * k], NT).astype(BF16) for b in range(nz)]
        to[1, at] = jnp.concatenate(back, axis=0).reshape(g_n, rh, k)

    def triangles(q, lr, to, base):
        def one(r, carry):
            triangle(q * cq + r, lr, (q - base) * cq + r, to)
            return carry
        lax.fori_loop(0, cq, one, 0)

    def in_copy(q, r, z_to):
        at = (q - q0) * cq + r
        return send(lrb.at[:, pl.ds(q * cq + r, 1)], lrh.at[:, pl.ds(at, 1)], hls, hlr.at[at], (a, z_to, h))

    def g_copy(q, b, step):
        g = peer_g(step)
        place = lax.rem(g, na) * nh + lax.div(g, na)
        return send(gs.at[:, pl.ds(q * cq, cq), place, pl.ds(b * br, br)],
                    gr.at[:, pl.ds(q * nc + me_g * cq, cq), pl.ds(b * br, br)],
                    gsend.at[q], grecv.at[q, b], plane(g))

    def back_copy(q, b, z_to):
        return send(gsh.at[:, pl.ds((q - q0) * cq, cq), :, pl.ds(b * br, br)],
                    gs.at[:, pl.ds(q * cq, cq), :, pl.ds(b * br, br)],
                    hgs, hgr.at[q - q0, b], (a, z_to, h))

    def direct(q):
        return q == nq - 1 and q >= q0

    def direct_copy(q, b, step):
        g = peer_g(step)
        place = lax.rem(g, na) * nh + lax.div(g, na)
        return send(gsh.at[:, pl.ds((q - q0) * cq, cq), place, pl.ds(b * br, br)],
                    gr.at[:, pl.ds(q * nc + me_g * cq, cq), pl.ds(b * br, br)],
                    hgs, grecv.at[q, b], (lax.rem(g, na), outward, lax.div(g, na)))

    def out_copy(b, step):
        return send(outv.at[pl.ds(b * br, br)], out_hbm.at[pl.ds(h * rh + b * br, br)],
                    osend.at[b, step], orecv.at[b, step], (a, z, lax.rem(h + step, nh)))

    def keep_copy(b):
        return pltpu.make_async_copy(
            outv.at[pl.ds(b * br, br)], out_hbm.at[pl.ds(h * rh + b * br, br)], keep.at[b])

    def at_n(n):
        return (lax.div(n, nz), lax.rem(n, nz), h)

    def owner(o):
        return (o // s.per * s.stride, s.base + o % s.per)

    def other(o, half=None):
        away = (a != owner(o)[0]) | (z != owner(o)[1])
        return away if half is None else away | (h != half)

    me_o = lax.div(a, s.stride) * s.per + z - s.base
    is_owner = (lax.rem(a, s.stride) == 0) & (z >= s.base) & (z < s.base + s.per)
    batches = [(0, nq - 1), (nq - 1, nq)] if nq > 1 else [(0, nq)]
    final = len(batches) - 1

    def r2_copy(batch, half, o, sender):
        lo, hi = batches[batch]
        return send(raw.at[lo:hi, half, o], rx2.at[sender, lo:hi],
                    r2s.at[batch], r2r.at[batch], (*owner(o), half))

    def r2_start(batch):
        for half in range(nh):
            for o in range(s.no):
                @pl.when(other(o, half))
                def _(half=half, o=o):
                    r2_copy(batch, half, o, me_t).start()

    def r3_copy(batch, o, step):
        lo, hi = batches[batch]
        ref = rx3.at[o, lo:hi]
        return send(ref, ref, r3s.at[batch], r3r.at[batch], at_n(lax.rem(me_n + step, s.naz)))

    def sq_copy(slot, step):
        ref = sq.at[slot]
        return send(ref, ref, qs, qr, at_t(lax.rem(me_t + step, total)))

    def r2_sum(batch):
        lo, hi = batches[batch]

        @pl.when(is_owner)
        def _():
            def one(step, mine):
                return mine + rx2[lax.rem(me_t + step, total), lo:hi]
            sent(rx2.at[pl.ds(0, total - 1), lo:hi], r2r.at[batch])
            rx3[me_o, lo:hi] = lax.fori_loop(1, total, one, raw[lo:hi, h, me_o])
            for step in range(1, s.naz):
                r3_copy(batch, me_o, step).start()
            if batch == final:
                slot = h * s.no + me_o
                found = rx3[me_o].reshape(nq * s.rs, d)
                sq[slot] = jnp.sum(found * found, axis=0, keepdims=True)
                for step in range(1, total):
                    sq_copy(slot, step).start()

    def at_role(wait):
        @pl.when(is_owner)
        def _():
            wait(1)

        @pl.when(jnp.logical_not(is_owner))
        def _():
            wait(0)

    def r3_wait(batch):
        lo, hi = batches[batch]
        at_role(lambda own: sent(rx2.at[pl.ds(0, s.no - own), lo:hi], r3r.at[batch]))

    def sq_wait():
        at_role(lambda own: sent(sq.at[pl.ds(0, nh * s.no - own)], qr))

    def gather(q, b):
        def came(count):
            sent(gr.at[:, pl.ds(0, count * cq), pl.ds(0, br)], grecv.at[q, b])

        if direct(q):
            @pl.when(is_end)
            def _():
                came(g_n)

            @pl.when(jnp.logical_not(is_end))
            def _():
                came(g_n - 1)
        else:
            came(g_n - 1)

        def spread(n, carry):
            for side in range(2):
                tile = gr[side, q * nc + n, b * br:(b + 1) * br, :].astype(F32)
                turn[side, pl.ds(pl.multiple_of(n * s.tp, 8), br), :] = tile
            return carry
        lax.fori_loop(0, nc, spread, 0, unroll=4)
        if b == 0:
            raw[q] = jnp.zeros((nh, s.no, s.rs, d), F32)

        def one(sub, carry):
            t0 = b * (br // 2) + sub * s.tb
            terms = []
            for side in range(2):
                both = jnp.concatenate(
                    [turn[side, pl.ds(2 * s.tb * sub + e, nc, stride=s.tp), :] for e in range(2 * s.tb)], axis=1)
                for w in range(2):
                    factor = jnp.concatenate([fac[t0 + u, q, 2 * side + w] for u in range(s.tb)], axis=1)
                    terms.append((both * factor.astype(F32)).astype(BF16))
            grads = jnp.concatenate(
                [term[half * m:(half + 1) * m] for half in range(nh) for term in terms], axis=0)
            normed = jnp.concatenate([nt_s[t0 + u] for u in range(s.tb)], axis=1)
            raw[q] += dot(grads, normed, NT).reshape(nh, s.no, s.rs, d)
            part = dot(wt[q], grads, NN)
            for u in range(s.tb):
                piece = part[:, u * 2 * k:(u + 1) * 2 * k]
                ng[t0 + u] = ng[t0 + u] + piece if q else piece
            return carry
        lax.fori_loop(0, br // 2 // s.tb, one, 0)

    def norm_back(b):
        def one(sub, carry):
            t = b * (br // 2) + sub
            unit = unit_s[t]
            scaled = ng[t] * gain[...]
            first = jnp.mean(scaled, axis=0, keepdims=True)
            second = jnp.mean(scaled * unit, axis=0, keepdims=True)
            res = (inv_s[t] * (scaled - first - unit * second)).astype(BF16)
            for e in range(2):
                outv[2 * t + e] = dot(eye_k, res[:, e * k:(e + 1) * k], NT).astype(BF16)
            return carry
        lax.fori_loop(0, br // 2, one, 0, unroll=2)
        keep_copy(b).start()
        for step in range(1, nh):
            out_copy(b, step).start()

    def lr_wait(q):
        sent(lrs.at[:, pl.ds(0, (g_n - 1) * cq)], lrecv.at[q])

    def g_out(q, b):
        for step in range(1, g_n):
            g_copy(q, b, step).start()
        for side in range(2):
            for r in range(cq):
                gr[side, q * nc + me_g * cq + r, b * br:(b + 1) * br, :] = gs[
                    side, q * cq + r, a * nh + h, b * br:(b + 1) * br, :]

    def g_send(q, b):
        if direct(q):
            @pl.when(jnp.logical_not(is_end))
            def _():
                g_out(q, b)
        else:
            g_out(q, b)

    def help_end(q):
        @pl.when(is_near)
        def _():
            if q != q0:
                z_rest(q)
            for r in range(cq):
                if q == q0:
                    z_rest(q, [pieces(q)[r]])
                in_copy(q, r, outward).wait_recv()
                triangle(q * cq + r, lrh, (q - q0) * cq + r, gsh)
            for b in range(nb):
                if direct(q):
                    for step in range(g_n):
                        direct_copy(q, b, step).start()
                else:
                    back_copy(q, b, outward).start()

    def make(q):
        if q < q0:
            z_rest(q)
            lr_wait(q)
            triangles(q, lrb, gs, 0)
            return

        @pl.when(jnp.logical_not(is_near | is_end))
        def _():
            z_rest(q)

        @pl.when(jnp.logical_not(is_end))
        def _():
            lr_wait(q)
            triangles(q, lrb, gs, 0)

    def came_back(q, b):
        if q >= q0 and not direct(q):
            @pl.when(is_end)
            def _():
                back_copy(q, b, outward).wait_recv()

    for hop in range(1, nz - 1):
        for q in range(q0):
            z_forward(q, hop)
        if hop == 1 and q0 < nq:
            @pl.when(jnp.logical_not(is_end))
            def _():
                z_own(q0)
    def relay_on(q):
        if q >= nq:
            return
        for hop in range(1, nz - 1):
            z_forward(q, hop)
        if q + 1 < nq:
            @pl.when(jnp.logical_not(is_end))
            def _():
                z_own(q + 1)

    relay_on(q0)

    @pl.when(is_end)
    def _():
        for q in range(q0, nq):
            lr_wait(q)
            for r in range(cq):
                in_copy(q, r, inward).start()
            if q + 1 < nq:
                z_own(q + 1)

    def drain():
        for step in range(1, nh):
            w_copy(step).wait_send()
        sent(pt.at[pl.ds(0, (na - 1) * s.cp)], psend)
        sent(lrs.at[:, pl.ds(0, (g_n - 1) * nq * cq)], lsend)
        for q in range(nq):
            if direct(q):
                @pl.when(jnp.logical_not(is_end))
                def _(q=q):
                    sent(gs.at[:, pl.ds(q * cq, cq), pl.ds(0, g_n - 1)], gsend.at[q])
            else:
                sent(gs.at[:, pl.ds(q * cq, cq), pl.ds(0, g_n - 1)], gsend.at[q])
            for count in range(1, nz):
                @pl.when((z + 1 == count) & goes_up(q))
                def _(q=q, count=count):
                    sent(pg.at[pl.ds(0, count), pl.ds(q * cq, cq)], zsend.at[q, 0])

                @pl.when((nz - z == count) & goes_down(q))
                def _(q=q, count=count):
                    sent(pg.at[pl.ds(0, count), pl.ds(q * cq, cq)], zsend.at[q, 1])
        if q0 < nq:
            @pl.when(is_end)
            def _():
                sent(lrh, hls)

            @pl.when(is_near)
            def _():
                sent(gsh, hgs)

    last = nq - 1
    queue = []

    def run(count):
        for _ in range(min(count, len(queue))):
            q, b = queue.pop(0)
            gather(q, b)
            if b == nb - 1 and q == last - 1:
                r2_start(0)
            if b == nb - 1 and q == last:
                r2_start(final)

    for q in range(nq):
        if q == q0 - 1 and q0 < nq:
            help_end(q0)
            relay_on(q0 + 1)
        elif q > q0:
            help_end(q)
            relay_on(q + 1)
        make(q)
        if q > 1:
            queue += [(q - 2, b) for b in range(nb)]
        if q == last:
            queue += [(last - 1, b) for b in range(nb)] if q else []
            run(max(len(queue) - 2 * nb, 0))
        for b in range(nb):
            run(1 if q < last else 0)
            came_back(q, b)
            g_send(q, b)
            if q == last:
                run(3 if b < nb - 1 else 0)
                if b:
                    queue.append((last, b - 1))
    queue.append((last, nb - 1))
    run(max(len(queue) - 1, 0))
    if nb > 1:
        norm_back(0)
    run(1)
    waiting = list(range(len(batches)))
    for b in range(1 if nb > 1 else 0, nb):
        if len(waiting) > 1:
            r2_sum(waiting.pop(0))
        norm_back(b)
    for batch in waiting:
        r2_sum(batch)
    drain()
    for batch in range(len(batches)):
        r3_wait(batch)
    found_out = pltpu.make_async_copy(rx3, found_hbm, leave.at[0])
    found_out.start()
    sq_wait()
    sq_out = pltpu.make_async_copy(sq.at[pl.ds(0, nh * s.no)], sq_hbm, leave.at[1])
    sq_out.start()
    for b in range(nb):
        keep_copy(b).wait()
        for step in range(1, nh):
            out_copy(b, step).wait()
    for batch, (lo, hi) in enumerate(batches):
        @pl.when(is_owner)
        def _(batch=batch, lo=lo, hi=hi):
            sent(rx2.at[pl.ds(0, nh * s.no - 1), lo:hi], r2s.at[batch])
            sent(rx2.at[pl.ds(0, s.naz - 1), lo:hi], r3s.at[batch])

        @pl.when(jnp.logical_not(is_owner))
        def _(batch=batch, lo=lo, hi=hi):
            sent(rx2.at[pl.ds(0, nh * s.no), lo:hi], r2s.at[batch])

    @pl.when(is_owner)
    def _():
        sent(sq.at[pl.ds(0, total - 1)], qs)
    found_out.wait()
    sq_out.wait()


def finish(s, blocks, from_hbm, found_ref, sq_ref, out_hbm, wg_ref, held, sem_in, sem_out):
    size = held.shape[0] // blocks

    def came(b):
        at = pl.ds(b * size, size)
        return pltpu.make_async_copy(from_hbm.at[at], held.at[at], sem_in.at[b])

    def leaves(b):
        at = pl.ds(b * size, size)
        return pltpu.make_async_copy(held.at[at], out_hbm.at[at], sem_out.at[b])

    for b in range(blocks):
        came(b).start()
    squares = jnp.sum(jnp.sum(sq_ref[...], axis=0), axis=1, keepdims=True)
    factor = jnp.minimum(1.0, CLIP_LIMIT * lax.rsqrt(squares + 1e-06))
    for q in range(s.nq):
        for o in range(s.no):
            w, at = o * s.rs // s.m, q * s.m + o * s.rs % s.m
            wg_ref[w, at:at + s.rs, :] = found_ref[o, q] * factor
    for b in range(blocks):
        came(b).wait()
        leaves(b).start()
    for b in range(blocks):
        leaves(b).wait()


def on_device(na, nz, nh, pair_rep, norm_gain, weights, residue_mask, product_grad):
    rows, cols, depth = pair_rep.shape
    ch = product_grad.shape[1]
    s = Sizes(na, nz, nh, rows, cols, depth, ch)
    vm = pl.BlockSpec(memory_space=pltpu.VMEM)
    anywhere = pl.BlockSpec(memory_space=pl.ANY)
    dma = pltpu.SemaphoreType.DMA
    half = s.rh // 2
    scratch = [
        pltpu.VMEM((s.rh, cols, depth), BF16),
        pltpu.VMEM((rows, ch, cols), BF16),
        pltpu.VMEM((ch, rows, cols), BF16),
        pltpu.VMEM((nz, s.cp, s.i, cols), BF16),
        pltpu.VMEM((nh, 4, ch, depth), BF16),
        pltpu.VMEM((s.nq, depth, 4 * s.nc), BF16),
        pltpu.VMEM((depth, 2 * cols), F32),
        pltpu.VMEM((half, depth, 2 * cols), F32),
        pltpu.VMEM((half, 1, 2 * cols), F32),
        pltpu.VMEM((half, depth, 2 * cols), BF16),
        pltpu.VMEM((4 * s.hid, 2 * cols), F32),
        pltpu.VMEM((half, s.nq, 4, s.nc, 2 * cols), BF16),
        pltpu.VMEM((2, max(s.br * s.sp, s.bi * s.pp), cols), F32),
        pltpu.VMEM((2, s.hid, s.rh, cols), BF16),
        pltpu.VMEM((2, s.cp, s.i, cols), BF16),
        pltpu.VMEM((2, s.helped * s.cq, s.i, cols), BF16),
        pltpu.VMEM((2, s.cp, s.g, s.rh, cols), BF16),
        pltpu.VMEM((2, s.helped * s.cq, s.g, s.rh, cols), BF16),
        pltpu.VMEM((2, s.hid, s.rh, cols), BF16),
        pltpu.VMEM((2, s.nc * s.tp, cols), F32),
        pltpu.VMEM((half, depth, 2 * cols), F32),
        pltpu.VMEM((s.rh, cols, depth), BF16),
        pltpu.VMEM((s.nq, nh, s.no, s.rs, depth), F32),
        pltpu.VMEM((s.naz * nh, s.nq, s.rs, depth), F32),
        pltpu.VMEM((s.no, s.nq, s.rs, depth), F32),
        pltpu.VMEM((s.naz * nh, 1, depth), F32),
        dma(()), dma((s.nq,)), dma((nh,)), dma((nh,)),
        dma(()), dma((2 * s.cq + s.nq,)), dma((s.nq, 2)), dma((2 * s.cq + s.nq, nz)),
        dma(()), dma((s.nq,)), dma((s.nq,)), dma((s.nq, s.nb)),
        dma((s.nb, nh)), dma((s.nb, nh)),
        dma((2,)), dma((2,)), dma((2,)), dma((2,)),
        dma(()), dma(()), dma((s.nb,)), dma((2,)),
        dma(()), dma((s.helped * s.cq,)), dma(()), dma((s.helped, s.nb)),
    ]
    grad, found, squares = pl.pallas_call(
        functools.partial(kernel, s),
        out_shape=(
            jax.ShapeDtypeStruct((rows, cols, depth), BF16),
            jax.ShapeDtypeStruct((s.no, s.nq, s.rs, depth), F32),
            jax.ShapeDtypeStruct((nh * s.no, 1, depth), F32),
        ),
        in_specs=[anywhere, anywhere, vm, vm, vm, pl.BlockSpec(memory_space=pltpu.SMEM)],
        out_specs=(anywhere, anywhere, anywhere),
        scratch_shapes=scratch,
        compiler_params=pltpu.CompilerParams(
            collective_id=0, has_side_effects=True, vmem_limit_bytes=VMEM_LIMIT),
    )(product_grad, pair_rep, weights.transpose(0, 2, 1), norm_gain.reshape(1, depth),
      residue_mask.reshape(nz, cols), residue_mask)
    blocks = math.gcd(rows, 4)
    pair_grad, weight_grads = pl.pallas_call(
        functools.partial(finish, s, blocks),
        out_shape=(
            jax.ShapeDtypeStruct((rows, cols, depth), BF16),
            jax.ShapeDtypeStruct((4, ch, depth), F32),
        ),
        in_specs=[pl.BlockSpec(memory_space=pl.ANY), vm, vm],
        out_specs=(pl.BlockSpec(memory_space=pl.ANY), vm),
        scratch_shapes=[pltpu.VMEM((rows, cols, depth), BF16), dma((blocks,)), dma((blocks,))],
    )(grad, found, squares)
    return (pair_grad, weight_grads.transpose(0, 2, 1))


def solution(mesh):
    sizes = mesh.shape["ia"], mesh.shape["ja"], mesh.shape["col"]
    placed = (P("ia", "ja", None), P(), P(None, None, "col"), P(), P("ia", "col", "ja"))

    def step(*args):
        return on_device(*sizes, *args)

    return jax.shard_map(
        step,
        mesh=mesh,
        in_specs=placed,
        out_specs=(P("ia", "ja", None), P(None, None, "col")),
        check_vma=False,
    )
```
